256 devices in a mesh: grp: 2 (over y), gx: 64 (over x, z), gy: 2 (over core).
Axes of the slice: x: 4, y: 2, z: 16, core: 2. Of those that a mesh axis runs over, the one named last changes fastest.
The devices are a block of a 4x16x16 slice.
Arguments:
- residue_feats: bfloat16 [2048, 256], P(('grp', 'gx')), parts along dimension 0, may hold values from -6 to 6
- pair_feats: bfloat16 [64, 2048, 1024], P(None, ('grp', 'gx'), 'gy'), parts along dimension 1, may hold values from -30 to 30
- w_row: bfloat16 [256, 64], replicated, may hold values from -0.375 to 0.375
- w_col: bfloat16 [256, 64], replicated, may hold values from -0.375 to 0.375
- first_taps: bfloat16 [9, 64, 64], replicated, may hold values from -0.25 to 0.25
- second_taps: bfloat16 [9, 64, 64], replicated, may hold values from -0.25 to 0.25
- norm_scale: float32 [2, 64], replicated, may hold values from 0.25 to 1.75
- norm_shift: float32 [2, 64], replicated, may hold values from -2 to 2
Outputs:
- symmetric: bfloat16 [64, 2048, 1024], P(None, ('grp', 'gx'), 'gy'), parts along dimension 1
The draws below stay inside these ranges and needn't reach their ends.
There are 2 independent parts, one for each index of `grp`. The reference program is written for one: setup_inputs(seed, part) draws one part's arguments, and reference() takes and returns one part's arrays. A program takes and returns all parts, laid end to end along the dimension named above; an argument that names none is the same for every part. Nothing has to cross between parts.
All inputs are finite; a program needn't handle non-finite values.
Results may differ from the reference program's by a relative error of at most 0.012.
Values may be sent and summed in bfloat16 or wider, within the bound.
No kernel may reach another device: no remote copies, remote signals or barrier semaphores. Data moves between devices by JAX's collectives and lax.ppermute only.
A program may use at most 64 MiB of HBM per device.

```python
import math
import jax
import jax.numpy as jnp
from jax import lax

CH = 64
FEAT = 256
DILATION_STEP = 8
L = 1024


def draw_pair_feats(key, part):
    key_noise = jax.random.fold_in(key, 11)
    key_rows = jax.random.fold_in(key, 12)
    key_cols = jax.random.fold_in(key, 13)
    key_level = jax.random.fold_in(key, 14)
    row_scale = jnp.exp(jax.random.uniform(key_rows, (L,), jnp.float32, 0.0, 0.5 * math.log(10.0)))
    col_scale = jnp.exp(jax.random.uniform(key_cols, (L,), jnp.float32, 0.0, 0.5 * math.log(10.0)))
    level = 0.5 * jax.random.truncated_normal(key_level, -3.0, 3.0, (CH, 1, 1), jnp.float32)
    position = jnp.arange(L, dtype=jnp.float32) / L
    noise = jax.random.truncated_normal(key_noise, -5.0, 5.0, (CH, L, L), jnp.float32)
    ramp = 0.5 + 1.5 * position
    value = noise * row_scale[None, :, None] * col_scale[None, None, :] / 3.0 + level * ramp[None, :, None]
    return value.astype(jnp.bfloat16)


def steps_of(own_key, shape, shards, smallest, largest):
    factor_of = 1.0
    for dim, shards_of in shards:
        heights = jax.random.uniform(jax.random.fold_in(jax.random.fold_in(own_key, 6), dim), (shards_of,), jnp.float32, smallest / len(shards), largest / len(shards))
        factor_of = factor_of * jnp.repeat(jnp.exp(heights), shape[dim] // shards_of).reshape((-1,) + (1,) * (len(shape) - 1 - dim))
    return factor_of


def normal_values(own_key, dims, scale, bound, split=(), kind=jnp.bfloat16):
    result = jax.random.normal(own_key, dims, jnp.float32) * scale
    if len(split) > 0:
        result = steps_of(own_key, dims, split, -0.22, 0.18) * result
    return jnp.clip(result, min=-bound, max=bound).astype(kind)


def setup_inputs(seed: int = 0, part: int = 0) -> dict:
    key_list = jax.random.split(jax.random.key(seed), 9)
    own_keys = jax.random.split(jax.random.fold_in(key_list[8], part), 9)
    residue_feats = normal_values(own_keys[0], (L, FEAT), 1.0, 6.0, ((0, 64),))
    pair_feats = draw_pair_feats(jax.random.fold_in(jax.random.fold_in(key_list[8], part), 71), part)
    w_row = normal_values(key_list[2], (FEAT, CH), FEAT ** -0.5, 0.375)
    w_col = normal_values(key_list[3], (FEAT, CH), FEAT ** -0.5, 0.375)
    first_taps = normal_values(key_list[4], (9, CH, CH), (9 * CH) ** -0.5, 0.25)
    second_taps = normal_values(key_list[5], (9, CH, CH), (9 * CH) ** -0.5, 0.25)
    norm_scale = jnp.clip(1.0 + 0.15 * jax.random.normal(key_list[6], (2, CH), jnp.float32), 0.25, 1.75)
    norm_shift = normal_values(key_list[7], (2, CH), 0.5, 2.0, (), jnp.float32)
    return {"residue_feats": residue_feats, "pair_feats": pair_feats, "w_row": w_row, "w_col": w_col, "first_taps": first_taps, "second_taps": second_taps, "norm_scale": norm_scale, "norm_shift": norm_shift}


epsilon = 1e-05

def dilated(receptive_region, weights):
    filter_weight = jnp.transpose(weights.reshape(3, 3, CH, CH), (2, 3, 0, 1))
    tap_sum_total = lax.conv_general_dilated(receptive_region[None], filter_weight, (1, 1), ((DILATION_STEP, DILATION_STEP), (DILATION_STEP, DILATION_STEP)), rhs_dilation=(DILATION_STEP, DILATION_STEP), dimension_numbers=('NCHW', 'OIHW', 'NCHW'), preferred_element_type=jnp.float32)
    return tap_sum_total[0]

def normalized(tap_sum_total, gain, shift):
    average = lax.optimization_barrier(jnp.mean(tap_sum_total, axis=(1, 2)))
    centred = tap_sum_total - average[:, None, None]
    spread = lax.optimization_barrier(jnp.mean(centred * centred, axis=(1, 2)))
    factor = gain * lax.rsqrt(spread + epsilon)
    return centred * factor[:, None, None] + shift[:, None, None]

def reference(residue_feats, pair_feats, w_row, w_col, first_taps, second_taps, norm_scale, norm_shift):
    row_part = jnp.dot(residue_feats, w_row, preferred_element_type=jnp.float32).astype(jnp.bfloat16)
    col_part = jnp.dot(residue_feats, w_col, preferred_element_type=jnp.float32).astype(jnp.bfloat16)
    block_in = (pair_feats.astype(jnp.float32) + row_part.T.astype(jnp.float32)[:, :, None] + col_part.T.astype(jnp.float32)[:, None, :]).astype(jnp.bfloat16)
    first_conv = dilated(block_in, first_taps)
    activated = jax.nn.elu(normalized(first_conv, norm_scale[0], norm_shift[0])).astype(jnp.bfloat16)
    second_conv = dilated(activated, second_taps)
    block_out = jax.nn.elu(block_in.astype(jnp.float32) + normalized(second_conv, norm_scale[1], norm_shift[1])).astype(jnp.bfloat16)
    mirrored = jnp.transpose(block_out, (0, 2, 1))
    return (0.5 * (block_out.astype(jnp.float32) + mirrored.astype(jnp.float32))).astype(jnp.bfloat16)
```

```python
import functools

import jax
import jax.numpy as jnp
from jax import lax
from jax.experimental import pallas as pl
from jax.experimental.pallas import tpu as pltpu
from jax.sharding import Mesh
from jax.sharding import PartitionSpec as P

STEP = 8
GX = ("gx_0", "gx_1")
ALL = ("gx_0", "gx_1", "gy")
GRP_GX = ("grp", "gx_0", "gx_1")
LANES = 128
SWAP = [(0, 1), (1, 0)]
VMEM = pl.BlockSpec(memory_space=pltpu.VMEM)
SMEM = pl.BlockSpec(memory_space=pltpu.SMEM)

epsilon = 1e-05


def chain(count, step):
    pairs = [(i, i + 1) for i in range(count - 1)]
    return pairs if step > 0 else [(b, a) for a, b in pairs]


def cross_chain(count, step):
    return [(2 * a + k, 2 * b + 1 - k) for a, b in chain(count, step) for k in range(2)]


def call(kernel, out_shape, scratch, flops, operands, n_smem=1):
    specs = [SMEM] * n_smem + [VMEM] * (len(operands) - n_smem)
    return pl.pallas_call(
        kernel,
        out_shape=out_shape,
        in_specs=specs,
        out_specs=jax.tree.map(lambda _: VMEM, out_shape),
        scratch_shapes=scratch,
        cost_estimate=pl.CostEstimate(flops=flops, bytes_accessed=1 << 20, transcendentals=0),
        compiler_params=pltpu.CompilerParams(vmem_limit_bytes=56 << 20),
    )(*operands)


def elu(v):
    return jnp.where(v > 0, v, jnp.exp(jnp.minimum(v, 0.0)) - 1.0)


def side_mask(core, channels, valid=1):
    lane = lax.broadcasted_iota(jnp.int32, (channels, LANES), 1)
    first = (LANES - STEP) * core
    return (lane >= first) & (lane < first + STEP * valid)


def as_float(flag):
    return jnp.asarray(flag, jnp.int32).astype(jnp.float32)


def above_valid(row_at):
    return jnp.minimum(row_at, 1)


def below_valid(row_at, devices):
    return jnp.minimum(devices - 1 - row_at, 1)


def term_rows(terms_ref, start, count):
    rows = terms_ref[pl.ds(pl.multiple_of(start, 16), count), :]
    return jnp.transpose(rows.astype(jnp.float32))


def conv_row(x_ref, row, weights):
    stacked = jnp.concatenate([x_ref[row], x_ref[row + STEP], x_ref[row + 2 * STEP]], axis=0)
    taps = jnp.dot(weights, stacked, preferred_element_type=jnp.float32)
    channels, cols = taps.shape[0] // 3, taps.shape[1]
    total = (
        pltpu.roll(taps[:channels], STEP, 1)
        + taps[channels : 2 * channels]
        + pltpu.roll(taps[2 * channels :], cols - STEP, 1)
    )
    return total[:, : cols - LANES]


def sums_of(total, squares):
    both = jnp.concatenate(
        [jnp.sum(total, axis=1, keepdims=True), jnp.sum(squares, axis=1, keepdims=True)], axis=0
    )
    return jnp.transpose(jnp.broadcast_to(both, (LANES, LANES)))[0:1]


def affine_of(stats_refs, gain_ref, shift_ref, cells):
    row = sum(jnp.sum(ref[...], axis=0, keepdims=True) for ref in stats_refs)
    column = jnp.transpose(jnp.broadcast_to(row, (LANES, LANES)))[:, 0:1] / cells
    channels = LANES // 2
    average = column[:channels]
    spread = column[channels:] - average * average
    factor = gain_ref[...] * lax.rsqrt(spread + epsilon)
    return factor, shift_ref[...] - average * factor


def first_kernel(
    devices, place, own, above, below, side, side_above, side_below, terms, weights,
    x_ref, conv_ref, edge_ref, stats_ref,
):
    row_at, core = place[0], place[1]
    rows, channels, cols = own.shape
    col_terms = term_rows(terms, core * cols, cols)[channels:]
    side_start = jnp.where(core == 0, cols, cols - LANES)
    side_terms = term_rows(terms, side_start, LANES)[channels:]
    groups = (
        (above, side_above, 0, STEP, rows - STEP, jnp.maximum(row_at - 1, 0), above_valid(row_at)),
        (own, side, STEP, rows, 0, row_at, 1),
        (below, side_below, STEP + rows, STEP, 0, jnp.minimum(row_at + 1, devices - 1),
         below_valid(row_at, devices)),
    )
    for ref, side_ref, first, count, skip, at, valid in groups:
        row_terms = term_rows(terms, at * rows, rows)[:channels]
        mask, inside = side_mask(core, channels, valid), as_float(valid)
        for r in range(count):
            row = row_terms[:, skip + r : skip + r + 1]
            main = ref[r].astype(jnp.float32) + row + col_terms
            beyond = side_ref[skip + r].astype(jnp.float32) + row + side_terms
            main = main * inside
            beyond = jnp.where(mask, beyond, 0.0)
            x_ref[first + r, :, :cols] = main.astype(jnp.bfloat16)
            x_ref[first + r, :, cols:] = beyond.astype(jnp.bfloat16)

    w = weights[...]

    def step(r, carry):
        total, squares = carry
        out = conv_row(x_ref, r, w)
        conv_ref[r] = out
        edge_ref[r] = jnp.where(core == 0, out[:, cols - LANES :], out[:, :LANES])
        return total + out, squares + out * out

    zero = jnp.zeros((channels, cols), jnp.float32)
    total, squares = lax.fori_loop(0, rows, step, (zero, zero))
    stats_ref[...] = jnp.broadcast_to(sums_of(total, squares), stats_ref.shape)


def far_kernel(
    devices, place, near, above, below, side_above, side_below, terms, weights,
    conv_ref, edge_ref, x_ref,
):
    row_at, core = place[0], place[1]
    channels, cols = above.shape[1], above.shape[2]
    rows = near.shape[0] - 2 * STEP
    col_terms = term_rows(terms, core * cols, cols)[channels:]
    side_terms = term_rows(terms, jnp.where(core == 0, cols, cols - LANES), LANES)[channels:]
    groups = (
        (above, side_above, 0, 0, jnp.maximum(row_at - 1, 0), above_valid(row_at)),
        (below, side_below, 5 * STEP, rows - STEP, jnp.minimum(row_at + 1, devices - 1),
         below_valid(row_at, devices)),
    )
    for ref, side_ref, first, skip, at, valid in groups:
        row_terms = term_rows(terms, at * rows, rows)[:channels]
        mask, inside = side_mask(core, channels, valid), as_float(valid)
        for r in range(STEP):
            row = row_terms[:, skip + r : skip + r + 1]
            main = ref[r].astype(jnp.float32) + row + col_terms
            beyond = side_ref[skip + r].astype(jnp.float32) + row + side_terms
            main = main * inside
            beyond = jnp.where(mask, beyond, 0.0)
            x_ref[first + r, :, :cols] = main.astype(jnp.bfloat16)
            x_ref[first + r, :, cols:] = beyond.astype(jnp.bfloat16)
    x_ref[STEP : 3 * STEP] = near[: 2 * STEP]
    x_ref[3 * STEP : 5 * STEP] = near[rows:]
    w = weights[...]

    def step(r, _):
        for half in range(2):
            out = conv_row(x_ref, r + 3 * STEP * half, w)
            conv_ref[r + STEP * half] = out
            edge_ref[r + STEP * half] = jnp.where(
                core == 0, out[:, cols - LANES :], out[:, :LANES]
            )
        return 0

    lax.fori_loop(0, STEP, step, 0)


def second_kernel(
    devices, cells, place, own, far, side, side_far, stats, stats_other, gain, shift, weights,
    conv_ref, swap_ref, stats_ref, a_ref,
):
    row_at, core = place[0], place[1]
    rows, channels, cols = own.shape
    factor, offset = affine_of((stats, stats_other), gain, shift, cells)
    factor_main = jnp.broadcast_to(factor, (channels, cols))
    offset_main = jnp.broadcast_to(offset, (channels, cols))
    factor_side, offset_side = factor_main[:, :LANES], offset_main[:, :LANES]

    def fill(source, source_side, at, to, valid):
        main = elu(source[at] * factor_main + offset_main)
        beyond = elu(source_side[at] * factor_side + offset_side)
        a_ref[to, :, :cols] = (main * as_float(valid)).astype(jnp.bfloat16)
        mask = side_mask(core, channels, valid)
        a_ref[to, :, cols:] = jnp.where(mask, beyond, 0.0).astype(jnp.bfloat16)

    def outer(r, _):
        fill(far, side_far, r, r, above_valid(row_at))
        fill(far, side_far, r + STEP, r + STEP + rows, below_valid(row_at, devices))
        return 0

    def inner(r, _):
        fill(own, side, r, r + STEP, 1)
        return 0

    lax.fori_loop(0, STEP, outer, 0)
    lax.fori_loop(0, rows, inner, 0)
    w = weights[...]

    def step(r, carry):
        total, squares = carry
        out = conv_row(a_ref, r, w)
        conv_ref[r] = out
        return total + out, squares + out * out

    zero = jnp.zeros((channels, cols), jnp.float32)
    total, squares = lax.fori_loop(0, rows, step, (zero, zero))
    stats_ref[...] = jnp.broadcast_to(sums_of(total, squares), stats_ref.shape)
    give = jnp.where(core == 0, rows // 2, 0)
    swap_ref[...] = conv_ref[pl.ds(give, rows // 2)].astype(jnp.bfloat16)


def pack_kernel(
    cells, place, near, near_other, conv, conv_other, stats, stats_other, gain, shift,
    out_ref, send_ref,
):
    core = place[1]
    rows, channels, cols = conv.shape
    half = rows // 2
    factor, offset = affine_of((stats, stats_other), gain, shift, cells)
    factor = jnp.broadcast_to(factor, (channels, cols))
    offset = jnp.broadcast_to(offset, (channels, cols))
    peers = cols // rows

    def own(r, _):
        value = near[r + STEP, :, :cols].astype(jnp.float32) + conv[r] * factor + offset
        out_ref[r] = elu(value).astype(jnp.bfloat16)
        return 0

    lax.fori_loop(0, rows, own, 0)

    def place_cells(value, r, first):
        both = jnp.concatenate([value, pltpu.roll(value, cols - STEP, 1)], axis=0)
        turned = jnp.transpose(both).reshape(peers, 2, STEP, 2 * channels)[:, 0]
        send_ref[pl.ds(first, peers), r] = turned.astype(jnp.bfloat16)

    def step(r, _):
        mine = out_ref[r + half * core].astype(jnp.float32)
        place_cells(mine, r, peers * core)
        value = (
            near_other[r].astype(jnp.float32)
            + conv_other[r].astype(jnp.float32) * factor
            + offset
        )
        other = elu(value).astype(jnp.bfloat16).astype(jnp.float32)
        place_cells(other, r, peers * (1 - core))
        return 0

    lax.fori_loop(0, half, step, 0)


def merge_kernel(place, own, received, other, out_ref, cells_ref):
    core = place[1]
    rows, channels, cols = own.shape
    peers, half = other.shape[0], other.shape[1]

    def gather(s, _):
        mine = received[peers * core + s].astype(jnp.float32)
        cells_ref[s, core] = mine
        cells_ref[s, 1 - core] = other[s].astype(jnp.float32)
        return 0

    lax.fori_loop(0, peers, gather, 0)
    flat = cells_ref.reshape(cols * STEP, 2 * channels)
    for low in range(STEP):
        mirrored = jnp.transpose(flat[pl.ds(low, cols, stride=STEP), :])
        for high in range(rows // STEP):
            r = high * STEP + low
            value = own[r].astype(jnp.float32) + mirrored[channels * high : channels * (high + 1)]
            out_ref[r] = (0.5 * value).astype(jnp.bfloat16)


def body(residue_feats, pair_feats, w_row, w_col, first_taps, second_taps, norm_scale, norm_shift):
    channels, rows, cols = pair_feats.shape
    cores = lax.axis_size("gy")
    devices = lax.axis_size(GX)
    core = lax.axis_index("gy")
    place = jnp.stack([lax.axis_index(GX), core]).astype(jnp.int32)
    first_core = core == 0
    cells = devices * rows * cores * cols
    half = rows // 2
    bf16, f32 = jnp.bfloat16, jnp.float32
    shape = jax.ShapeDtypeStruct
    conv_flops = 2 * 9 * channels * channels * rows * cols

    def arranged(taps):
        return taps.reshape(3, 3, channels, channels).transpose(1, 2, 0, 3).reshape(
            3 * channels, 3 * channels
        )

    first_weights, second_weights = arranged(first_taps), arranged(second_taps)

    own_terms = jnp.dot(
        residue_feats, jnp.concatenate([w_row, w_col], axis=1), preferred_element_type=f32
    ).astype(bf16)
    terms = lax.all_to_all(
        jnp.broadcast_to(own_terms[None], (devices, *own_terms.shape)), GX, 0, 0, tiled=True
    ).reshape(devices * rows, 2 * channels)

    raw = jnp.transpose(pair_feats, (1, 0, 2))
    top, bottom = raw[:STEP], raw[STEP:]
    down = functools.partial(lax.ppermute, axis_name=GX, perm=chain(devices, 1))
    up = functools.partial(lax.ppermute, axis_name=GX, perm=chain(devices, -1))
    above_near, below_near = down(bottom), up(top)
    edge = jnp.where(first_core, raw[:, :, cols - STEP :], raw[:, :, :STEP])

    def widened(side):
        pad = LANES - STEP
        return jnp.where(
            first_core,
            jnp.pad(side, ((0, 0), (0, 0), (0, pad))),
            jnp.pad(side, ((0, 0), (0, 0), (pad, 0))),
        )

    side = widened(lax.ppermute(edge, "gy", SWAP))
    side_above = widened(lax.ppermute(edge, ALL, cross_chain(devices, 1)))
    side_below = widened(lax.ppermute(edge, ALL, cross_chain(devices, -1)))
    above_far, below_far = down(top), up(bottom)

    wide = cols + LANES
    near, conv_own, edge_own, stats = call(
        functools.partial(first_kernel, devices),
        (
            shape((rows + 2 * STEP, channels, wide), bf16),
            shape((rows, channels, cols), f32),
            shape((rows, channels, LANES), f32),
            shape((devices, LANES), f32),
        ),
        [],
        conv_flops,
        (place, raw, above_near, below_near, side, side_above, side_below, terms, first_weights),
    )

    def everywhere(sums):
        sums = lax.all_to_all(sums, GX, 0, 0, tiled=True)
        return sums, lax.ppermute(sums, "gy", SWAP)

    stats = everywhere(stats)
    conv_far, edge_far = call(
        functools.partial(far_kernel, devices),
        (
            shape((2 * STEP, channels, cols), f32),
            shape((2 * STEP, channels, LANES), f32),
        ),
        [pltpu.VMEM((6 * STEP, channels, wide), bf16)],
        conv_flops,
        (place, near, above_far, below_far, side_above, side_below, terms, first_weights),
    )
    edge_own, edge_far = lax.ppermute(edge_own, "gy", SWAP), lax.ppermute(edge_far, "gy", SWAP)
    near_rows = near[STEP : STEP + rows, :, :cols]
    near_other = lax.ppermute(
        jnp.where(first_core, near_rows[half:], near_rows[:half]), "gy", SWAP
    )
    gains, shifts = norm_scale[:, :, None], norm_shift[:, :, None]
    conv_second, swap, stats = call(
        functools.partial(second_kernel, devices, cells),
        (
            shape((rows, channels, cols), f32),
            shape((half, channels, cols), bf16),
            shape((devices, LANES), f32),
        ),
        [pltpu.VMEM((rows + 2 * STEP, channels, wide), bf16)],
        conv_flops,
        (place, conv_own, conv_far, edge_own, edge_far, *stats, gains[0], shifts[0],
         second_weights),
    )
    stats = everywhere(stats)
    conv_other = lax.ppermute(swap, "gy", SWAP)
    block_out, send = call(
        functools.partial(pack_kernel, cells),
        (
            shape((rows, channels, cols), bf16),
            shape((devices, half, STEP, 2 * channels), bf16),
        ),
        [],
        conv_flops,
        (place, near, near_other, conv_second, conv_other, *stats, gains[1], shifts[1]),
    )
    received = lax.all_to_all(send, GX, 0, 0, tiled=True)
    peers = devices // cores
    give = jnp.where(first_core, received[peers:], received[:peers])
    other = lax.ppermute(give, "gy", SWAP)
    out = call(
        merge_kernel,
        shape((rows, channels, cols), bf16),
        [pltpu.VMEM((peers, cores, half, STEP, 2 * channels), f32)],
        conv_flops,
        (place, block_out, received, other),
    )
    return jnp.transpose(out, (1, 0, 2))


def solution(mesh):
    torus = Mesh(
        mesh.devices.reshape(mesh.shape["grp"], 4, 16, mesh.shape["gy"]),
        ("grp", "gx_0", "gx_1", "gy"),
    )
    placed = (P(GRP_GX, None), P(None, GRP_GX, "gy"), P(), P(), P(), P(), P(), P())
    return jax.shard_map(
        body, mesh=torus, in_specs=placed, out_specs=P(None, GRP_GX, "gy"), check_vma=False
    )
```

```python
import functools

import jax
import jax.numpy as jnp
from jax import lax
from jax.experimental import pallas as pl
from jax.experimental.pallas import tpu as pltpu
from jax.sharding import Mesh
from jax.sharding import PartitionSpec as P

STEP = 8
GX = ("gx_0", "gx_1")
GRP_GX = ("grp", "gx_0", "gx_1")
LANES = 128
SWAP = [(0, 1), (1, 0)]
VMEM = pl.BlockSpec(memory_space=pltpu.VMEM)

epsilon = 1e-05


def chain(count, step):
    pairs = [(i, i + 1) for i in range(count - 1)]
    return pairs if step > 0 else [(b, a) for a, b in pairs]


def call(kernel, out_shape, scratch, flops, operands):
    held = [pltpu.with_memory_space_constraint(x, pltpu.VMEM) for x in operands]
    return pl.pallas_call(
        kernel,
        out_shape=jax.tree.map(lambda s: pltpu.VMEM(s.shape, s.dtype), out_shape),
        in_specs=[VMEM] * len(operands),
        out_specs=jax.tree.map(lambda _: VMEM, out_shape),
        scratch_shapes=scratch,
        cost_estimate=pl.CostEstimate(flops=flops, bytes_accessed=1 << 20, transcendentals=0),
        compiler_params=pltpu.CompilerParams(vmem_limit_bytes=16 << 20),
    )(*held)


def elu(v):
    return jnp.where(v > 0, v, jnp.exp(jnp.minimum(v, 0.0)) - 1.0)


def as_float(flag):
    return jnp.asarray(flag, jnp.int32).astype(jnp.float32)


def above_valid(row_at):
    return jnp.minimum(row_at, 1)


def below_valid(row_at, devices):
    return jnp.minimum(devices - 1 - row_at, 1)


def side_mask(core, channels, valid=1):
    lane = lax.broadcasted_iota(jnp.int32, (channels, LANES), 1)
    first = (LANES - STEP) * core
    return (lane >= first) & (lane < first + STEP * valid)


def edge_of(value, core):
    return jnp.where(core == 0, value[..., value.shape[-1] - LANES :], value[..., :LANES])


def term_rows(terms_ref, start, count):
    rows = terms_ref[pl.ds(pl.multiple_of(start, 16), count), :]
    return jnp.transpose(rows.astype(jnp.float32))


def column_of(row):
    return jnp.transpose(jnp.broadcast_to(row, (LANES, LANES)))[:, 0:1]


def arranged(taps_ref):
    return jnp.concatenate(
        [jnp.concatenate([taps_ref[3 * ky + kx] for ky in range(3)], axis=1) for kx in range(3)],
        axis=0,
    )


def flat_of(channels, rows, cols):
    return pltpu.VMEM((cols // LANES, channels * rows, LANES), jnp.float32)


def widen(source_ref, flat_ref):
    channels, rows, cols = source_ref.shape
    some = 64 // rows if channels % (64 // rows) == 0 else 1

    def step(i, _):
        for block in range(cols // LANES):
            value = source_ref[pl.ds(i * some, some), :, block * LANES : (block + 1) * LANES]
            flat_ref[block, pl.ds(pl.multiple_of(i * some * rows, 8), some * rows), :] = (
                value.astype(jnp.float32).reshape(some * rows, LANES)
            )
        return 0

    lax.fori_loop(0, channels // some, step, 0)


def conv_row(x_ref, row, weights):
    stacked = jnp.concatenate([x_ref[row], x_ref[row + STEP], x_ref[row + 2 * STEP]], axis=0)
    taps = jnp.dot(weights, stacked, preferred_element_type=jnp.float32)
    channels, cols = taps.shape[0] // 3, taps.shape[1]
    total = (
        pltpu.roll(taps[:channels], STEP, 1)
        + taps[channels : 2 * channels]
        + pltpu.roll(taps[2 * channels :], cols - STEP, 1)
    )
    return total[:, : cols - LANES]


def folded(value):
    return sum(value[:, i : i + LANES] for i in range(0, value.shape[1], LANES))


def conv_rows(x_ref, weights, rows, store):
    channels = x_ref.shape[1]

    def step(r, carry):
        total, squares = carry
        out = conv_row(x_ref, r, weights)
        store(r, out)
        return total + folded(out), squares + folded(out * out)

    zero = jnp.zeros((channels, LANES), jnp.float32)
    total, squares = lax.fori_loop(0, rows, step, (zero, zero))
    both = jnp.concatenate(
        [jnp.sum(total, axis=1, keepdims=True), jnp.sum(squares, axis=1, keepdims=True)], axis=0
    )
    return jnp.transpose(jnp.broadcast_to(both, (LANES, LANES)))[0:1]


def affine_of(which, stats_refs, gains_ref, cells):
    column = column_of(sum(jnp.sum(ref[...], axis=0, keepdims=True) for ref in stats_refs)) / cells
    gain_shift = column_of(gains_ref[which : which + 1])
    channels = LANES // 2
    average = column[:channels]
    spread = column[channels:] - average * average
    factor = gain_shift[:channels] * lax.rsqrt(spread + epsilon)
    return factor, gain_shift[channels:] - average * factor


def fill_block_in(
    x_ref, to, source, first, count, side_source, side_first, row_terms, skip, col_terms,
    side_terms, valid, core,
):
    cols = col_terms.shape[1]
    channels = col_terms.shape[0]
    mask, inside = side_mask(core, channels, valid), as_float(valid)
    flat, rows = source
    side_flat, side_rows = side_source
    for r in range(count):
        row = jnp.broadcast_to(row_terms[:, skip + r : skip + r + 1], (channels, LANES))
        for block in range(cols // LANES):
            at = slice(block * LANES, (block + 1) * LANES)
            main = flat[block, pl.ds(first + r, channels, stride=rows), :] + row + col_terms[:, at]
            x_ref[to + r, :, at] = (main * inside).astype(jnp.bfloat16)
        beyond = side_flat[0, pl.ds(side_first + r, channels, stride=side_rows), :]
        beyond = beyond + row + side_terms
        x_ref[to + r, :, cols:] = jnp.where(mask, beyond, 0.0).astype(jnp.bfloat16)


def first_kernel(
    devices, own, above, below, side, terms, taps,
    x_ref, conv_ref, edge_ref, give_ref, stats_ref, own_flat, above_flat, below_flat, side_flat,
):
    row_at, core = lax.axis_index(GX), lax.axis_index("gy")
    channels, rows, cols = own.shape
    half = rows // 2
    for ref, flat in ((own, own_flat), (above, above_flat), (below, below_flat), (side, side_flat)):
        widen(ref, flat)
    col_terms = term_rows(terms, core * cols, cols)[channels:]
    side_terms = term_rows(terms, jnp.where(core == 0, cols, cols - LANES), LANES)[channels:]

    def fill(to, flat, flat_rows, count, side_first, at, skip, valid):
        row_terms = term_rows(terms, at * rows, rows)[:channels]
        fill_block_in(
            x_ref, to, (flat, flat_rows), 0, count, (side_flat, rows + 2 * STEP), side_first,
            row_terms, skip, col_terms, side_terms, valid, core,
        )

    up, down = jnp.maximum(row_at - 1, 0), jnp.minimum(row_at + 1, devices - 1)
    fill(0, above_flat, STEP, STEP, 0, up, rows - STEP, above_valid(row_at))
    fill(STEP, own_flat, rows, rows, STEP, row_at, 0, 1)
    fill(STEP + rows, below_flat, STEP, STEP, STEP + rows, down, 0, below_valid(row_at, devices))

    def store(r, out):
        conv_ref[r] = out.astype(jnp.bfloat16)
        edge_ref[r] = edge_of(out, core).astype(jnp.bfloat16)

    stats = conv_rows(x_ref, arranged(taps), rows, store)
    stats_ref[...] = jnp.broadcast_to(stats, stats_ref.shape)
    give_ref[...] = x_ref[pl.ds(STEP + half * (1 - core), half), :, :cols]


def far_kernel(
    devices, near, edge_own, above, below, side, terms, taps,
    conv_ref, edge_ref, x_ref, above_flat, below_flat, side_flat,
):
    row_at, core = lax.axis_index(GX), lax.axis_index("gy")
    channels, _, cols = above.shape
    rows = near.shape[0] - 2 * STEP
    for ref, flat in ((above, above_flat), (below, below_flat), (side, side_flat)):
        widen(ref, flat)
    col_terms = term_rows(terms, core * cols, cols)[channels:]
    side_terms = term_rows(terms, jnp.where(core == 0, cols, cols - LANES), LANES)[channels:]

    def fill(to, flat, side_first, at, skip, valid):
        row_terms = term_rows(terms, at * rows, rows)[:channels]
        fill_block_in(
            x_ref, to, (flat, STEP), 0, STEP, (side_flat, 2 * STEP), side_first,
            row_terms, skip, col_terms, side_terms, valid, core,
        )

    up, down = jnp.maximum(row_at - 1, 0), jnp.minimum(row_at + 1, devices - 1)
    fill(0, above_flat, 0, up, 0, above_valid(row_at))
    fill(5 * STEP, below_flat, STEP, down, rows - STEP, below_valid(row_at, devices))
    x_ref[STEP : 3 * STEP] = near[: 2 * STEP]
    x_ref[3 * STEP : 5 * STEP] = near[rows:]
    w = arranged(taps)

    def step(r, _):
        for half in range(2):
            out = conv_row(x_ref, r + 3 * STEP * half, w)
            conv_ref[r + STEP * half] = out.astype(jnp.bfloat16)
            edge_ref[r + (STEP + rows) * half] = edge_of(out, core).astype(jnp.bfloat16)
        return 0

    lax.fori_loop(0, STEP, step, 0)
    edge_ref[STEP : STEP + rows] = edge_own[...]


def second_kernel(
    devices, cells, own, far, side, stats, stats_other, gains, taps,
    conv_ref, give_ref, stats_ref, a_ref,
):
    row_at, core = lax.axis_index(GX), lax.axis_index("gy")
    rows, channels, cols = own.shape
    half = rows // 2
    factor, offset = affine_of(0, (stats, stats_other), gains, cells)
    factor_side = jnp.broadcast_to(factor, (channels, LANES))
    offset_side = jnp.broadcast_to(offset, (channels, LANES))

    def fill(source, at, to, valid):
        inside = as_float(valid)
        for i in range(0, cols, LANES):
            value = source[at, :, i : i + LANES].astype(jnp.float32)
            value = elu(value * factor_side + offset_side) * inside
            a_ref[to, :, i : i + LANES] = value.astype(jnp.bfloat16)
        beyond = elu(side[to].astype(jnp.float32) * factor_side + offset_side)
        mask = side_mask(core, channels, valid)
        a_ref[to, :, cols:] = jnp.where(mask, beyond, 0.0).astype(jnp.bfloat16)

    def outer(r, _):
        fill(far, r, r, above_valid(row_at))
        fill(far, r + STEP, r + STEP + rows, below_valid(row_at, devices))
        return 0

    def inner(r, _):
        fill(own, r, r + STEP, 1)
        return 0

    lax.fori_loop(0, STEP, outer, 0)
    lax.fori_loop(0, rows, inner, 0)

    def store(r, out):
        conv_ref[r] = out.astype(jnp.bfloat16)

    stats = conv_rows(a_ref, arranged(taps), rows, store)
    stats_ref[...] = jnp.broadcast_to(stats, stats_ref.shape)
    give_ref[...] = conv_ref[pl.ds(half * (1 - core), half)]


def pack_kernel(
    cells, near, near_other, conv, conv_other, stats, stats_other, gains, out_ref, send_ref
):
    core = lax.axis_index("gy")
    rows, channels, cols = conv.shape
    half = rows // 2
    factor, offset = affine_of(1, (stats, stats_other), gains, cells)
    factor = jnp.broadcast_to(factor, (channels, LANES))
    offset = jnp.broadcast_to(offset, (channels, LANES))
    peers = cols // rows

    def block_out(block_in, value):
        value = block_in.astype(jnp.float32) + value.astype(jnp.float32) * factor + offset
        return elu(value).astype(jnp.bfloat16)

    def own(r, _):
        for i in range(0, cols, LANES):
            out_ref[r, :, i : i + LANES] = block_out(
                near[r + STEP, :, i : i + LANES], conv[r, :, i : i + LANES]
            )
        return 0

    lax.fori_loop(0, rows, own, 0)
    some = LANES // rows

    def place_cells(value, r, first):
        value = value.astype(jnp.float32)
        both = jnp.concatenate([value, pltpu.roll(value, LANES - STEP, 1)], axis=0)
        turned = jnp.transpose(both).reshape(some, 2, STEP, 2 * channels)[:, 0]
        send_ref[pl.ds(first, some), r] = turned.astype(jnp.bfloat16)

    def step(r, _):
        for i in range(0, cols, LANES):
            at = i // rows
            place_cells(out_ref[r + half * core, :, i : i + LANES], r, peers * core + at)
            other = block_out(near_other[r, :, i : i + LANES], conv_other[r, :, i : i + LANES])
            place_cells(other, r, peers * (1 - core) + at)
        return 0

    lax.fori_loop(0, half, step, 0)


def merge_kernel(own, received, other, out_ref, cells_ref, flat_ref):
    core = lax.axis_index("gy")
    rows, channels, cols = own.shape
    peers = other.shape[0]

    def gather(s, _):
        cells_ref[s, core] = received[peers * core + s].astype(jnp.float32)
        cells_ref[s, 1 - core] = other[s].astype(jnp.float32)
        return 0

    lax.fori_loop(0, peers, gather, 0)
    flat = cells_ref.reshape(cols * STEP, 2 * channels)
    for low in range(STEP):
        mirrored = jnp.transpose(flat[pl.ds(low, cols, stride=STEP), :])
        for high in range(rows // STEP):
            r = high * STEP + low
            value = own[r].astype(jnp.float32) + mirrored[channels * high : channels * (high + 1)]
            for block in range(cols // LANES):
                flat_ref[block, pl.ds(r, channels, stride=rows), :] = (
                    0.5 * value[:, block * LANES : (block + 1) * LANES]
                )

    def store(c, _):
        for block in range(cols // LANES):
            value = flat_ref[block, pl.ds(pl.multiple_of(c * rows, 8), rows), :]
            out_ref[c, :, block * LANES : (block + 1) * LANES] = value.astype(jnp.bfloat16)
        return 0

    lax.fori_loop(0, channels, store, 0)


def body(residue_feats, pair_feats, w_row, w_col, first_taps, second_taps, norm_scale, norm_shift):
    channels, rows, cols = pair_feats.shape
    cores = lax.axis_size("gy")
    devices = lax.axis_size(GX)
    first_core = lax.axis_index("gy") == 0
    cells = devices * rows * cores * cols
    half = rows // 2
    bf16, f32 = jnp.bfloat16, jnp.float32
    shape = jax.ShapeDtypeStruct
    conv_flops = 2 * 9 * channels * channels * rows * cols

    def edge(x):
        return jnp.where(first_core, x[..., cols - LANES :], x[..., :LANES])

    def swap(x):
        return lax.ppermute(x, "gy", SWAP)

    down = functools.partial(lax.ppermute, axis_name=GX, perm=chain(devices, 1))
    up = functools.partial(lax.ppermute, axis_name=GX, perm=chain(devices, -1))
    top, bottom = pair_feats[:, :STEP], pair_feats[:, STEP:]
    above_near, below_near = down(bottom), up(top)
    above_far, below_far = down(top), up(bottom)
    own_terms = jnp.dot(
        residue_feats, jnp.concatenate([w_row, w_col], axis=1), preferred_element_type=f32
    ).astype(bf16)
    terms = lax.all_to_all(
        jnp.broadcast_to(own_terms[None], (devices, *own_terms.shape)), GX, 0, 0, tiled=True
    )
    terms = terms.reshape(devices * rows, 2 * channels)
    gains = jnp.concatenate([norm_scale, norm_shift], axis=1)

    near_side = swap(
        jnp.concatenate([edge(above_near), edge(pair_feats), edge(below_near)], axis=1)
    )
    far_side = swap(jnp.concatenate([edge(above_far), edge(below_far)], axis=1))

    wide = cols + LANES
    near, conv_own, edge_own, near_give, stats = call(
        functools.partial(first_kernel, devices),
        (
            shape((rows + 2 * STEP, channels, wide), bf16),
            shape((rows, channels, cols), bf16),
            shape((rows, channels, LANES), bf16),
            shape((half, channels, cols), bf16),
            shape((devices, LANES), f32),
        ),
        [
            flat_of(channels, rows, cols),
            flat_of(channels, STEP, cols),
            flat_of(channels, STEP, cols),
            flat_of(channels, rows + 2 * STEP, LANES),
        ],
        conv_flops,
        (pair_feats, above_near, below_near, near_side, terms, first_taps),
    )
    stats = lax.all_to_all(stats, GX, 0, 0, tiled=True)
    stats_other = swap(stats)
    conv_far, edges = call(
        functools.partial(far_kernel, devices),
        (shape((2 * STEP, channels, cols), bf16), shape((rows + 2 * STEP, channels, LANES), bf16)),
        [
            pltpu.VMEM((6 * STEP, channels, wide), bf16),
            flat_of(channels, STEP, cols),
            flat_of(channels, STEP, cols),
            flat_of(channels, 2 * STEP, LANES),
        ],
        conv_flops,
        (near, edge_own, above_far, below_far, far_side, terms, first_taps),
    )
    edges = swap(edges)
    near_other = swap(near_give)
    conv_second, second_give, stats = call(
        functools.partial(second_kernel, devices, cells),
        (
            shape((rows, channels, cols), bf16),
            shape((half, channels, cols), bf16),
            shape((devices, LANES), f32),
        ),
        [pltpu.VMEM((rows + 2 * STEP, channels, wide), bf16)],
        conv_flops,
        (conv_own, conv_far, edges, stats, stats_other, gains, second_taps),
    )
    stats = lax.all_to_all(stats, GX, 0, 0, tiled=True)
    stats_other = swap(stats)
    conv_other = swap(second_give)
    block_out, send = call(
        functools.partial(pack_kernel, cells),
        (
            shape((rows, channels, cols), bf16),
            shape((devices, half, STEP, 2 * channels), bf16),
        ),
        [],
        conv_flops,
        (near, near_other, conv_second, conv_other, stats, stats_other, gains),
    )
    received = lax.all_to_all(send, GX, 0, 0, tiled=True)
    peers = devices // cores
    other = swap(jnp.where(first_core, received[peers:], received[:peers]))
    return call(
        merge_kernel,
        shape((channels, rows, cols), bf16),
        [pltpu.VMEM((peers, cores, half, STEP, 2 * channels), f32), flat_of(channels, rows, cols)],
        conv_flops,
        (block_out, received, other),
    )


def solution(mesh):
    torus = Mesh(
        mesh.devices.reshape(mesh.shape["grp"], 4, 16, mesh.shape["gy"]),
        ("grp", "gx_0", "gx_1", "gy"),
    )
    placed = (P(GRP_GX, None), P(None, GRP_GX, "gy"), P(), P(), P(), P(), P(), P())
    return jax.shard_map(
        body, mesh=torus, in_specs=placed, out_specs=P(None, GRP_GX, "gy"), check_vma=False
    )
```

```python
import functools

import jax
import jax.numpy as jnp
from jax import lax
from jax.experimental import pallas as pl
from jax.experimental.pallas import tpu as pltpu
from jax.sharding import Mesh
from jax.sharding import PartitionSpec as P

STEP = 8
GX = ("gx_0", "gx_1")
GRP_GX = ("grp", "gx_0", "gx_1")
LANES = 128
SWAP = [(0, 1), (1, 0)]
HBM, VMEM = pltpu.HBM, pltpu.VMEM

epsilon = 1e-05


def chain(count, step):
    pairs = [(i, i + 1) for i in range(count - 1)]
    return pairs if step > 0 else [(b, a) for a, b in pairs]


def call(kernel, outs, scratch, n_copies, flops, operands):
    spaces = [space for space, _ in operands]
    held = [pltpu.with_memory_space_constraint(x, space) for space, x in operands]
    return pl.pallas_call(
        kernel,
        out_shape=[space(shape, dtype) for space, shape, dtype in outs],
        in_specs=[pl.BlockSpec(memory_space=space) for space in spaces],
        out_specs=[pl.BlockSpec(memory_space=space) for space, _, _ in outs],
        scratch_shapes=[*scratch, pltpu.SemaphoreType.DMA((n_copies,))],
        cost_estimate=pl.CostEstimate(flops=flops, bytes_accessed=1 << 20, transcendentals=0),
        compiler_params=pltpu.CompilerParams(vmem_limit_bytes=24 << 20),
    )(*held)


def start_all(sem, first, pairs):
    copies = [
        pltpu.make_async_copy(src, dst, sem.at[first + i]) for i, (src, dst) in enumerate(pairs)
    ]
    for copy in copies:
        copy.start()
    return copies


def wait_all(copies):
    for copy in copies:
        copy.wait()


def elu(v):
    return jnp.where(v > 0, v, jnp.exp(jnp.minimum(v, 0.0)) - 1.0)


def as_float(flag):
    return jnp.asarray(flag, jnp.int32).astype(jnp.float32)


def above_valid(row_at):
    return jnp.minimum(row_at, 1)


def below_valid(row_at, devices):
    return jnp.minimum(devices - 1 - row_at, 1)


def side_mask(core, channels, valid=1):
    lane = lax.broadcasted_iota(jnp.int32, (channels, LANES), 1)
    first = (LANES - STEP) * core
    return (lane >= first) & (lane < first + STEP * valid)


def edge_of(value, core):
    return jnp.where(core == 0, value[..., value.shape[-1] - LANES :], value[..., :LANES])


def term_rows(terms_ref, start, count):
    rows = terms_ref[pl.ds(pl.multiple_of(start, 16), count), :]
    return jnp.transpose(rows.astype(jnp.float32))


def column_of(row):
    return jnp.transpose(jnp.broadcast_to(row, (LANES, LANES)))[:, 0:1]


def arranged(taps_ref):
    return jnp.concatenate(
        [jnp.concatenate([taps_ref[3 * ky + kx] for ky in range(3)], axis=1) for kx in range(3)],
        axis=0,
    )


def flat_of(channels, rows, cols):
    return pltpu.VMEM((cols // LANES, channels * rows, LANES), jnp.float32)


def widen(source_ref, flat_ref):
    channels, rows, cols = source_ref.shape
    some = 64 // rows if channels % (64 // rows) == 0 else 1

    def step(i, _):
        for block in range(cols // LANES):
            value = source_ref[pl.ds(i * some, some), :, block * LANES : (block + 1) * LANES]
            flat_ref[block, pl.ds(pl.multiple_of(i * some * rows, 8), some * rows), :] = (
                value.astype(jnp.float32).reshape(some * rows, LANES)
            )
        return 0

    lax.fori_loop(0, channels // some, step, 0)


def conv_row(x_ref, row, weights):
    stacked = jnp.concatenate([x_ref[row], x_ref[row + STEP], x_ref[row + 2 * STEP]], axis=0)
    taps = jnp.dot(weights, stacked, preferred_element_type=jnp.float32)
    channels, cols = taps.shape[0] // 3, taps.shape[1]
    total = (
        pltpu.roll(taps[:channels], STEP, 1)
        + taps[channels : 2 * channels]
        + pltpu.roll(taps[2 * channels :], cols - STEP, 1)
    )
    return total[:, : cols - LANES]


def folded(value):
    return sum(value[:, i : i + LANES] for i in range(0, value.shape[1], LANES))


def conv_rows(x_ref, weights, rows, store):
    channels = x_ref.shape[1]

    def step(r, carry):
        total, squares = carry
        out = conv_row(x_ref, r, weights)
        store(r, out)
        return total + folded(out), squares + folded(out * out)

    zero = jnp.zeros((channels, LANES), jnp.float32)
    total, squares = lax.fori_loop(0, rows, step, (zero, zero))
    both = jnp.concatenate(
        [jnp.sum(total, axis=1, keepdims=True), jnp.sum(squares, axis=1, keepdims=True)], axis=0
    )
    return jnp.transpose(jnp.broadcast_to(both, (LANES, LANES)))[0:1]


def affine_of(which, stats_refs, gains_ref, cells):
    column = column_of(sum(jnp.sum(ref[...], axis=0, keepdims=True) for ref in stats_refs)) / cells
    gain_shift = column_of(gains_ref[which : which + 1])
    channels = LANES // 2
    average = column[:channels]
    spread = column[channels:] - average * average
    factor = gain_shift[:channels] * lax.rsqrt(spread + epsilon)
    return factor, gain_shift[channels:] - average * factor


def fill_block_in(
    x_ref, to, source, first, count, side_source, side_first, row_terms, skip, col_terms,
    side_terms, valid, core,
):
    cols = col_terms.shape[1]
    channels = col_terms.shape[0]
    mask, inside = side_mask(core, channels, valid), as_float(valid)
    flat, rows = source
    side_flat, side_rows = side_source
    for r in range(count):
        row = jnp.broadcast_to(row_terms[:, skip + r : skip + r + 1], (channels, LANES))
        for block in range(cols // LANES):
            at = slice(block * LANES, (block + 1) * LANES)
            main = flat[block, pl.ds(first + r, channels, stride=rows), :] + row + col_terms[:, at]
            x_ref[to + r, :, at] = (main * inside).astype(jnp.bfloat16)
        beyond = side_flat[0, pl.ds(side_first + r, channels, stride=side_rows), :]
        beyond = beyond + row + side_terms
        x_ref[to + r, :, cols:] = jnp.where(mask, beyond, 0.0).astype(jnp.bfloat16)


def prepare_kernel(
    pair, feats, w_row, w_col, top_out, bottom_out, terms_ref, top, bottom, feats_in, row_in,
    col_in, sem,
):
    halves = start_all(sem, 0, ((pair.at[:, :STEP], top), (pair.at[:, STEP:], bottom)))
    inputs = start_all(sem, 2, ((feats, feats_in), (w_row, row_in), (w_col, col_in)))
    wait_all(inputs)
    terms = jnp.concatenate(
        [
            lax.dot_general(
                feats_in[...], w[...], (((1,), (1,)), ((), ())), preferred_element_type=jnp.float32
            )
            for w in (row_in, col_in)
        ],
        axis=1,
    ).astype(jnp.bfloat16)
    terms_ref[...] = jnp.broadcast_to(terms[None], terms_ref.shape)
    wait_all(halves)
    wait_all(start_all(sem, 0, ((top, top_out), (bottom, bottom_out))))


def first_kernel(
    devices, own_in, above_in, below_in, side_in, terms_in, taps_in,
    near_out, conv_out, give_out, stats_ref,
    x_ref, conv_ref, own, above, below, side, terms, taps,
    own_flat, above_flat, below_flat, side_flat, sem,
):
    row_at, core = lax.axis_index(GX), lax.axis_index("gy")
    channels, rows, cols = own.shape
    half = rows // 2
    inputs = start_all(
        sem, 0,
        ((terms_in, terms), (side_in, side), (above_in, above), (own_in, own), (below_in, below),
         (taps_in, taps)),
    )
    inputs[0].wait()
    col_terms = term_rows(terms, core * cols, cols)[channels:]
    side_terms = term_rows(terms, jnp.where(core == 0, cols, cols - LANES), LANES)[channels:]
    inputs[1].wait()
    widen(side, side_flat)

    def fill(copy, ref, to, flat, flat_rows, count, side_first, at, skip, valid):
        row_terms = term_rows(terms, at * rows, rows)[:channels]
        copy.wait()
        widen(ref, flat)
        fill_block_in(
            x_ref, to, (flat, flat_rows), 0, count, (side_flat, rows + 2 * STEP), side_first,
            row_terms, skip, col_terms, side_terms, valid, core,
        )

    up, down = jnp.maximum(row_at - 1, 0), jnp.minimum(row_at + 1, devices - 1)
    fill(inputs[2], above, 0, above_flat, STEP, STEP, 0, up, rows - STEP, above_valid(row_at))
    fill(inputs[3], own, STEP, own_flat, rows, rows, STEP, row_at, 0, 1)
    fill(inputs[4], below, STEP + rows, below_flat, STEP, STEP, STEP + rows, down, 0,
         below_valid(row_at, devices))
    given = x_ref.at[pl.ds(STEP + half * (1 - core), half), :, pl.ds(0, cols)]
    outputs = start_all(sem, 6, ((x_ref, near_out), (given, give_out)))
    inputs[5].wait()

    def store(r, out):
        conv_ref[r] = out.astype(jnp.bfloat16)

    stats = conv_rows(x_ref, arranged(taps), rows, store)
    outputs += start_all(sem, 8, ((conv_ref, conv_out),))
    stats_ref[...] = jnp.broadcast_to(stats, stats_ref.shape)
    wait_all(outputs)


def far_kernel(
    devices, near_in, own_in, above_in, below_in, side_in, terms_in, taps_in,
    conv_out, edge_out,
    x_ref, conv_ref, edge_ref, above, below, side, terms, taps,
    above_flat, below_flat, side_flat, sem,
):
    row_at, core = lax.axis_index(GX), lax.axis_index("gy")
    channels, _, cols = above.shape
    rows = own_in.shape[0]
    edge_at = pl.multiple_of((cols - LANES) * (1 - core), LANES)
    inputs = start_all(
        sem, 0,
        ((terms_in, terms), (side_in, side), (above_in, above), (below_in, below),
         (near_in.at[pl.ds(0, 2 * STEP)], x_ref.at[pl.ds(STEP, 2 * STEP)]),
         (near_in.at[pl.ds(rows, 2 * STEP)], x_ref.at[pl.ds(3 * STEP, 2 * STEP)]),
         (own_in.at[:, :, pl.ds(edge_at, LANES)], edge_ref.at[pl.ds(STEP, rows)]),
         (taps_in, taps)),
    )
    inputs[0].wait()
    col_terms = term_rows(terms, core * cols, cols)[channels:]
    side_terms = term_rows(terms, jnp.where(core == 0, cols, cols - LANES), LANES)[channels:]
    inputs[1].wait()
    widen(side, side_flat)

    def fill(copy, ref, to, flat, side_first, at, skip, valid):
        row_terms = term_rows(terms, at * rows, rows)[:channels]
        copy.wait()
        widen(ref, flat)
        fill_block_in(
            x_ref, to, (flat, STEP), 0, STEP, (side_flat, 2 * STEP), side_first,
            row_terms, skip, col_terms, side_terms, valid, core,
        )

    up, down = jnp.maximum(row_at - 1, 0), jnp.minimum(row_at + 1, devices - 1)
    fill(inputs[2], above, 0, above_flat, 0, up, 0, above_valid(row_at))
    fill(inputs[3], below, 5 * STEP, below_flat, STEP, down, rows - STEP,
         below_valid(row_at, devices))
    wait_all(inputs[4:])
    w = arranged(taps)

    def step(r, _):
        for half in range(2):
            out = conv_row(x_ref, r + 3 * STEP * half, w)
            conv_ref[r + STEP * half] = out.astype(jnp.bfloat16)
            edge_ref[r + (STEP + rows) * half] = edge_of(out, core).astype(jnp.bfloat16)
        return 0

    lax.fori_loop(0, STEP, step, 0)
    wait_all(start_all(sem, 0, ((edge_ref, edge_out), (conv_ref, conv_out))))


def second_kernel(
    devices, cells, own_in, far_in, side_in, stats, stats_other, gains, taps_in,
    conv_out, give_out, stats_ref,
    a_ref, conv_ref, own, far, side, taps, sem,
):
    row_at, core = lax.axis_index(GX), lax.axis_index("gy")
    rows, channels, cols = own.shape
    half = rows // 2
    inputs = start_all(
        sem, 0, ((side_in, side), (far_in, far), (own_in, own), (taps_in, taps))
    )
    factor, offset = affine_of(0, (stats, stats_other), gains, cells)
    factor_side = jnp.broadcast_to(factor, (channels, LANES))
    offset_side = jnp.broadcast_to(offset, (channels, LANES))

    def fill(source, at, to, valid):
        inside = as_float(valid)
        for i in range(0, cols, LANES):
            value = source[at, :, i : i + LANES].astype(jnp.float32)
            value = elu(value * factor_side + offset_side) * inside
            a_ref[to, :, i : i + LANES] = value.astype(jnp.bfloat16)
        beyond = elu(side[to].astype(jnp.float32) * factor_side + offset_side)
        mask = side_mask(core, channels, valid)
        a_ref[to, :, cols:] = jnp.where(mask, beyond, 0.0).astype(jnp.bfloat16)

    def outer(r, _):
        fill(far, r, r, above_valid(row_at))
        fill(far, r + STEP, r + STEP + rows, below_valid(row_at, devices))
        return 0

    def inner(r, _):
        fill(own, r, r + STEP, 1)
        return 0

    wait_all(inputs[:2])
    lax.fori_loop(0, STEP, outer, 0)
    wait_all(inputs[2:])
    lax.fori_loop(0, rows, inner, 0)

    def store(r, out):
        conv_ref[r] = out.astype(jnp.bfloat16)

    stats = conv_rows(a_ref, arranged(taps), rows, store)
    given = conv_ref.at[pl.ds(half * (1 - core), half)]
    outputs = start_all(sem, 0, ((given, give_out), (conv_ref, conv_out)))
    stats_ref[...] = jnp.broadcast_to(stats, stats_ref.shape)
    wait_all(outputs)


def pack_kernel(
    cells, near_in, near_other_in, conv_in, conv_other_in, stats, stats_other, gains,
    block_out_out, send_ref,
    out_ref, near, near_other, conv, conv_other, sem,
):
    core = lax.axis_index("gy")
    rows, channels, cols = conv.shape
    half = rows // 2
    inputs = start_all(
        sem, 0,
        ((near_in.at[pl.ds(STEP, rows), :, pl.ds(0, cols)], near), (conv_in, conv),
         (near_other_in, near_other), (conv_other_in, conv_other)),
    )
    factor, offset = affine_of(1, (stats, stats_other), gains, cells)
    factor = jnp.broadcast_to(factor, (channels, LANES))
    offset = jnp.broadcast_to(offset, (channels, LANES))
    peers = cols // rows

    def block_out(block_in, value):
        value = block_in.astype(jnp.float32) + value.astype(jnp.float32) * factor + offset
        return elu(value).astype(jnp.bfloat16)

    def own(r, _):
        for i in range(0, cols, LANES):
            out_ref[r, :, i : i + LANES] = block_out(
                near[r, :, i : i + LANES], conv[r, :, i : i + LANES]
            )
        return 0

    wait_all(inputs[:2])
    lax.fori_loop(0, rows, own, 0)
    outputs = start_all(sem, 4, ((out_ref, block_out_out),))
    some = LANES // rows

    def place_cells(value, r, first):
        value = value.astype(jnp.float32)
        both = jnp.concatenate([value, pltpu.roll(value, LANES - STEP, 1)], axis=0)
        turned = jnp.transpose(both).reshape(some, 2, STEP, 2 * channels)[:, 0]
        send_ref[pl.ds(first, some), r] = turned.astype(jnp.bfloat16)

    def step(r, _):
        for i in range(0, cols, LANES):
            at = i // rows
            place_cells(out_ref[r + half * core, :, i : i + LANES], r, peers * core + at)
            other = block_out(near_other[r, :, i : i + LANES], conv_other[r, :, i : i + LANES])
            place_cells(other, r, peers * (1 - core) + at)
        return 0

    wait_all(inputs[2:])
    lax.fori_loop(0, half, step, 0)
    wait_all(outputs)


def merge_kernel(own_in, received, other, result, out_ref, own, cells_ref, flat_ref, sem):
    core = lax.axis_index("gy")
    rows, channels, cols = own.shape
    peers = other.shape[0]
    inputs = start_all(sem, 0, ((own_in, own),))

    def gather(s, _):
        cells_ref[s, core] = received[peers * core + s].astype(jnp.float32)
        cells_ref[s, 1 - core] = other[s].astype(jnp.float32)
        return 0

    lax.fori_loop(0, peers, gather, 0)
    wait_all(inputs)
    flat = cells_ref.reshape(cols * STEP, 2 * channels)
    for low in range(STEP):
        mirrored = jnp.transpose(flat[pl.ds(low, cols, stride=STEP), :])
        for high in range(rows // STEP):
            r = high * STEP + low
            value = own[r].astype(jnp.float32) + mirrored[channels * high : channels * (high + 1)]
            for block in range(cols // LANES):
                flat_ref[block, pl.ds(r, channels, stride=rows), :] = (
                    0.5 * value[:, block * LANES : (block + 1) * LANES]
                )

    def store(c, _):
        for block in range(cols // LANES):
            value = flat_ref[block, pl.ds(pl.multiple_of(c * rows, 8), rows), :]
            out_ref[c, :, block * LANES : (block + 1) * LANES] = value.astype(jnp.bfloat16)
        return 0

    part = channels // 2
    lax.fori_loop(0, part, store, 0)
    outputs = start_all(sem, 1, ((out_ref.at[pl.ds(0, part)], result.at[pl.ds(0, part)]),))
    lax.fori_loop(part, channels, store, 0)
    outputs += start_all(sem, 2, ((out_ref.at[pl.ds(part, part)], result.at[pl.ds(part, part)]),))
    wait_all(outputs)


def body(residue_feats, pair_feats, w_row, w_col, first_taps, second_taps, norm_scale, norm_shift):
    channels, rows, cols = pair_feats.shape
    cores = lax.axis_size("gy")
    devices = lax.axis_size(GX)
    first_core = lax.axis_index("gy") == 0
    cells = devices * rows * cores * cols
    half = rows // 2
    bf16, f32 = jnp.bfloat16, jnp.float32
    conv_flops = 2 * 9 * channels * channels * rows * cols
    wide = cols + LANES

    def edge(x):
        return jnp.where(first_core, x[..., cols - LANES :], x[..., :LANES])

    def swap(x):
        return lax.ppermute(x, "gy", SWAP)

    down = functools.partial(lax.ppermute, axis_name=GX, perm=chain(devices, 1))
    up = functools.partial(lax.ppermute, axis_name=GX, perm=chain(devices, -1))
    eight = (channels, STEP, cols)
    top, bottom, terms = call(
        prepare_kernel,
        (
            (HBM, eight, bf16),
            (HBM, eight, bf16),
            (VMEM, (devices, rows, 2 * channels), bf16),
        ),
        [
            VMEM(eight, bf16),
            VMEM(eight, bf16),
            VMEM(residue_feats.shape, bf16),
            VMEM(w_row.T.shape, bf16),
            VMEM(w_col.T.shape, bf16),
        ],
        5,
        conv_flops // 16,
        ((HBM, pair_feats), (HBM, residue_feats), (HBM, w_row.T), (HBM, w_col.T)),
    )
    above_near, below_near = down(bottom), up(top)
    above_far, below_far = down(top), up(bottom)
    terms = lax.all_to_all(terms, GX, 0, 0, tiled=True)
    terms = terms.reshape(devices * rows, 2 * channels)
    gains = jnp.concatenate([norm_scale, norm_shift], axis=1)

    near_side = swap(
        jnp.concatenate([edge(above_near), edge(pair_feats), edge(below_near)], axis=1)
    )
    far_side = swap(jnp.concatenate([edge(above_far), edge(below_far)], axis=1))

    taps_shape = VMEM(first_taps.shape, bf16)
    terms_shape = VMEM(terms.shape, bf16)
    whole = (rows, channels, cols)
    part = (half, channels, cols)
    sums = (devices, LANES)
    near, conv_own, near_give, stats = call(
        functools.partial(first_kernel, devices),
        (
            (HBM, (rows + 2 * STEP, channels, wide), bf16),
            (HBM, whole, bf16),
            (HBM, part, bf16),
            (VMEM, sums, f32),
        ),
        [
            VMEM((rows + 2 * STEP, channels, wide), bf16),
            VMEM(whole, bf16),
            VMEM(pair_feats.shape, bf16),
            VMEM(eight, bf16),
            VMEM(eight, bf16),
            VMEM(near_side.shape, bf16),
            terms_shape,
            taps_shape,
            flat_of(channels, rows, cols),
            flat_of(channels, STEP, cols),
            flat_of(channels, STEP, cols),
            flat_of(channels, rows + 2 * STEP, LANES),
        ],
        9,
        conv_flops,
        ((HBM, pair_feats), (HBM, above_near), (HBM, below_near), (HBM, near_side),
         (HBM, terms), (HBM, first_taps)),
    )
    stats = lax.all_to_all(stats, GX, 0, 0, tiled=True)
    stats_other = swap(stats)
    conv_far, edges = call(
        functools.partial(far_kernel, devices),
        ((HBM, (2 * STEP, channels, cols), bf16), (HBM, (rows + 2 * STEP, channels, LANES), bf16)),
        [
            VMEM((6 * STEP, channels, wide), bf16),
            VMEM((2 * STEP, channels, cols), bf16),
            VMEM((rows + 2 * STEP, channels, LANES), bf16),
            VMEM(eight, bf16),
            VMEM(eight, bf16),
            VMEM(far_side.shape, bf16),
            terms_shape,
            taps_shape,
            flat_of(channels, STEP, cols),
            flat_of(channels, STEP, cols),
            flat_of(channels, 2 * STEP, LANES),
        ],
        8,
        conv_flops,
        ((HBM, near), (HBM, conv_own), (HBM, above_far), (HBM, below_far), (HBM, far_side),
         (HBM, terms), (HBM, first_taps)),
    )
    edges = swap(edges)
    near_other = swap(near_give)
    conv_second, second_give, stats = call(
        functools.partial(second_kernel, devices, cells),
        ((HBM, whole, bf16), (HBM, part, bf16), (VMEM, sums, f32)),
        [
            VMEM((rows + 2 * STEP, channels, wide), bf16),
            VMEM(whole, bf16),
            VMEM(whole, bf16),
            VMEM((2 * STEP, channels, cols), bf16),
            VMEM(edges.shape, bf16),
            taps_shape,
        ],
        4,
        conv_flops,
        ((HBM, conv_own), (HBM, conv_far), (HBM, edges), (VMEM, stats), (VMEM, stats_other),
         (VMEM, gains), (HBM, second_taps)),
    )
    stats = lax.all_to_all(stats, GX, 0, 0, tiled=True)
    stats_other = swap(stats)
    conv_other = swap(second_give)
    block_out, send = call(
        functools.partial(pack_kernel, cells),
        ((HBM, whole, bf16), (VMEM, (devices, half, STEP, 2 * channels), bf16)),
        [
            VMEM(whole, bf16),
            VMEM(whole, bf16),
            VMEM(part, bf16),
            VMEM(whole, bf16),
            VMEM(part, bf16),
        ],
        5,
        conv_flops,
        ((HBM, near), (HBM, near_other), (HBM, conv_second), (HBM, conv_other),
         (VMEM, stats), (VMEM, stats_other), (VMEM, gains)),
    )
    received = lax.all_to_all(send, GX, 0, 0, tiled=True)
    peers = devices // cores
    other = swap(jnp.where(first_core, received[peers:], received[:peers]))
    return call(
        merge_kernel,
        ((HBM, pair_feats.shape, bf16),),
        [
            VMEM(pair_feats.shape, bf16),
            VMEM(whole, bf16),
            VMEM((peers, cores, half, STEP, 2 * channels), f32),
            flat_of(channels, rows, cols),
        ],
        3,
        conv_flops,
        ((HBM, block_out), (VMEM, received), (VMEM, other)),
    )[0]


def solution(mesh):
    torus = Mesh(
        mesh.devices.reshape(mesh.shape["grp"], 4, 16, mesh.shape["gy"]),
        ("grp", "gx_0", "gx_1", "gy"),
    )
    placed = (P(GRP_GX, None), P(None, GRP_GX, "gy"), P(), P(), P(), P(), P(), P())
    return jax.shard_map(
        body, mesh=torus, in_specs=placed, out_specs=P(None, GRP_GX, "gy"), check_vma=False
    )
```

```python
import functools

import jax
import jax.numpy as jnp
from jax import lax
from jax.experimental import pallas as pl
from jax.experimental.pallas import tpu as pltpu
from jax.sharding import Mesh
from jax.sharding import PartitionSpec as P

STEP = 8
GX = ("gx_0", "gx_1")
GRP_GX = ("grp", "gx_0", "gx_1")
LANES = 128
SWAP = [(0, 1), (1, 0)]
HBM, VMEM = pltpu.HBM, pltpu.VMEM

epsilon = 1e-05


def chain(count, step):
    pairs = [(i, i + 1) for i in range(count - 1)]
    return pairs if step > 0 else [(b, a) for a, b in pairs]


def call(kernel, outs, scratch, n_copies, flops, operands):
    spaces = [space for space, _ in operands]
    held = [pltpu.with_memory_space_constraint(x, space) for space, x in operands]
    return pl.pallas_call(
        kernel,
        out_shape=[space(shape, dtype) for space, shape, dtype in outs],
        in_specs=[pl.BlockSpec(memory_space=space) for space in spaces],
        out_specs=[pl.BlockSpec(memory_space=space) for space, _, _ in outs],
        scratch_shapes=[*scratch, pltpu.SemaphoreType.DMA((n_copies,))],
        cost_estimate=pl.CostEstimate(flops=flops, bytes_accessed=1 << 20, transcendentals=0),
        compiler_params=pltpu.CompilerParams(vmem_limit_bytes=24 << 20),
    )(*held)


def start_all(sem, first, pairs):
    copies = [
        pltpu.make_async_copy(src, dst, sem.at[first + i]) for i, (src, dst) in enumerate(pairs)
    ]
    for copy in copies:
        copy.start()
    return copies


def wait_all(copies):
    for copy in copies:
        copy.wait()


def elu(v):
    return jnp.where(v > 0, v, jnp.exp(jnp.minimum(v, 0.0)) - 1.0)


def as_float(flag):
    return jnp.asarray(flag, jnp.int32).astype(jnp.float32)


def lane_half(rows):
    return lax.broadcasted_iota(jnp.int32, (rows, LANES), 1) < LANES // 2


def halves(first, second):
    return jnp.where(lane_half(first.shape[0]), first, pltpu.roll(second, LANES // 2, 1))


def reach_mask(core):
    row = lax.broadcasted_iota(jnp.int32, (2 * STEP, LANES), 0)
    first = STEP * core
    return (row >= first) & (row < first + STEP)


def inside_of(row_at, devices):
    above = as_float(jnp.minimum(row_at, 1))
    below = as_float(jnp.minimum(devices - 1 - row_at, 1))
    return jnp.where(lane_half(1), above, below)


def flat_of(channels, rows, cols):
    return pltpu.VMEM((cols // LANES, channels * rows, LANES), jnp.float32)


def widen(source_ref, flat_ref):
    channels, rows, cols = source_ref.shape
    some = 64 // rows

    def step(i, _):
        for block in range(cols // LANES):
            value = source_ref[pl.ds(i * some, some), :, block * LANES : (block + 1) * LANES]
            flat_ref[block, pl.ds(pl.multiple_of(i * some * rows, 8), some * rows), :] = (
                value.astype(jnp.float32).reshape(some * rows, LANES)
            )
        return 0

    lax.fori_loop(0, channels // some, step, 0)


def term_group(terms_ref, start):
    return terms_ref[pl.ds(pl.multiple_of(start, 2 * STEP), 2 * STEP), :].astype(jnp.float32)


def column_terms(terms_ref, core, cols, out_ref):
    def twice(rows):
        return jnp.where(lane_half(rows.shape[0]), pltpu.roll(rows, LANES // 2, 1), rows)

    for first in range(0, cols, LANES):
        at = pl.multiple_of(core * cols + first, LANES)
        out_ref[first : first + LANES] = twice(terms_ref[pl.ds(at, LANES), :].astype(jnp.float32))
    out_ref[cols:] = twice(term_group(terms_ref, cols - 2 * STEP * core))


def fill_rows(x_ref, sources, side_sources, row_terms, col_terms, scale, core, mask):
    cols = col_terms.shape[0] - 2 * STEP
    channels = LANES // 2

    def pair(sources, block, i):
        return jnp.transpose(
            jnp.concatenate(
                [
                    flat[block, pl.ds(first + i, channels, stride=rows), :]
                    for flat, first, rows in sources
                ],
                axis=0,
            )
        )

    def step(i, _):
        row = row_terms[pl.ds(i, 1), :]
        for block in range(cols // LANES):
            at = slice(block * LANES, (block + 1) * LANES)
            value = pair(sources, block, i) + (row + col_terms[at, :])
            if scale is not None:
                value = value * scale
            x_ref[i, at, :] = value.astype(jnp.bfloat16)
        side = pair(side_sources, 0, i)
        value = jnp.where(core == 0, side[: 2 * STEP], side[LANES - 2 * STEP :])
        value = value + (row + col_terms[cols:, :])
        if scale is not None:
            value = value * scale
        x_ref[i, cols:, :] = jnp.where(mask, value, 0.0).astype(jnp.bfloat16)
        return 0

    lax.fori_loop(0, STEP, step, 0)


def weights_of(taps_ref, wanted):
    channels = taps_ref.shape[1]
    zero = jnp.zeros((channels, channels), jnp.bfloat16)
    return jnp.concatenate(
        [
            jnp.concatenate(
                [zero if ky is None else taps_ref[3 * ky + kx] for ky in inputs], axis=1
            )
            for kx in range(3)
            for inputs in wanted
        ],
        axis=0,
    )


OWN_TAPS = ((1, 2, 0, None), (0, 1, None, 2))
NEAR_TAPS = ((2, None, 1, None), (None, 0, None, 1))
FAR_TAPS = ((0, None), (None, 2))


def product(values, weights):
    return lax.dot_general(
        values, weights, (((1,), (1,)), ((), ())), preferred_element_type=jnp.float32
    )


def shifted_sum(p_ref, first):
    last = p_ref.shape[0]
    if first == 0:
        left = jnp.concatenate([p_ref[last - STEP :, :LANES], p_ref[: LANES - STEP, :LANES]], axis=0)
    else:
        left = p_ref[first - STEP : first - STEP + LANES, :LANES]
    centre = p_ref[first : first + LANES, LANES : 2 * LANES]
    right = p_ref[first + STEP : first + STEP + LANES, 2 * LANES :]
    return left + centre + right


def conv_own_rows(own_ref, near_ref, weights, p_ref, out_ref):
    cols = out_ref.shape[1]
    total = jnp.zeros((STEP, LANES), jnp.float32)
    squares = total
    for i in range(STEP):
        p = p_ref.at[i % 2]
        p[...] = product(jnp.concatenate([own_ref[i], near_ref[i]], axis=1), weights)
        for first in range(0, cols, LANES):
            value = shifted_sum(p, first)
            out_ref[i, first : first + LANES, :] = value.astype(jnp.bfloat16)
            value = value.reshape(LANES // STEP, STEP, LANES)
            total = total + jnp.sum(value, axis=0)
            squares = squares + jnp.sum(value * value, axis=0)
    total = total + pltpu.roll(total, LANES // 2, 1)
    squares = squares + pltpu.roll(squares, LANES // 2, 1)
    return jnp.sum(jnp.where(lane_half(STEP), total, squares), axis=0, keepdims=True)


def affine_of(which, stats_refs, gains_ref, cells):
    row = sum(jnp.sum(ref[...], axis=0, keepdims=True) for ref in stats_refs) / cells
    row = jnp.broadcast_to(row, (STEP, LANES))
    other = pltpu.roll(row, LANES // 2, 1)
    average = jnp.where(lane_half(STEP), row, other)
    spread = jnp.where(lane_half(STEP), other, row) - average * average
    factor = gains_ref[which : which + 1] * lax.rsqrt(spread + epsilon)
    offset = gains_ref[2 + which : 3 + which] - average * factor
    return factor[0:1], offset[0:1]


def prepare_kernel(
    pair, feats, w_row, w_col, top_out, bottom_out, terms_ref, top, bottom, feats_in, row_in,
    col_in, sem,
):
    parts = start_all(sem, 0, ((pair.at[:, :STEP], top), (pair.at[:, STEP:], bottom)))
    inputs = start_all(sem, 2, ((feats, feats_in), (w_row, row_in), (w_col, col_in)))
    wait_all(inputs)
    terms = jnp.concatenate(
        [product(feats_in[...], w[...]) for w in (row_in, col_in)], axis=1
    ).astype(jnp.bfloat16)
    terms_ref[...] = jnp.broadcast_to(terms[None], terms_ref.shape)
    wait_all(parts)
    wait_all(start_all(sem, 0, ((top, top_out), (bottom, bottom_out))))


def first_kernel(
    devices, own_in, above_in, below_in, side_in, terms_in, taps_in,
    own_out, near_out, conv_out, give_out, stats_ref,
    x_own, x_near, conv_ref, p_ref, own, above, below, side, terms, taps,
    own_flat, above_flat, below_flat, side_flat, col_terms, row_terms, sem,
):
    row_at, core = lax.axis_index(GX), lax.axis_index("gy")
    _, rows, cols = own.shape
    half = STEP // 2
    inputs = start_all(
        sem, 0,
        ((terms_in, terms), (side_in, side), (own_in, own), (above_in, above), (below_in, below),
         (taps_in, taps)),
    )
    inputs[0].wait()
    column_terms(terms, core, cols, col_terms)
    mine = term_group(terms, row_at * rows)
    up = term_group(terms, jnp.maximum(row_at - 1, 0) * rows)
    down = term_group(terms, jnp.minimum(row_at + 1, devices - 1) * rows)
    row_terms[0] = halves(mine[:STEP], mine[STEP:])
    row_terms[1] = halves(up[STEP:], down[:STEP])
    mask = reach_mask(core)
    tall = rows + 2 * STEP
    inputs[1].wait()
    widen(side, side_flat)
    inputs[2].wait()
    widen(own, own_flat)
    fill_rows(
        x_own, ((own_flat, 0, rows), (own_flat, STEP, rows)),
        ((side_flat, STEP, tall), (side_flat, 2 * STEP, tall)),
        row_terms.at[0], col_terms, None, core, mask,
    )
    given = x_own.at[pl.ds(half * (1 - core), half), pl.ds(0, cols)]
    outputs = start_all(sem, 6, ((x_own, own_out), (given, give_out)))
    wait_all(inputs[3:5])
    widen(above, above_flat)
    widen(below, below_flat)
    fill_rows(
        x_near, ((above_flat, 0, STEP), (below_flat, 0, STEP)),
        ((side_flat, 0, tall), (side_flat, STEP + rows, tall)),
        row_terms.at[1], col_terms, inside_of(row_at, devices), core, mask,
    )
    outputs += start_all(sem, 8, ((x_near, near_out),))
    inputs[5].wait()
    stats = conv_own_rows(x_own, x_near, weights_of(taps, OWN_TAPS), p_ref, conv_ref)
    outputs += start_all(sem, 9, ((conv_ref, conv_out),))
    stats_ref[...] = jnp.broadcast_to(stats, stats_ref.shape)
    wait_all(outputs)


def far_kernel(
    devices, own_in, near_in, conv_in, above_in, below_in, side_in, terms_in, taps_in,
    conv_out, edge_out,
    x_own, x_near, x_far, conv_ref, edge_ref, p_ref, above, below, side, terms, taps,
    above_flat, below_flat, side_flat, col_terms, row_terms, sem,
):
    row_at, core = lax.axis_index(GX), lax.axis_index("gy")
    _, _, cols = above.shape
    rows = 2 * STEP
    edge_at = pl.multiple_of((cols - 2 * STEP) * (1 - core), 2 * STEP)
    inputs = start_all(
        sem, 0,
        ((terms_in, terms), (side_in, side), (above_in, above), (below_in, below),
         (own_in, x_own), (near_in, x_near),
         (conv_in.at[:, pl.ds(edge_at, 2 * STEP)], edge_ref.at[0]), (taps_in, taps)),
    )
    inputs[0].wait()
    column_terms(terms, core, cols, col_terms)
    up = term_group(terms, jnp.maximum(row_at - 1, 0) * rows)
    down = term_group(terms, jnp.minimum(row_at + 1, devices - 1) * rows)
    row_terms[...] = halves(up[:STEP], down[STEP:])
    wait_all(inputs[1:4])
    widen(side, side_flat)
    widen(above, above_flat)
    widen(below, below_flat)
    fill_rows(
        x_far, ((above_flat, 0, STEP), (below_flat, 0, STEP)),
        ((side_flat, 0, 2 * STEP), (side_flat, STEP, 2 * STEP)),
        row_terms, col_terms, inside_of(row_at, devices), core, reach_mask(core),
    )
    wait_all(inputs[4:])
    near_weights, far_weights = weights_of(taps, NEAR_TAPS), weights_of(taps, FAR_TAPS)
    for i in range(STEP):
        p = p_ref.at[i % 2]
        near = jnp.concatenate([x_own[i], x_near[i]], axis=1)
        p[...] = product(near, near_weights) + product(x_far[i], far_weights)
        for first in range(0, cols, LANES):
            conv_ref[i, first : first + LANES, :] = shifted_sum(p, first).astype(jnp.bfloat16)
    edge_ref[1] = conv_ref[:, pl.ds(edge_at, 2 * STEP), :]
    wait_all(start_all(sem, 0, ((edge_ref, edge_out), (conv_ref, conv_out))))


def second_kernel(
    devices, cells, own_in, far_in, side, stats, stats_other, gains, taps_in,
    conv_out, give_out, stats_ref,
    a_own, a_near, conv_ref, p_ref, own, far, taps, sem,
):
    row_at, core = lax.axis_index(GX), lax.axis_index("gy")
    cols = own.shape[1]
    half = STEP // 2
    inputs = start_all(sem, 0, ((far_in, far), (own_in, own), (taps_in, taps)))
    factor, offset = affine_of(0, (stats, stats_other), gains, cells)
    inside = inside_of(row_at, devices)
    mask = reach_mask(core)

    def activated(value, scale):
        value = elu(value.astype(jnp.float32) * factor + offset)
        return value if scale is None else value * scale

    def fill(to_ref, source, which, scale):
        def step(i, _):
            for first in range(0, cols, LANES):
                at = slice(first, first + LANES)
                to_ref[i, at, :] = activated(source[i, at, :], scale).astype(jnp.bfloat16)
            beyond = jnp.where(mask, activated(side[which, i], scale), 0.0)
            to_ref[i, cols:, :] = beyond.astype(jnp.bfloat16)
            return 0

        lax.fori_loop(0, STEP, step, 0)

    inputs[0].wait()
    fill(a_near, far, 1, inside)
    wait_all(inputs[1:])
    fill(a_own, own, 0, None)
    stats = conv_own_rows(a_own, a_near, weights_of(taps, OWN_TAPS), p_ref, conv_ref)
    given = conv_ref.at[pl.ds(half * (1 - core), half)]
    outputs = start_all(sem, 0, ((given, give_out), (conv_ref, conv_out)))
    stats_ref[...] = jnp.broadcast_to(stats, stats_ref.shape)
    wait_all(outputs)


def pack_kernel(
    cells, block_in, block_in_other, conv_in, conv_other_in, stats, stats_other, gains,
    block_out_out, send_ref,
    out_ref, own, other, conv, conv_other, sem,
):
    core = lax.axis_index("gy")
    cols = conv.shape[1]
    half = STEP // 2
    inputs = start_all(
        sem, 0,
        ((block_in.at[:, pl.ds(0, cols)], own), (conv_in, conv), (block_in_other, other),
         (conv_other_in, conv_other)),
    )
    factor, offset = affine_of(1, (stats, stats_other), gains, cells)
    wide = 2 * STEP
    peers, some = cols // wide, LANES // wide

    def block_out(x, value):
        value = x.astype(jnp.float32) + value.astype(jnp.float32) * factor + offset
        return elu(value).astype(jnp.bfloat16)

    def mine(i, _):
        for first in range(0, cols, LANES):
            at = slice(first, first + LANES)
            out_ref[i, at, :] = block_out(own[i, at, :], conv[i, at, :])
        return 0

    wait_all(inputs[:2])
    lax.fori_loop(0, STEP, mine, 0)
    outputs = start_all(sem, 4, ((out_ref, block_out_out),))

    def step(i, _):
        for first in range(0, cols, LANES):
            at = slice(first, first + LANES)
            value = out_ref[half * core + i, at, :].reshape(some, wide, LANES)
            send_ref[pl.ds(peers * core + first // wide, some), i] = value
            value = block_out(other[i, at, :], conv_other[i, at, :]).reshape(some, wide, LANES)
            send_ref[pl.ds(peers * (1 - core) + first // wide, some), i] = value
        return 0

    wait_all(inputs[2:])
    lax.fori_loop(0, half, step, 0)
    wait_all(outputs)


def merge_kernel(own_in, received, other, result, out_ref, own, cells_ref, flat_ref, sem):
    core = lax.axis_index("gy")
    channels, rows, cols = out_ref.shape
    peers = other.shape[0]
    inputs = start_all(sem, 0, ((own_in, own),))

    def gather(s, _):
        cells_ref[s, core] = received[peers * core + s].astype(jnp.float32)
        cells_ref[s, 1 - core] = other[s].astype(jnp.float32)
        return 0

    lax.fori_loop(0, peers, gather, 0)
    wait_all(inputs)
    flat = cells_ref.reshape(peers * STEP * rows, LANES)
    some = LANES // rows
    lower = lane_half(some * STEP)

    def step(i, _):
        for block in range(cols // LANES):
            first = block * some * STEP * rows
            upper_row = flat[pl.ds(first + i, some * STEP, stride=rows), :]
            lower_row = flat[pl.ds(first + STEP + i, some * STEP, stride=rows), :]
            even = jnp.where(lower, upper_row, pltpu.roll(lower_row, channels, 1))
            odd = jnp.where(lower, pltpu.roll(upper_row, channels, 1), lower_row)
            mirrored = jnp.concatenate(
                [
                    part[s * STEP : (s + 1) * STEP]
                    for s in range(some)
                    for part in (even, odd)
                ],
                axis=0,
            )
            value = own[i, block * LANES : (block + 1) * LANES, :].astype(jnp.float32) + mirrored
            value = jnp.transpose(0.5 * value)
            for high in range(rows // STEP):
                flat_ref[block, pl.ds(high * STEP + i, channels, stride=rows), :] = value[
                    channels * high : channels * (high + 1)
                ]
        return 0

    lax.fori_loop(0, STEP, step, 0)

    def store(c, _):
        for block in range(cols // LANES):
            value = flat_ref[block, pl.ds(pl.multiple_of(c * rows, 8), rows), :]
            out_ref[c, :, block * LANES : (block + 1) * LANES] = value.astype(jnp.bfloat16)
        return 0

    part = channels // 2
    lax.fori_loop(0, part, store, 0)
    outputs = start_all(sem, 1, ((out_ref.at[pl.ds(0, part)], result.at[pl.ds(0, part)]),))
    lax.fori_loop(part, channels, store, 0)
    outputs += start_all(sem, 2, ((out_ref.at[pl.ds(part, part)], result.at[pl.ds(part, part)]),))
    wait_all(outputs)


def body(residue_feats, pair_feats, w_row, w_col, first_taps, second_taps, norm_scale, norm_shift):
    channels, rows, cols = pair_feats.shape
    cores = lax.axis_size("gy")
    devices = lax.axis_size(GX)
    first_core = lax.axis_index("gy") == 0
    cells = devices * rows * cores * cols
    bf16, f32 = jnp.bfloat16, jnp.float32
    conv_flops = 2 * 9 * channels * channels * rows * cols

    def edge(x):
        return jnp.where(first_core, x[..., cols - LANES :], x[..., :LANES])

    def swap(x):
        return lax.ppermute(x, "gy", SWAP)

    down = functools.partial(lax.ppermute, axis_name=GX, perm=chain(devices, 1))
    up = functools.partial(lax.ppermute, axis_name=GX, perm=chain(devices, -1))
    eight = (channels, STEP, cols)
    top, bottom, terms = call(
        prepare_kernel,
        (
            (HBM, eight, bf16),
            (HBM, eight, bf16),
            (VMEM, (devices, rows, 2 * channels), bf16),
        ),
        [
            VMEM(eight, bf16),
            VMEM(eight, bf16),
            VMEM(residue_feats.shape, bf16),
            VMEM(w_row.T.shape, bf16),
            VMEM(w_col.T.shape, bf16),
        ],
        5,
        conv_flops // 16,
        ((HBM, pair_feats), (HBM, residue_feats), (HBM, w_row.T), (HBM, w_col.T)),
    )
    above_near, below_near = down(bottom), up(top)
    above_far, below_far = down(top), up(bottom)
    terms = lax.all_to_all(terms, GX, 0, 0, tiled=True)
    terms = terms.reshape(devices * rows, 2 * channels)
    gains = jnp.tile(jnp.concatenate([norm_scale, norm_shift], axis=0), (1, 2))

    near_side = swap(
        jnp.concatenate([edge(above_near), edge(pair_feats), edge(below_near)], axis=1)
    )
    far_side = swap(jnp.concatenate([edge(above_far), edge(below_far)], axis=1))

    taps_shape = VMEM(first_taps.shape, bf16)
    terms_shape = VMEM(terms.shape, bf16)
    whole = (STEP, cols, LANES)
    part = (STEP // 2, cols, LANES)
    wide = (STEP, cols + 2 * STEP, LANES)
    products = VMEM((2, cols + 2 * STEP, 3 * LANES), f32)
    sums = (devices, LANES)
    own_rows, near_rows, conv_own, own_give, stats = call(
        functools.partial(first_kernel, devices),
        (
            (HBM, wide, bf16),
            (HBM, wide, bf16),
            (HBM, whole, bf16),
            (HBM, part, bf16),
            (VMEM, sums, f32),
        ),
        [
            VMEM(wide, bf16),
            VMEM(wide, bf16),
            VMEM(whole, bf16),
            products,
            VMEM(pair_feats.shape, bf16),
            VMEM(eight, bf16),
            VMEM(eight, bf16),
            VMEM(near_side.shape, bf16),
            terms_shape,
            taps_shape,
            flat_of(channels, rows, cols),
            flat_of(channels, STEP, cols),
            flat_of(channels, STEP, cols),
            flat_of(channels, rows + 2 * STEP, LANES),
            VMEM(wide[1:], f32),
            VMEM((2, STEP, LANES), f32),
        ],
        10,
        conv_flops,
        ((HBM, pair_feats), (HBM, above_near), (HBM, below_near), (HBM, near_side),
         (HBM, terms), (HBM, first_taps)),
    )
    stats = lax.all_to_all(stats, GX, 0, 0, tiled=True)
    stats_other = swap(stats)
    conv_far, edges = call(
        functools.partial(far_kernel, devices),
        ((HBM, whole, bf16), (HBM, (2, STEP, 2 * STEP, LANES), bf16)),
        [
            VMEM(wide, bf16),
            VMEM(wide, bf16),
            VMEM(wide, bf16),
            VMEM(whole, bf16),
            VMEM((2, STEP, 2 * STEP, LANES), bf16),
            products,
            VMEM(eight, bf16),
            VMEM(eight, bf16),
            VMEM(far_side.shape, bf16),
            terms_shape,
            taps_shape,
            flat_of(channels, STEP, cols),
            flat_of(channels, STEP, cols),
            flat_of(channels, 2 * STEP, LANES),
            VMEM(wide[1:], f32),
            VMEM((STEP, LANES), f32),
        ],
        8,
        conv_flops,
        ((HBM, own_rows), (HBM, near_rows), (HBM, conv_own), (HBM, above_far),
         (HBM, below_far), (HBM, far_side), (HBM, terms), (HBM, first_taps)),
    )
    edges = swap(edges)
    own_other = swap(own_give)
    conv_second, second_give, stats = call(
        functools.partial(second_kernel, devices, cells),
        ((HBM, whole, bf16), (HBM, part, bf16), (VMEM, sums, f32)),
        [
            VMEM(wide, bf16),
            VMEM(wide, bf16),
            VMEM(whole, bf16),
            products,
            VMEM(whole, bf16),
            VMEM(whole, bf16),
            taps_shape,
        ],
        3,
        conv_flops,
        ((HBM, conv_own), (HBM, conv_far), (VMEM, edges), (VMEM, stats), (VMEM, stats_other),
         (VMEM, gains), (HBM, second_taps)),
    )
    stats = lax.all_to_all(stats, GX, 0, 0, tiled=True)
    stats_other = swap(stats)
    conv_other = swap(second_give)
    block_out, send = call(
        functools.partial(pack_kernel, cells),
        ((HBM, whole, bf16), (VMEM, (devices, STEP // 2, rows, LANES), bf16)),
        [
            VMEM(whole, bf16),
            VMEM(whole, bf16),
            VMEM(part, bf16),
            VMEM(whole, bf16),
            VMEM(part, bf16),
        ],
        5,
        conv_flops,
        ((HBM, own_rows), (HBM, own_other), (HBM, conv_second), (HBM, conv_other),
         (VMEM, stats), (VMEM, stats_other), (VMEM, gains)),
    )
    received = lax.all_to_all(send, GX, 0, 0, tiled=True)
    peers = devices // cores
    other = swap(jnp.where(first_core, received[peers:], received[:peers]))
    return call(
        merge_kernel,
        ((HBM, pair_feats.shape, bf16),),
        [
            VMEM(pair_feats.shape, bf16),
            VMEM(whole, bf16),
            VMEM((peers, cores, STEP // 2, rows, LANES), f32),
            flat_of(channels, rows, cols),
        ],
        3,
        conv_flops,
        ((HBM, block_out), (VMEM, received), (VMEM, other)),
    )[0]


def solution(mesh):
    torus = Mesh(
        mesh.devices.reshape(mesh.shape["grp"], 4, 16, mesh.shape["gy"]),
        ("grp", "gx_0", "gx_1", "gy"),
    )
    placed = (P(GRP_GX, None), P(None, GRP_GX, "gy"), P(), P(), P(), P(), P(), P())
    return jax.shard_map(
        body, mesh=torus, in_specs=placed, out_specs=P(None, GRP_GX, "gy"), check_vma=False
    )
```

```python
import functools

import jax
import jax.numpy as jnp
from jax import lax
from jax.experimental import pallas as pl
from jax.experimental.pallas import tpu as pltpu
from jax.sharding import Mesh
from jax.sharding import PartitionSpec as P

STEP = 8
GX = ("gx_0", "gx_1")
GRP_GX = ("grp", "gx_0", "gx_1")
LANES = 128
SWAP = [(0, 1), (1, 0)]
HBM, VMEM = pltpu.HBM, pltpu.VMEM

epsilon = 1e-05


def chain(count, step):
    pairs = [(i, i + 1) for i in range(count - 1)]
    return pairs if step > 0 else [(b, a) for a, b in pairs]


def call(kernel, outs, scratch, n_copies, flops, operands):
    spaces = [space for space, _ in operands]
    held = [pltpu.with_memory_space_constraint(x, space) for space, x in operands]
    return pl.pallas_call(
        kernel,
        out_shape=[space(shape, dtype) for space, shape, dtype in outs],
        in_specs=[pl.BlockSpec(memory_space=space) for space in spaces],
        out_specs=[pl.BlockSpec(memory_space=space) for space, _, _ in outs],
        scratch_shapes=[*scratch, pltpu.SemaphoreType.DMA((n_copies,))],
        cost_estimate=pl.CostEstimate(flops=flops, bytes_accessed=1 << 20, transcendentals=0),
        compiler_params=pltpu.CompilerParams(vmem_limit_bytes=24 << 20),
    )(*held)


def start_all(sem, first, pairs):
    copies = [
        pltpu.make_async_copy(src, dst, sem.at[first + i]) for i, (src, dst) in enumerate(pairs)
    ]
    for copy in copies:
        copy.start()
    return copies


def wait_all(copies):
    for copy in copies:
        copy.wait()


def elu(v):
    return jnp.where(v > 0, v, jnp.exp(jnp.minimum(v, 0.0)) - 1.0)


def as_float(flag):
    return jnp.asarray(flag, jnp.int32).astype(jnp.float32)


def lane_half(rows):
    return lax.broadcasted_iota(jnp.int32, (rows, LANES), 1) < LANES // 2


def halves(first, second):
    return jnp.where(lane_half(first.shape[0]), first, pltpu.roll(second, LANES // 2, 1))


def reach_mask(core):
    row = lax.broadcasted_iota(jnp.int32, (2 * STEP, LANES), 0)
    first = STEP * core
    return (row >= first) & (row < first + STEP)


def inside_of(row_at, devices):
    above = as_float(jnp.minimum(row_at, 1))
    below = as_float(jnp.minimum(devices - 1 - row_at, 1))
    return jnp.where(lane_half(1), above, below)


def flat_of(channels, rows, cols):
    return pltpu.VMEM((cols // LANES, channels * rows, LANES), jnp.float32)


def widen(source_ref, flat_ref):
    channels, rows, cols = source_ref.shape
    some = 64 // rows

    def step(i, _):
        for block in range(cols // LANES):
            value = source_ref[pl.ds(i * some, some), :, block * LANES : (block + 1) * LANES]
            flat_ref[block, pl.ds(pl.multiple_of(i * some * rows, 8), some * rows), :] = (
                value.astype(jnp.float32).reshape(some * rows, LANES)
            )
        return 0

    lax.fori_loop(0, channels // some, step, 0)


def fill_rows(x_ref, sources, side_sources, row_terms, col_terms, scale, core, mask):
    cols = col_terms.shape[0] - 2 * STEP
    channels = LANES // 2

    def pair(sources, block, i):
        return jnp.transpose(
            jnp.concatenate(
                [
                    flat[block, pl.ds(first + i, channels, stride=rows), :]
                    for flat, first, rows in sources
                ],
                axis=0,
            )
        )

    def step(i, _):
        row = row_terms[pl.ds(i, 1), :]
        for block in range(cols // LANES):
            at = slice(block * LANES, (block + 1) * LANES)
            value = pair(sources, block, i) + (row + col_terms[at, :])
            if scale is not None:
                value = value * scale
            x_ref[i, at, :] = value.astype(jnp.bfloat16)
        side = pair(side_sources, 0, i)
        value = jnp.where(core == 0, side[: 2 * STEP], side[LANES - 2 * STEP :])
        value = value + (row + col_terms[cols:, :])
        if scale is not None:
            value = value * scale
        x_ref[i, cols:, :] = jnp.where(mask, value, 0.0).astype(jnp.bfloat16)
        return 0

    lax.fori_loop(0, STEP, step, 0)


def weights_of(taps_ref, wanted):
    channels = taps_ref.shape[1]
    zero = jnp.zeros((channels, channels), jnp.bfloat16)
    return jnp.concatenate(
        [
            jnp.concatenate(
                [zero if ky is None else taps_ref[3 * ky + kx] for ky in inputs], axis=1
            )
            for kx in range(3)
            for inputs in wanted
        ],
        axis=0,
    )


OWN_TAPS = ((1, 2, 0, None), (0, 1, None, 2))


def product(values, weights):
    return lax.dot_general(
        values, weights, (((1,), (1,)), ((), ())), preferred_element_type=jnp.float32
    )


def shifted_sum(p_ref, first):
    last = p_ref.shape[0]
    if first == 0:
        left = jnp.concatenate([p_ref[last - STEP :, :LANES], p_ref[: LANES - STEP, :LANES]], axis=0)
    else:
        left = p_ref[first - STEP : first - STEP + LANES, :LANES]
    centre = p_ref[first : first + LANES, LANES : 2 * LANES]
    right = p_ref[first + STEP : first + STEP + LANES, 2 * LANES :]
    return left + centre + right


def conv_own_rows(own_ref, near_ref, weights, p_ref, out_ref):
    cols = out_ref.shape[1]
    total = jnp.zeros((STEP, LANES), jnp.float32)
    squares = total
    for i in range(STEP):
        p = p_ref.at[i % 2]
        p[...] = product(jnp.concatenate([own_ref[i], near_ref[i]], axis=1), weights)
        for first in range(0, cols, LANES):
            value = shifted_sum(p, first)
            out_ref[i, first : first + LANES, :] = value.astype(jnp.bfloat16)
            value = value.reshape(LANES // STEP, STEP, LANES)
            total = total + jnp.sum(value, axis=0)
            squares = squares + jnp.sum(value * value, axis=0)
    total = total + pltpu.roll(total, LANES // 2, 1)
    squares = squares + pltpu.roll(squares, LANES // 2, 1)
    return jnp.sum(jnp.where(lane_half(STEP), total, squares), axis=0, keepdims=True)


def affine_of(which, stats_refs, gains_ref, cells):
    row = sum(jnp.sum(ref[...], axis=0, keepdims=True) for ref in stats_refs) / cells
    row = jnp.broadcast_to(row, (STEP, LANES))
    other = pltpu.roll(row, LANES // 2, 1)
    average = jnp.where(lane_half(STEP), row, other)
    spread = jnp.where(lane_half(STEP), other, row) - average * average
    factor = gains_ref[which : which + 1] * lax.rsqrt(spread + epsilon)
    offset = gains_ref[2 + which : 3 + which] - average * factor
    return factor[0:1], offset[0:1]


def prepare_kernel(
    pair, feats, w_row, w_col, top, bottom, col_terms, row_terms, feats_in, row_in, col_in, sem
):
    channels = pair.shape[0]
    parts = start_all(
        sem, 0,
        ((pair.at[:, :STEP], top.at[pl.ds(0, channels)]),
         (pair.at[:, STEP:], bottom.at[pl.ds(0, channels)])),
    )
    inputs = start_all(sem, 2, ((feats, feats_in), (w_row, row_in), (w_col, col_in)))
    wait_all(inputs)
    zero = jnp.zeros((2 * STEP, LANES - channels), jnp.float32)
    row = jnp.concatenate([product(feats_in[...], row_in[...]), zero], axis=1)
    col = jnp.concatenate([product(feats_in[...], col_in[...]), zero], axis=1)
    packed = halves(col[:STEP], col[STEP:]).astype(jnp.bfloat16)
    col_terms[...] = jnp.broadcast_to(packed[None], col_terms.shape)
    row_terms[...] = halves(row[:STEP], row[STEP:])
    empty = jnp.zeros((STEP, top.shape[2] - LANES), jnp.float32)
    for ref, rows in ((top, row[:STEP]), (bottom, row[STEP:])):
        ref[channels] = jnp.concatenate([rows, empty], axis=1).astype(jnp.bfloat16)
    wait_all(parts)


def first_kernel(
    devices, own_in, above_in, below_in, side, terms, mine, taps_in,
    own_out, conv_out, give_out, down_out, up_out, edge_ref, stats_ref,
    x_own, x_near, conv_ref, p_ref, down_ref, up_ref, own, above, below, taps,
    own_flat, above_flat, below_flat, side_flat, col_terms, row_terms, sem,
):
    row_at, core = lax.axis_index(GX), lax.axis_index("gy")
    channels, rows, cols = own.shape
    half = STEP // 2
    inputs = start_all(
        sem, 0, ((own_in, own), (above_in, above), (below_in, below), (taps_in, taps))
    )

    def put_terms(source, at):
        value = terms[source].astype(jnp.float32)
        other = pltpu.roll(value, LANES // 2, 1)
        col_terms[pl.ds(at, STEP), :] = jnp.where(lane_half(STEP), value, other)
        col_terms[pl.ds(at + STEP, STEP), :] = jnp.where(lane_half(STEP), other, value)

    peers = cols // rows

    def put_own(i, _):
        put_terms(peers * core + i, pl.multiple_of(i * rows, 2 * STEP))
        return 0

    lax.fori_loop(0, peers, put_own, 0)
    put_terms(peers - core, cols)
    row_terms[0] = mine[...].astype(jnp.bfloat16).astype(jnp.float32)
    mask = reach_mask(core)
    tall = rows + 2 * STEP
    widen(side, side_flat)
    inputs[0].wait()
    widen(own, own_flat)
    fill_rows(
        x_own, ((own_flat, 0, rows), (own_flat, STEP, rows)),
        ((side_flat, STEP, tall), (side_flat, 2 * STEP, tall)),
        row_terms.at[0], col_terms, None, core, mask,
    )
    given = x_own.at[pl.ds(half * (1 - core), half), pl.ds(0, cols)]
    outputs = start_all(sem, 4, ((x_own.at[:, pl.ds(0, cols)], own_out), (given, give_out)))
    wait_all(inputs[1:3])
    widen(above.at[pl.ds(0, channels)], above_flat)
    widen(below.at[pl.ds(0, channels)], below_flat)
    row_terms[1] = halves(
        above[channels, :, :LANES].astype(jnp.float32),
        below[channels, :, :LANES].astype(jnp.float32),
    )
    fill_rows(
        x_near, ((above_flat, 0, STEP), (below_flat, 0, STEP)),
        ((side_flat, 0, tall), (side_flat, STEP + rows, tall)),
        row_terms.at[1], col_terms, inside_of(row_at, devices), core, mask,
    )
    inputs[3].wait()
    stats = conv_own_rows(x_own, x_near, weights_of(taps, OWN_TAPS), p_ref, conv_ref)
    outputs += start_all(sem, 6, ((conv_ref, conv_out),))
    lower = lane_half(LANES)
    for i in range(half):
        for first in range(0, cols, LANES):
            at = slice(first, first + LANES)
            one = conv_ref[i, at, :].astype(jnp.float32)
            two = conv_ref[i + half, at, :].astype(jnp.float32)
            up_ref[i, at, :] = jnp.where(lower, one, pltpu.roll(two, LANES // 2, 1)).astype(
                jnp.bfloat16
            )
            down_ref[i, at, :] = jnp.where(lower, pltpu.roll(one, LANES // 2, 1), two).astype(
                jnp.bfloat16
            )
    outputs += start_all(sem, 7, ((down_ref, down_out), (up_ref, up_out)))
    edge_at = pl.multiple_of((cols - 2 * STEP) * (1 - core), 2 * STEP)
    edge_ref[...] = conv_ref[:, pl.ds(edge_at, 2 * STEP), :]
    stats_ref[...] = jnp.broadcast_to(stats, stats_ref.shape)
    wait_all(outputs)


def second_kernel(
    devices, cells, own_in, above_in, below_in, edge, corner, stats, stats_other, gains, taps_in,
    conv_out, give_out, stats_ref,
    a_own, a_near, conv_ref, p_ref, own, above, below, taps, sem,
):
    row_at, core = lax.axis_index(GX), lax.axis_index("gy")
    cols = own.shape[1]
    half = STEP // 2
    inputs = start_all(
        sem, 0, ((own_in, own), (above_in, above), (below_in, below), (taps_in, taps))
    )
    factor, offset = affine_of(0, (stats, stats_other), gains, cells)
    inside = inside_of(row_at, devices)
    mask = reach_mask(core)

    def activated(value):
        return elu(value.astype(jnp.float32) * factor + offset)

    def fill_own(i, _):
        for first in range(0, cols, LANES):
            at = slice(first, first + LANES)
            a_own[i, at, :] = activated(own[i, at, :]).astype(jnp.bfloat16)
        beyond = jnp.where(mask, activated(edge[i]), 0.0)
        a_own[i, cols:, :] = beyond.astype(jnp.bfloat16)
        return 0

    def two_rows(up, down):
        up, down = up.astype(jnp.float32), down.astype(jnp.float32)
        lower = lane_half(up.shape[0])
        return (
            jnp.where(lower, up, pltpu.roll(down, LANES // 2, 1)),
            jnp.where(lower, pltpu.roll(up, LANES // 2, 1), down),
        )

    def fill_near(i, _):
        for first in range(0, cols, LANES):
            at = slice(first, first + LANES)
            for k, value in enumerate(two_rows(above[i, at, :], below[i, at, :])):
                a_near[i + half * k, at, :] = (activated(value) * inside).astype(jnp.bfloat16)
        for k, value in enumerate(two_rows(corner[0, i], corner[1, i])):
            beyond = jnp.where(mask, activated(value) * inside, 0.0)
            a_near[i + half * k, cols:, :] = beyond.astype(jnp.bfloat16)
        return 0

    inputs[0].wait()
    lax.fori_loop(0, STEP, fill_own, 0)
    wait_all(inputs[1:])
    lax.fori_loop(0, half, fill_near, 0)
    stats = conv_own_rows(a_own, a_near, weights_of(taps, OWN_TAPS), p_ref, conv_ref)
    given = conv_ref.at[pl.ds(half * (1 - core), half)]
    outputs = start_all(sem, 0, ((given, give_out), (conv_ref, conv_out)))
    stats_ref[...] = jnp.broadcast_to(stats, stats_ref.shape)
    wait_all(outputs)


def pack_kernel(
    cells, block_in, other, conv_in, conv_other, stats, stats_other, gains,
    block_out_out, send_ref,
    out_ref, own, conv, sem,
):
    core = lax.axis_index("gy")
    cols = conv.shape[1]
    half = STEP // 2
    inputs = start_all(sem, 0, ((block_in, own), (conv_in, conv)))
    factor, offset = affine_of(1, (stats, stats_other), gains, cells)
    wide = 2 * STEP
    peers, some = cols // wide, LANES // wide

    def block_out(x, value):
        value = x.astype(jnp.float32) + value.astype(jnp.float32) * factor + offset
        return elu(value).astype(jnp.bfloat16)

    def mine(i, _):
        for first in range(0, cols, LANES):
            at = slice(first, first + LANES)
            out_ref[i, at, :] = block_out(own[i, at, :], conv[i, at, :])
        return 0

    wait_all(inputs[:2])
    lax.fori_loop(0, STEP, mine, 0)
    outputs = start_all(sem, 2, ((out_ref, block_out_out),))

    def step(i, _):
        for first in range(0, cols, LANES):
            at = slice(first, first + LANES)
            value = out_ref[half * core + i, at, :].reshape(some, wide, LANES)
            send_ref[pl.ds(peers * core + first // wide, some), i] = value
            value = block_out(other[i, at, :], conv_other[i, at, :]).reshape(some, wide, LANES)
            send_ref[pl.ds(peers * (1 - core) + first // wide, some), i] = value
        return 0

    lax.fori_loop(0, half, step, 0)
    wait_all(outputs)


def merge_kernel(own_in, received, other, result, out_ref, own, cells_ref, flat_ref, sem):
    core = lax.axis_index("gy")
    channels, rows, cols = out_ref.shape
    peers = other.shape[0]
    inputs = start_all(sem, 0, ((own_in, own),))

    def gather(s, _):
        cells_ref[s, core] = received[peers * core + s].astype(jnp.float32)
        cells_ref[s, 1 - core] = other[s].astype(jnp.float32)
        return 0

    lax.fori_loop(0, peers, gather, 0)
    wait_all(inputs)
    flat = cells_ref.reshape(peers * STEP * rows, LANES)
    some = LANES // rows
    lower = lane_half(some * STEP)

    def step(i, _):
        for block in range(cols // LANES):
            first = block * some * STEP * rows
            upper_row = flat[pl.ds(first + i, some * STEP, stride=rows), :]
            lower_row = flat[pl.ds(first + STEP + i, some * STEP, stride=rows), :]
            even = jnp.where(lower, upper_row, pltpu.roll(lower_row, channels, 1))
            odd = jnp.where(lower, pltpu.roll(upper_row, channels, 1), lower_row)
            mirrored = jnp.concatenate(
                [
                    part[s * STEP : (s + 1) * STEP]
                    for s in range(some)
                    for part in (even, odd)
                ],
                axis=0,
            )
            value = own[i, block * LANES : (block + 1) * LANES, :].astype(jnp.float32) + mirrored
            value = jnp.transpose(0.5 * value)
            for high in range(rows // STEP):
                flat_ref[block, pl.ds(high * STEP + i, channels, stride=rows), :] = value[
                    channels * high : channels * (high + 1)
                ]
        return 0

    lax.fori_loop(0, STEP, step, 0)

    def store(c, _):
        for block in range(cols // LANES):
            value = flat_ref[block, pl.ds(pl.multiple_of(c * rows, 8), rows), :]
            out_ref[c, :, block * LANES : (block + 1) * LANES] = value.astype(jnp.bfloat16)
        return 0

    part = channels // 2
    lax.fori_loop(0, part, store, 0)
    outputs = start_all(sem, 1, ((out_ref.at[pl.ds(0, part)], result.at[pl.ds(0, part)]),))
    lax.fori_loop(part, channels, store, 0)
    outputs += start_all(sem, 2, ((out_ref.at[pl.ds(part, part)], result.at[pl.ds(part, part)]),))
    wait_all(outputs)


def body(residue_feats, pair_feats, w_row, w_col, first_taps, second_taps, norm_scale, norm_shift):
    channels, rows, cols = pair_feats.shape
    cores = lax.axis_size("gy")
    devices = lax.axis_size(GX)
    first_core = lax.axis_index("gy") == 0
    cells = devices * rows * cores * cols
    bf16, f32 = jnp.bfloat16, jnp.float32
    conv_flops = 2 * 9 * channels * channels * rows * cols

    def edge(x):
        return jnp.where(first_core, x[..., cols - LANES :], x[..., :LANES])

    def swap(x):
        return lax.ppermute(x, "gy", SWAP)

    down = functools.partial(lax.ppermute, axis_name=GX, perm=chain(devices, 1))
    up = functools.partial(lax.ppermute, axis_name=GX, perm=chain(devices, -1))
    eight = (channels + 1, STEP, cols)
    top, bottom, terms, mine = call(
        prepare_kernel,
        (
            (VMEM, eight, bf16),
            (VMEM, eight, bf16),
            (VMEM, (devices, STEP, LANES), bf16),
            (VMEM, (STEP, LANES), f32),
        ),
        [
            VMEM(residue_feats.shape, bf16),
            VMEM(w_row.T.shape, bf16),
            VMEM(w_col.T.shape, bf16),
        ],
        5,
        conv_flops // 16,
        ((HBM, pair_feats), (HBM, residue_feats), (HBM, w_row.T), (HBM, w_col.T)),
    )
    above, below = down(bottom), up(top)
    terms = lax.all_to_all(terms, GX, 0, 0, tiled=True)
    gains = jnp.tile(jnp.concatenate([norm_scale, norm_shift], axis=0), (1, 2))
    near_side = swap(
        jnp.concatenate([edge(above[:channels]), edge(pair_feats), edge(below[:channels])], axis=1)
    )

    taps_shape = VMEM(first_taps.shape, bf16)
    whole = (STEP, cols, LANES)
    part = (STEP // 2, cols, LANES)
    wide = (STEP, cols + 2 * STEP, LANES)
    products = VMEM((2, cols + 2 * STEP, 3 * LANES), f32)
    sums = (devices, LANES)
    own_rows, conv_own, own_give, conv_down, conv_up, edges, stats = call(
        functools.partial(first_kernel, devices),
        (
            (HBM, whole, bf16),
            (HBM, whole, bf16),
            (HBM, part, bf16),
            (HBM, part, bf16),
            (HBM, part, bf16),
            (VMEM, (STEP, 2 * STEP, LANES), bf16),
            (VMEM, sums, f32),
        ),
        [
            VMEM(wide, bf16),
            VMEM(wide, bf16),
            VMEM(whole, bf16),
            products,
            VMEM(part, bf16),
            VMEM(part, bf16),
            VMEM(pair_feats.shape, bf16),
            VMEM(eight, bf16),
            VMEM(eight, bf16),
            taps_shape,
            flat_of(channels, rows, cols),
            flat_of(channels, STEP, cols),
            flat_of(channels, STEP, cols),
            flat_of(channels, rows + 2 * STEP, LANES),
            VMEM(wide[1:], f32),
            VMEM((2, STEP, LANES), f32),
        ],
        9,
        conv_flops,
        ((HBM, pair_feats), (HBM, above), (HBM, below), (VMEM, near_side), (VMEM, terms),
         (VMEM, mine), (HBM, first_taps)),
    )
    conv_above, conv_below = down(conv_down), up(conv_up)
    stats = lax.all_to_all(stats, GX, 0, 0, tiled=True)
    stats_other = swap(stats)
    edges = swap(edges)
    last = cols - 2 * STEP
    corners = swap(
        jnp.stack(
            [jnp.where(first_core, x[:, last:], x[:, : 2 * STEP]) for x in (conv_above, conv_below)]
        )
    )
    own_other = swap(own_give)
    conv_second, second_give, stats = call(
        functools.partial(second_kernel, devices, cells),
        ((HBM, whole, bf16), (HBM, part, bf16), (VMEM, sums, f32)),
        [
            VMEM(wide, bf16),
            VMEM(wide, bf16),
            VMEM(whole, bf16),
            products,
            VMEM(whole, bf16),
            VMEM(part, bf16),
            VMEM(part, bf16),
            taps_shape,
        ],
        4,
        conv_flops,
        ((HBM, conv_own), (HBM, conv_above), (HBM, conv_below), (VMEM, edges),
         (VMEM, corners), (VMEM, stats), (VMEM, stats_other), (VMEM, gains),
         (HBM, second_taps)),
    )
    stats = lax.all_to_all(stats, GX, 0, 0, tiled=True)
    stats_other = swap(stats)
    conv_other = swap(second_give)
    block_out, send = call(
        functools.partial(pack_kernel, cells),
        ((HBM, whole, bf16), (VMEM, (devices, STEP // 2, rows, LANES), bf16)),
        [
            VMEM(whole, bf16),
            VMEM(whole, bf16),
            VMEM(whole, bf16),
        ],
        3,
        conv_flops,
        ((HBM, own_rows), (VMEM, own_other), (HBM, conv_second), (VMEM, conv_other),
         (VMEM, stats), (VMEM, stats_other), (VMEM, gains)),
    )
    received = lax.all_to_all(send, GX, 0, 0, tiled=True)
    peers = devices // cores
    other = swap(jnp.where(first_core, received[peers:], received[:peers]))
    return call(
        merge_kernel,
        ((HBM, pair_feats.shape, bf16),),
        [
            VMEM(pair_feats.shape, bf16),
            VMEM(whole, bf16),
            VMEM((peers, cores, STEP // 2, rows, LANES), f32),
            flat_of(channels, rows, cols),
        ],
        3,
        conv_flops,
        ((HBM, block_out), (VMEM, received), (VMEM, other)),
    )[0]


def solution(mesh):
    torus = Mesh(
        mesh.devices.reshape(mesh.shape["grp"], 4, 16, mesh.shape["gy"]),
        ("grp", "gx_0", "gx_1", "gy"),
    )
    placed = (P(GRP_GX, None), P(None, GRP_GX, "gy"), P(), P(), P(), P(), P(), P())
    return jax.shard_map(
        body, mesh=torus, in_specs=placed, out_specs=P(None, GRP_GX, "gy"), check_vma=False
    )
```

```python
import functools

import jax
import jax.numpy as jnp
from jax import lax
from jax.experimental import pallas as pl
from jax.experimental.pallas import tpu as pltpu
from jax.sharding import Mesh
from jax.sharding import PartitionSpec as P

STEP = 8
GX = ("gx_0", "gx_1")
GRP_GX = ("grp", "gx_0", "gx_1")
LANES = 128
SWAP = [(0, 1), (1, 0)]
HBM, VMEM = pltpu.HBM, pltpu.VMEM

epsilon = 1e-05


def pairs_of(count, first):
    return [p for i in range(first, count - 1, 2) for p in ((i, i + 1), (i + 1, i))]


def call(kernel, outs, scratch, n_copies, flops, operands):
    spaces = [space for space, _ in operands]
    held = [pltpu.with_memory_space_constraint(x, space) for space, x in operands]
    return pl.pallas_call(
        kernel,
        out_shape=[space(shape, dtype) for space, shape, dtype in outs],
        in_specs=[pl.BlockSpec(memory_space=space) for space in spaces],
        out_specs=[pl.BlockSpec(memory_space=space) for space, _, _ in outs],
        scratch_shapes=[*scratch, pltpu.SemaphoreType.DMA((n_copies,))],
        cost_estimate=pl.CostEstimate(flops=flops, bytes_accessed=1 << 20, transcendentals=0),
        compiler_params=pltpu.CompilerParams(vmem_limit_bytes=24 << 20),
    )(*held)


def start_all(sem, first, pairs):
    copies = [
        pltpu.make_async_copy(src, dst, sem.at[first + i]) for i, (src, dst) in enumerate(pairs)
    ]
    for copy in copies:
        copy.start()
    return copies


def wait_all(copies):
    for copy in copies:
        copy.wait()


def elu(v):
    return jnp.where(v > 0, v, jnp.exp(jnp.minimum(v, 0.0)) - 1.0)


def as_float(flag):
    return jnp.asarray(flag, jnp.int32).astype(jnp.float32)


def lane_half(rows):
    return lax.broadcasted_iota(jnp.int32, (rows, LANES), 1) < LANES // 2


def halves(first, second):
    return jnp.where(lane_half(first.shape[0]), first, pltpu.roll(second, LANES // 2, 1))


def reach_mask(core):
    row = lax.broadcasted_iota(jnp.int32, (2 * STEP, LANES), 0)
    first = STEP * core
    return (row >= first) & (row < first + STEP)


def inside_of(row_at, devices):
    above = as_float(jnp.minimum(row_at, 1))
    below = as_float(jnp.minimum(devices - 1 - row_at, 1))
    return jnp.where(lane_half(1), above, below)


def flat_of(channels, rows, cols):
    return pltpu.VMEM((cols // LANES, channels * rows, LANES), jnp.float32)


def widen(source_ref, flat_ref):
    channels, rows, cols = source_ref.shape
    some = 64 // rows

    def step(i, _):
        for block in range(cols // LANES):
            value = source_ref[pl.ds(i * some, some), :, block * LANES : (block + 1) * LANES]
            flat_ref[block, pl.ds(pl.multiple_of(i * some * rows, 8), some * rows), :] = (
                value.astype(jnp.float32).reshape(some * rows, LANES)
            )
        return 0

    lax.fori_loop(0, channels // some, step, 0)


def fill_rows(x_ref, sources, side_sources, row_terms, col_terms, scale, core, mask):
    cols = col_terms.shape[0] - 2 * STEP
    channels = LANES // 2

    def pair(sources, block, i):
        return jnp.transpose(
            jnp.concatenate(
                [
                    flat[block, pl.ds(first + i, channels, stride=rows), :]
                    for flat, first, rows in sources
                ],
                axis=0,
            )
        )

    def step(i, _):
        row = row_terms[pl.ds(i, 1), :]
        for block in range(cols // LANES):
            at = slice(block * LANES, (block + 1) * LANES)
            value = pair(sources, block, i) + (row + col_terms[at, :])
            if scale is not None:
                value = value * scale
            x_ref[i, at, :] = value.astype(jnp.bfloat16)
        side = pair(side_sources, 0, i)
        value = jnp.where(core == 0, side[: 2 * STEP], side[LANES - 2 * STEP :])
        value = value + (row + col_terms[cols:, :])
        if scale is not None:
            value = value * scale
        x_ref[i, cols:, :] = jnp.where(mask, value, 0.0).astype(jnp.bfloat16)
        return 0

    lax.fori_loop(0, STEP, step, 0)


def weights_of(taps_ref, wanted):
    channels = taps_ref.shape[1]
    zero = jnp.zeros((channels, channels), jnp.bfloat16)
    return jnp.concatenate(
        [
            jnp.concatenate(
                [zero if ky is None else taps_ref[3 * ky + kx] for ky in inputs], axis=1
            )
            for kx in range(3)
            for inputs in wanted
        ],
        axis=0,
    )


OWN_TAPS = ((1, 2, 0, None), (0, 1, None, 2))


def product(values, weights):
    return lax.dot_general(
        values, weights, (((1,), (1,)), ((), ())), preferred_element_type=jnp.float32
    )


def shifted_sum(p_ref, first):
    last = p_ref.shape[0]
    if first == 0:
        left = jnp.concatenate([p_ref[last - STEP :, :LANES], p_ref[: LANES - STEP, :LANES]], axis=0)
    else:
        left = p_ref[first - STEP : first - STEP + LANES, :LANES]
    centre = p_ref[first : first + LANES, LANES : 2 * LANES]
    right = p_ref[first + STEP : first + STEP + LANES, 2 * LANES :]
    return left + centre + right


def conv_own_rows(own_ref, near_ref, weights, p_ref, out_ref):
    cols = out_ref.shape[1]
    total = jnp.zeros((STEP, LANES), jnp.float32)
    squares = total
    for i in range(STEP):
        p = p_ref.at[i % 2]
        p[...] = product(jnp.concatenate([own_ref[i], near_ref[i]], axis=1), weights)
        for first in range(0, cols, LANES):
            value = shifted_sum(p, first)
            out_ref[i, first : first + LANES, :] = value.astype(jnp.bfloat16)
            value = value.reshape(LANES // STEP, STEP, LANES)
            total = total + jnp.sum(value, axis=0)
            squares = squares + jnp.sum(value * value, axis=0)
    total = total + pltpu.roll(total, LANES // 2, 1)
    squares = squares + pltpu.roll(squares, LANES // 2, 1)
    return jnp.sum(jnp.where(lane_half(STEP), total, squares), axis=0, keepdims=True)


def affine_of(which, stats_refs, gains_ref, cells):
    row = sum(jnp.sum(ref[...], axis=0, keepdims=True) for ref in stats_refs) / cells
    row = jnp.broadcast_to(row, (STEP, LANES))
    other = pltpu.roll(row, LANES // 2, 1)
    average = jnp.where(lane_half(STEP), row, other)
    spread = jnp.where(lane_half(STEP), other, row) - average * average
    factor = gains_ref[which : which + 1] * lax.rsqrt(spread + epsilon)
    offset = gains_ref[2 + which : 3 + which] - average * factor
    return factor[0:1], offset[0:1]


def prepare_kernel(
    pair, feats, w_row, w_col, one, two, col_terms, row_terms, feats_in, row_in, col_in, sem
):
    odd = lax.rem(lax.axis_index(GX), 2)
    channels = pair.shape[0]
    lower, upper = pl.multiple_of(STEP * (1 - odd), STEP), pl.multiple_of(STEP * odd, STEP)
    parts = start_all(
        sem, 0,
        ((pair.at[:, pl.ds(lower, STEP)], one.at[pl.ds(0, channels)]),
         (pair.at[:, pl.ds(upper, STEP)], two.at[pl.ds(0, channels)])),
    )
    inputs = start_all(sem, 2, ((feats, feats_in), (w_row, row_in), (w_col, col_in)))
    wait_all(inputs)
    zero = jnp.zeros((2 * STEP, LANES - channels), jnp.float32)
    row = jnp.concatenate([product(feats_in[...], row_in[...]), zero], axis=1)
    col = jnp.concatenate([product(feats_in[...], col_in[...]), zero], axis=1)
    packed = halves(col[:STEP], col[STEP:]).astype(jnp.bfloat16)
    col_terms[...] = jnp.broadcast_to(packed[None], col_terms.shape)
    row_terms[...] = halves(row[:STEP], row[STEP:])
    empty = jnp.zeros((STEP, one.shape[2] - LANES), jnp.float32)
    for ref, which in ((one, odd), (two, 1 - odd)):
        rows = jnp.where(which == 0, row[STEP:], row[:STEP])
        ref[channels] = jnp.concatenate([rows, empty], axis=1).astype(jnp.bfloat16)
    wait_all(parts)


def first_kernel(
    devices, own_in, one_in, two_in, side, terms, mine, taps_in,
    own_out, conv_out, give_out, one_out, two_out, edge_ref, stats_ref,
    x_own, x_near, conv_ref, p_ref, border_ref, own, halo, taps,
    own_flat, above_flat, below_flat, side_flat, col_terms, row_terms, sem,
):
    row_at, core = lax.axis_index(GX), lax.axis_index("gy")
    channels, rows, cols = own.shape
    half = STEP // 2
    odd = lax.rem(row_at, 2)
    inputs = start_all(
        sem, 0,
        ((own_in, own), (one_in, halo.at[1 - odd]), (two_in, halo.at[odd]), (taps_in, taps)),
    )
    above, below = halo.at[0], halo.at[1]

    def put_terms(source, at):
        value = terms[source].astype(jnp.float32)
        other = pltpu.roll(value, LANES // 2, 1)
        col_terms[pl.ds(at, STEP), :] = jnp.where(lane_half(STEP), value, other)
        col_terms[pl.ds(at + STEP, STEP), :] = jnp.where(lane_half(STEP), other, value)

    peers = cols // rows

    def put_own(i, _):
        put_terms(peers * core + i, pl.multiple_of(i * rows, 2 * STEP))
        return 0

    lax.fori_loop(0, peers, put_own, 0)
    put_terms(peers - core, cols)
    row_terms[0] = mine[...].astype(jnp.bfloat16).astype(jnp.float32)
    mask = reach_mask(core)
    tall = rows + 2 * STEP
    above_at, below_at = (STEP + rows) * (1 - odd), (STEP + rows) * odd
    widen(side, side_flat)
    inputs[0].wait()
    widen(own, own_flat)
    fill_rows(
        x_own, ((own_flat, 0, rows), (own_flat, STEP, rows)),
        ((side_flat, STEP, tall), (side_flat, 2 * STEP, tall)),
        row_terms.at[0], col_terms, None, core, mask,
    )
    given = x_own.at[pl.ds(half * (1 - core), half), pl.ds(0, cols)]
    outputs = start_all(sem, 4, ((x_own.at[:, pl.ds(0, cols)], own_out), (given, give_out)))
    wait_all(inputs[1:3])
    widen(above.at[pl.ds(0, channels)], above_flat)
    widen(below.at[pl.ds(0, channels)], below_flat)
    row_terms[1] = halves(
        above[channels, :, :LANES].astype(jnp.float32),
        below[channels, :, :LANES].astype(jnp.float32),
    )
    fill_rows(
        x_near, ((above_flat, 0, STEP), (below_flat, 0, STEP)),
        ((side_flat, above_at, tall), (side_flat, below_at, tall)),
        row_terms.at[1], col_terms, inside_of(row_at, devices), core, mask,
    )
    inputs[3].wait()
    stats = conv_own_rows(x_own, x_near, weights_of(taps, OWN_TAPS), p_ref, conv_ref)
    outputs += start_all(sem, 6, ((conv_ref, conv_out),))
    lower = lane_half(LANES)
    for i in range(half):
        for first in range(0, cols, LANES):
            at = slice(first, first + LANES)
            one = conv_ref[i, at, :].astype(jnp.float32)
            two = conv_ref[i + half, at, :].astype(jnp.float32)
            up = jnp.where(lower, one, pltpu.roll(two, LANES // 2, 1))
            down = jnp.where(lower, pltpu.roll(one, LANES // 2, 1), two)
            border_ref[0, i, at, :] = up.astype(jnp.bfloat16)
            border_ref[1, i, at, :] = down.astype(jnp.bfloat16)
    outputs += start_all(
        sem, 7, ((border_ref.at[1 - odd], one_out), (border_ref.at[odd], two_out))
    )
    edge_at = pl.multiple_of((cols - 2 * STEP) * (1 - core), 2 * STEP)
    edge_ref[...] = conv_ref[:, pl.ds(edge_at, 2 * STEP), :]
    stats_ref[...] = jnp.broadcast_to(stats, stats_ref.shape)
    wait_all(outputs)


def second_kernel(
    devices, cells, own_in, one_in, two_in, edge, corner, stats, stats_other, gains, taps_in,
    conv_out, give_out, stats_ref,
    a_own, a_near, conv_ref, p_ref, own, halo, taps, sem,
):
    row_at, core = lax.axis_index(GX), lax.axis_index("gy")
    cols = own.shape[1]
    half = STEP // 2
    odd = lax.rem(row_at, 2)
    inputs = start_all(
        sem, 0,
        ((own_in, own), (one_in, halo.at[1 - odd]), (two_in, halo.at[odd]), (taps_in, taps)),
    )
    factor, offset = affine_of(0, (stats, stats_other), gains, cells)
    inside = inside_of(row_at, devices)
    mask = reach_mask(core)

    def activated(value):
        return elu(value.astype(jnp.float32) * factor + offset)

    def fill_own(i, _):
        for first in range(0, cols, LANES):
            at = slice(first, first + LANES)
            a_own[i, at, :] = activated(own[i, at, :]).astype(jnp.bfloat16)
        beyond = jnp.where(mask, activated(edge[i]), 0.0)
        a_own[i, cols:, :] = beyond.astype(jnp.bfloat16)
        return 0

    def two_rows(up, down):
        up, down = up.astype(jnp.float32), down.astype(jnp.float32)
        lower = lane_half(up.shape[0])
        return (
            jnp.where(lower, up, pltpu.roll(down, LANES // 2, 1)),
            jnp.where(lower, pltpu.roll(up, LANES // 2, 1), down),
        )

    def fill_near(i, _):
        for first in range(0, cols, LANES):
            at = slice(first, first + LANES)
            for k, value in enumerate(two_rows(halo[0, i, at, :], halo[1, i, at, :])):
                a_near[i + half * k, at, :] = (activated(value) * inside).astype(jnp.bfloat16)
        for k, value in enumerate(two_rows(corner[1 - odd, i], corner[odd, i])):
            beyond = jnp.where(mask, activated(value) * inside, 0.0)
            a_near[i + half * k, cols:, :] = beyond.astype(jnp.bfloat16)
        return 0

    inputs[0].wait()
    lax.fori_loop(0, STEP, fill_own, 0)
    wait_all(inputs[1:])
    lax.fori_loop(0, half, fill_near, 0)
    stats = conv_own_rows(a_own, a_near, weights_of(taps, OWN_TAPS), p_ref, conv_ref)
    given = conv_ref.at[pl.ds(half * (1 - core), half)]
    outputs = start_all(sem, 0, ((given, give_out), (conv_ref, conv_out)))
    stats_ref[...] = jnp.broadcast_to(stats, stats_ref.shape)
    wait_all(outputs)


def pack_kernel(
    cells, block_in, other, conv_in, conv_other, stats, stats_other, gains,
    block_out_out, send_ref,
    out_ref, own, conv, sem,
):
    core = lax.axis_index("gy")
    cols = conv.shape[1]
    half = STEP // 2
    inputs = start_all(sem, 0, ((block_in, own), (conv_in, conv)))
    factor, offset = affine_of(1, (stats, stats_other), gains, cells)
    wide = 2 * STEP
    peers, some = cols // wide, LANES // wide

    def block_out(x, value):
        value = x.astype(jnp.float32) + value.astype(jnp.float32) * factor + offset
        return elu(value).astype(jnp.bfloat16)

    def mine(i, _):
        for first in range(0, cols, LANES):
            at = slice(first, first + LANES)
            out_ref[i, at, :] = block_out(own[i, at, :], conv[i, at, :])
        return 0

    wait_all(inputs[:2])
    lax.fori_loop(0, STEP, mine, 0)
    outputs = start_all(sem, 2, ((out_ref, block_out_out),))

    def step(i, _):
        for first in range(0, cols, LANES):
            at = slice(first, first + LANES)
            value = out_ref[half * core + i, at, :].reshape(some, wide, LANES)
            send_ref[pl.ds(peers * core + first // wide, some), i] = value
            value = block_out(other[i, at, :], conv_other[i, at, :]).reshape(some, wide, LANES)
            send_ref[pl.ds(peers * (1 - core) + first // wide, some), i] = value
        return 0

    lax.fori_loop(0, half, step, 0)
    wait_all(outputs)


def merge_kernel(own_in, received, other, result, out_ref, own, cells_ref, flat_ref, sem):
    core = lax.axis_index("gy")
    channels, rows, cols = out_ref.shape
    peers = other.shape[0]
    inputs = start_all(sem, 0, ((own_in, own),))

    def gather(s, _):
        cells_ref[s, core] = received[peers * core + s].astype(jnp.float32)
        cells_ref[s, 1 - core] = other[s].astype(jnp.float32)
        return 0

    lax.fori_loop(0, peers, gather, 0)
    wait_all(inputs)
    flat = cells_ref.reshape(peers * STEP * rows, LANES)
    some = LANES // rows
    lower = lane_half(some * STEP)

    def step(i, _):
        for block in range(cols // LANES):
            first = block * some * STEP * rows
            upper_row = flat[pl.ds(first + i, some * STEP, stride=rows), :]
            lower_row = flat[pl.ds(first + STEP + i, some * STEP, stride=rows), :]
            even = jnp.where(lower, upper_row, pltpu.roll(lower_row, channels, 1))
            odd = jnp.where(lower, pltpu.roll(upper_row, channels, 1), lower_row)
            mirrored = jnp.concatenate(
                [
                    part[s * STEP : (s + 1) * STEP]
                    for s in range(some)
                    for part in (even, odd)
                ],
                axis=0,
            )
            value = own[i, block * LANES : (block + 1) * LANES, :].astype(jnp.float32) + mirrored
            value = jnp.transpose(0.5 * value)
            for high in range(rows // STEP):
                flat_ref[block, pl.ds(high * STEP + i, channels, stride=rows), :] = value[
                    channels * high : channels * (high + 1)
                ]
        return 0

    lax.fori_loop(0, STEP, step, 0)

    def store(c, _):
        for block in range(cols // LANES):
            value = flat_ref[block, pl.ds(pl.multiple_of(c * rows, 8), rows), :]
            out_ref[c, :, block * LANES : (block + 1) * LANES] = value.astype(jnp.bfloat16)
        return 0

    part = channels // 2
    lax.fori_loop(0, part, store, 0)
    outputs = start_all(sem, 1, ((out_ref.at[pl.ds(0, part)], result.at[pl.ds(0, part)]),))
    lax.fori_loop(part, channels, store, 0)
    outputs += start_all(sem, 2, ((out_ref.at[pl.ds(part, part)], result.at[pl.ds(part, part)]),))
    wait_all(outputs)


def body(residue_feats, pair_feats, w_row, w_col, first_taps, second_taps, norm_scale, norm_shift):
    channels, rows, cols = pair_feats.shape
    cores = lax.axis_size("gy")
    devices = lax.axis_size(GX)
    first_core = lax.axis_index("gy") == 0
    cells = devices * rows * cores * cols
    bf16, f32 = jnp.bfloat16, jnp.float32
    conv_flops = 2 * 9 * channels * channels * rows * cols

    def edge(x):
        return jnp.where(first_core, x[..., cols - LANES :], x[..., :LANES])

    def swap(x):
        return lax.ppermute(x, "gy", SWAP)

    with_next = functools.partial(lax.ppermute, axis_name=GX, perm=pairs_of(devices, 0))
    with_last = functools.partial(lax.ppermute, axis_name=GX, perm=pairs_of(devices, 1))
    eight = (channels + 1, STEP, cols)
    one, two, terms, mine = call(
        prepare_kernel,
        (
            (VMEM, eight, bf16),
            (VMEM, eight, bf16),
            (VMEM, (devices, STEP, LANES), bf16),
            (VMEM, (STEP, LANES), f32),
        ),
        [
            VMEM(residue_feats.shape, bf16),
            VMEM(w_row.T.shape, bf16),
            VMEM(w_col.T.shape, bf16),
        ],
        5,
        conv_flops // 16,
        ((HBM, pair_feats), (HBM, residue_feats), (HBM, w_row.T), (HBM, w_col.T)),
    )
    one, two = with_next(one), with_last(two)
    terms = lax.all_to_all(terms, GX, 0, 0, tiled=True)
    gains = jnp.tile(jnp.concatenate([norm_scale, norm_shift], axis=0), (1, 2))
    near_side = swap(
        jnp.concatenate(
            [edge(one[:channels]), edge(pair_feats), edge(two[:channels])], axis=1
        )
    )

    taps_shape = VMEM(first_taps.shape, bf16)
    whole = (STEP, cols, LANES)
    part = (STEP // 2, cols, LANES)
    wide = (STEP, cols + 2 * STEP, LANES)
    products = VMEM((2, cols + 2 * STEP, 3 * LANES), f32)
    sums = (devices, LANES)
    own_rows, conv_own, own_give, conv_one, conv_two, edges, stats = call(
        functools.partial(first_kernel, devices),
        (
            (HBM, whole, bf16),
            (HBM, whole, bf16),
            (HBM, part, bf16),
            (HBM, part, bf16),
            (HBM, part, bf16),
            (VMEM, (STEP, 2 * STEP, LANES), bf16),
            (VMEM, sums, f32),
        ),
        [
            VMEM(wide, bf16),
            VMEM(wide, bf16),
            VMEM(whole, bf16),
            products,
            VMEM((2, *part), bf16),
            VMEM(pair_feats.shape, bf16),
            VMEM((2, *eight), bf16),
            taps_shape,
            flat_of(channels, rows, cols),
            flat_of(channels, STEP, cols),
            flat_of(channels, STEP, cols),
            flat_of(channels, rows + 2 * STEP, LANES),
            VMEM(wide[1:], f32),
            VMEM((2, STEP, LANES), f32),
        ],
        9,
        conv_flops,
        ((HBM, pair_feats), (HBM, one), (HBM, two), (VMEM, near_side), (VMEM, terms),
         (VMEM, mine), (HBM, first_taps)),
    )
    conv_one, conv_two = with_next(conv_one), with_last(conv_two)
    stats = lax.all_to_all(stats, GX, 0, 0, tiled=True)
    stats_other = swap(stats)
    edges = swap(edges)
    last = cols - 2 * STEP
    corners = swap(
        jnp.stack(
            [
                jnp.where(first_core, x[:, last:], x[:, : 2 * STEP])
                for x in (conv_one, conv_two)
            ]
        )
    )
    own_other = swap(own_give)
    conv_second, second_give, stats = call(
        functools.partial(second_kernel, devices, cells),
        ((HBM, whole, bf16), (HBM, part, bf16), (VMEM, sums, f32)),
        [
            VMEM(wide, bf16),
            VMEM(wide, bf16),
            VMEM(whole, bf16),
            products,
            VMEM(whole, bf16),
            VMEM((2, *part), bf16),
            taps_shape,
        ],
        4,
        conv_flops,
        ((HBM, conv_own), (HBM, conv_one), (HBM, conv_two), (VMEM, edges),
         (VMEM, corners), (VMEM, stats), (VMEM, stats_other), (VMEM, gains),
         (HBM, second_taps)),
    )
    stats = lax.all_to_all(stats, GX, 0, 0, tiled=True)
    stats_other = swap(stats)
    conv_other = swap(second_give)
    block_out, send = call(
        functools.partial(pack_kernel, cells),
        ((HBM, whole, bf16), (VMEM, (devices, STEP // 2, rows, LANES), bf16)),
        [
            VMEM(whole, bf16),
            VMEM(whole, bf16),
            VMEM(whole, bf16),
        ],
        3,
        conv_flops,
        ((HBM, own_rows), (VMEM, own_other), (HBM, conv_second), (VMEM, conv_other),
         (VMEM, stats), (VMEM, stats_other), (VMEM, gains)),
    )
    received = lax.all_to_all(send, GX, 0, 0, tiled=True)
    peers = devices // cores
    other = swap(jnp.where(first_core, received[peers:], received[:peers]))
    return call(
        merge_kernel,
        ((HBM, pair_feats.shape, bf16),),
        [
            VMEM(pair_feats.shape, bf16),
            VMEM(whole, bf16),
            VMEM((peers, cores, STEP // 2, rows, LANES), f32),
            flat_of(channels, rows, cols),
        ],
        3,
        conv_flops,
        ((HBM, block_out), (VMEM, received), (VMEM, other)),
    )[0]


def solution(mesh):
    torus = Mesh(
        mesh.devices.reshape(mesh.shape["grp"], 4, 16, mesh.shape["gy"]),
        ("grp", "gx_0", "gx_1", "gy"),
    )
    placed = (P(GRP_GX, None), P(None, GRP_GX, "gy"), P(), P(), P(), P(), P(), P())
    return jax.shard_map(
        body, mesh=torus, in_specs=placed, out_specs=P(None, GRP_GX, "gy"), check_vma=False
    )
```

```python
import functools

import jax
import jax.numpy as jnp
from jax import lax
from jax.experimental import pallas as pl
from jax.experimental.pallas import tpu as pltpu
from jax.sharding import Mesh
from jax.sharding import PartitionSpec as P

STEP = 8
GX = ("gx_0", "gx_1")
GRP_GX = ("grp", "gx_0", "gx_1")
LANES = 128
SWAP = [(0, 1), (1, 0)]
HBM, VMEM = pltpu.HBM, pltpu.VMEM

epsilon = 1e-05


def pairs_of(count, first):
    return [p for i in range(first, count - 1, 2) for p in ((i, i + 1), (i + 1, i))]


def call(kernel, outs, scratch, n_copies, flops, operands):
    spaces = [space for space, _ in operands]
    held = [pltpu.with_memory_space_constraint(x, space) for space, x in operands]
    return pl.pallas_call(
        kernel,
        out_shape=[space(shape, dtype) for space, shape, dtype in outs],
        in_specs=[pl.BlockSpec(memory_space=space) for space in spaces],
        out_specs=[pl.BlockSpec(memory_space=space) for space, _, _ in outs],
        scratch_shapes=[*scratch, pltpu.SemaphoreType.DMA((n_copies,))],
        cost_estimate=pl.CostEstimate(flops=flops, bytes_accessed=1 << 20, transcendentals=0),
        compiler_params=pltpu.CompilerParams(vmem_limit_bytes=24 << 20),
    )(*held)


def start_all(sem, first, pairs):
    copies = [
        pltpu.make_async_copy(src, dst, sem.at[first + i]) for i, (src, dst) in enumerate(pairs)
    ]
    for copy in copies:
        copy.start()
    return copies


def wait_all(copies):
    for copy in copies:
        copy.wait()


def elu(v):
    return jnp.where(v > 0, v, jnp.exp(jnp.minimum(v, 0.0)) - 1.0)


def as_float(flag):
    return jnp.asarray(flag, jnp.int32).astype(jnp.float32)


def lane_half(rows):
    return lax.broadcasted_iota(jnp.int32, (rows, LANES), 1) < LANES // 2


def halves(first, second):
    return jnp.where(lane_half(first.shape[0]), first, pltpu.roll(second, LANES // 2, 1))


def reach_mask(core):
    row = lax.broadcasted_iota(jnp.int32, (2 * STEP, LANES), 0)
    first = STEP * core
    return (row >= first) & (row < first + STEP)


def inside_of(row_at, devices):
    above = as_float(jnp.minimum(row_at, 1))
    below = as_float(jnp.minimum(devices - 1 - row_at, 1))
    return jnp.where(lane_half(1), above, below)


def flat_of(channels, rows, cols):
    return pltpu.VMEM((cols // LANES, channels * rows, LANES), jnp.float32)


def widen(source_ref, flat_ref):
    channels, rows, cols = source_ref.shape
    some = 64 // rows

    def step(i, _):
        for block in range(cols // LANES):
            value = source_ref[pl.ds(i * some, some), :, block * LANES : (block + 1) * LANES]
            flat_ref[block, pl.ds(pl.multiple_of(i * some * rows, 8), some * rows), :] = (
                value.astype(jnp.float32).reshape(some * rows, LANES)
            )
        return 0

    lax.fori_loop(0, channels // some, step, 0)


def two_rows_turned(sources, block, i):
    channels = LANES // 2
    return jnp.transpose(
        jnp.concatenate(
            [
                flat[block, pl.ds(first + i, channels, stride=rows), :]
                for flat, first, rows in sources
            ],
            axis=0,
        )
    )


def turn_rows(out_ref, sources):
    def step(i, _):
        for block in range(out_ref.shape[1] // LANES):
            at = slice(block * LANES, (block + 1) * LANES)
            out_ref[i, at, :] = two_rows_turned(sources, block, i).astype(jnp.bfloat16)
        return 0

    lax.fori_loop(0, STEP, step, 0)


def add_terms(x_ref, raw_ref, side_sources, row_terms, col_terms, scale, core, mask):
    cols = raw_ref.shape[1]

    def step(i, _):
        row = row_terms[pl.ds(i, 1), :]
        for block in range(cols // LANES):
            at = slice(block * LANES, (block + 1) * LANES)
            value = raw_ref[i, at, :].astype(jnp.float32) + (row + col_terms[at, :])
            if scale is not None:
                value = value * scale
            x_ref[i, at, :] = value.astype(jnp.bfloat16)
        side = two_rows_turned(side_sources, 0, i)
        value = jnp.where(core == 0, side[: 2 * STEP], side[LANES - 2 * STEP :])
        value = value + (row + col_terms[cols:, :])
        if scale is not None:
            value = value * scale
        x_ref[i, cols:, :] = jnp.where(mask, value, 0.0).astype(jnp.bfloat16)
        return 0

    lax.fori_loop(0, STEP, step, 0)


def weights_of(taps_ref, wanted):
    channels = taps_ref.shape[1]
    zero = jnp.zeros((channels, channels), jnp.bfloat16)
    return jnp.concatenate(
        [
            jnp.concatenate(
                [zero if ky is None else taps_ref[3 * ky + kx] for ky in inputs], axis=1
            )
            for kx in range(3)
            for inputs in wanted
        ],
        axis=0,
    )


OWN_TAPS = ((1, 2, 0, None), (0, 1, None, 2))


def product(values, weights):
    return lax.dot_general(
        values, weights, (((1,), (1,)), ((), ())), preferred_element_type=jnp.float32
    )


def shifted_sum(p_ref, first):
    last = p_ref.shape[0]
    if first == 0:
        left = jnp.concatenate([p_ref[last - STEP :, :LANES], p_ref[: LANES - STEP, :LANES]], axis=0)
    else:
        left = p_ref[first - STEP : first - STEP + LANES, :LANES]
    centre = p_ref[first : first + LANES, LANES : 2 * LANES]
    right = p_ref[first + STEP : first + STEP + LANES, 2 * LANES :]
    return left + centre + right


def conv_own_rows(own_ref, near_ref, weights, p_ref, out_ref):
    cols = out_ref.shape[1]
    total = jnp.zeros((STEP, LANES), jnp.float32)
    squares = total
    for i in range(STEP):
        p = p_ref.at[i % 2]
        p[...] = product(jnp.concatenate([own_ref[i], near_ref[i]], axis=1), weights)
        for first in range(0, cols, LANES):
            value = shifted_sum(p, first)
            out_ref[i, first : first + LANES, :] = value.astype(jnp.bfloat16)
            value = value.reshape(LANES // STEP, STEP, LANES)
            total = total + jnp.sum(value, axis=0)
            squares = squares + jnp.sum(value * value, axis=0)
    total = total + pltpu.roll(total, LANES // 2, 1)
    squares = squares + pltpu.roll(squares, LANES // 2, 1)
    return jnp.sum(jnp.where(lane_half(STEP), total, squares), axis=0, keepdims=True)


def affine_of(which, stats_refs, gains_ref, cells):
    row = sum(jnp.sum(ref[...], axis=0, keepdims=True) for ref in stats_refs) / cells
    row = jnp.broadcast_to(row, (STEP, LANES))
    other = pltpu.roll(row, LANES // 2, 1)
    average = jnp.where(lane_half(STEP), row, other)
    spread = jnp.where(lane_half(STEP), other, row) - average * average
    factor = gains_ref[which : which + 1] * lax.rsqrt(spread + epsilon)
    offset = gains_ref[2 + which : 3 + which] - average * factor
    return factor[0:1], offset[0:1]


def prepare_kernel(
    pair, feats, w_row, w_col, one, two, col_terms, row_terms, feats_in, row_in, col_in, sem
):
    odd = lax.rem(lax.axis_index(GX), 2)
    channels = pair.shape[0]
    lower, upper = pl.multiple_of(STEP * (1 - odd), STEP), pl.multiple_of(STEP * odd, STEP)
    parts = start_all(
        sem, 0,
        ((pair.at[:, pl.ds(lower, STEP)], one.at[pl.ds(0, channels)]),
         (pair.at[:, pl.ds(upper, STEP)], two.at[pl.ds(0, channels)])),
    )
    inputs = start_all(sem, 2, ((feats, feats_in), (w_row, row_in), (w_col, col_in)))
    wait_all(inputs)
    zero = jnp.zeros((2 * STEP, LANES - channels), jnp.float32)
    row = jnp.concatenate([product(feats_in[...], row_in[...]), zero], axis=1)
    col = jnp.concatenate([product(feats_in[...], col_in[...]), zero], axis=1)
    packed = halves(col[:STEP], col[STEP:]).astype(jnp.bfloat16)
    col_terms[...] = jnp.broadcast_to(packed[None], col_terms.shape)
    row_terms[...] = halves(row[:STEP], row[STEP:])
    empty = jnp.zeros((STEP, one.shape[2] - LANES), jnp.float32)
    for ref, which in ((one, odd), (two, 1 - odd)):
        rows = jnp.where(which == 0, row[STEP:], row[:STEP])
        ref[channels] = jnp.concatenate([rows, empty], axis=1).astype(jnp.bfloat16)
    wait_all(parts)


def turn_kernel(
    pair, one, two, own_ref, near_ref, row_terms, own, own_flat, above_flat, below_flat, sem
):
    odd = lax.rem(lax.axis_index(GX), 2)
    channels, rows, _ = own.shape
    inputs = start_all(sem, 0, ((pair, own),))
    one_rows, two_rows = one.at[pl.ds(0, channels)], two.at[pl.ds(0, channels)]

    @pl.when(odd == 0)
    def _():
        widen(two_rows, above_flat)
        widen(one_rows, below_flat)

    @pl.when(odd == 1)
    def _():
        widen(one_rows, above_flat)
        widen(two_rows, below_flat)

    one_terms = one[channels, :, :LANES].astype(jnp.float32)
    two_terms = two[channels, :, :LANES].astype(jnp.float32)
    row_terms[...] = halves(
        jnp.where(odd == 1, one_terms, two_terms), jnp.where(odd == 1, two_terms, one_terms)
    )
    turn_rows(near_ref, ((above_flat, 0, STEP), (below_flat, 0, STEP)))
    wait_all(inputs)
    widen(own, own_flat)
    turn_rows(own_ref, ((own_flat, 0, rows), (own_flat, STEP, rows)))


def first_kernel(
    devices, own_raw, near_raw, near_terms, side, terms, mine, taps_in,
    own_out, conv_out, give_out, one_ref, two_ref, edge_ref, stats_ref,
    x_own, x_near, conv_ref, p_ref, taps, side_flat, col_terms, row_terms, sem,
):
    row_at, core = lax.axis_index(GX), lax.axis_index("gy")
    cols = own_raw.shape[1]
    rows, half = 2 * STEP, STEP // 2
    odd = lax.rem(row_at, 2)
    inputs = start_all(sem, 0, ((taps_in, taps),))

    def put_terms(source, at):
        value = terms[source].astype(jnp.float32)
        other = pltpu.roll(value, LANES // 2, 1)
        col_terms[pl.ds(at, STEP), :] = jnp.where(lane_half(STEP), value, other)
        col_terms[pl.ds(at + STEP, STEP), :] = jnp.where(lane_half(STEP), other, value)

    peers = cols // rows

    def put_own(i, _):
        put_terms(peers * core + i, pl.multiple_of(i * rows, 2 * STEP))
        return 0

    lax.fori_loop(0, peers, put_own, 0)
    put_terms(peers - core, cols)
    row_terms[...] = mine[...].astype(jnp.bfloat16).astype(jnp.float32)
    mask = reach_mask(core)
    tall = rows + 2 * STEP
    above_at, below_at = (STEP + rows) * (1 - odd), (STEP + rows) * odd
    widen(side, side_flat)
    add_terms(
        x_own, own_raw, ((side_flat, STEP, tall), (side_flat, 2 * STEP, tall)),
        row_terms, col_terms, None, core, mask,
    )
    given = x_own.at[pl.ds(half * (1 - core), half), pl.ds(0, cols)]
    outputs = start_all(sem, 1, ((x_own.at[:, pl.ds(0, cols)], own_out), (given, give_out)))
    add_terms(
        x_near, near_raw, ((side_flat, above_at, tall), (side_flat, below_at, tall)),
        near_terms, col_terms, inside_of(row_at, devices), core, mask,
    )
    wait_all(inputs)
    stats = conv_own_rows(x_own, x_near, weights_of(taps, OWN_TAPS), p_ref, conv_ref)
    stats_ref[...] = jnp.broadcast_to(stats, stats_ref.shape)
    outputs += start_all(sem, 3, ((conv_ref, conv_out),))
    lower = lane_half(LANES)
    for i in range(half):
        for first in range(0, cols, LANES):
            at = slice(first, first + LANES)
            upper_one = conv_ref[i, at, :].astype(jnp.float32)
            upper_two = conv_ref[i + half, at, :].astype(jnp.float32)
            up = jnp.where(lower, upper_one, pltpu.roll(upper_two, LANES // 2, 1))
            down = jnp.where(lower, pltpu.roll(upper_one, LANES // 2, 1), upper_two)
            one_ref[i, at, :] = jnp.where(odd == 1, up, down).astype(jnp.bfloat16)
            two_ref[i, at, :] = jnp.where(odd == 1, down, up).astype(jnp.bfloat16)
    edge_at = pl.multiple_of((cols - 2 * STEP) * (1 - core), 2 * STEP)
    edge_ref[...] = conv_ref[:, pl.ds(edge_at, 2 * STEP), :]
    wait_all(outputs)


def second_kernel(
    devices, cells, own_in, one, two, edge, corner, stats, stats_other, gains, taps_in,
    conv_out, give_out, stats_ref,
    a_own, a_near, conv_ref, p_ref, own, taps, sem,
):
    row_at, core = lax.axis_index(GX), lax.axis_index("gy")
    cols = own.shape[1]
    half = STEP // 2
    odd = lax.rem(row_at, 2)
    inputs = start_all(sem, 0, ((own_in, own), (taps_in, taps)))
    factor, offset = affine_of(0, (stats, stats_other), gains, cells)
    inside = inside_of(row_at, devices)
    mask = reach_mask(core)

    def activated(value):
        return elu(value.astype(jnp.float32) * factor + offset)

    def fill_own(i, _):
        for first in range(0, cols, LANES):
            at = slice(first, first + LANES)
            a_own[i, at, :] = activated(own[i, at, :]).astype(jnp.bfloat16)
        beyond = jnp.where(mask, activated(edge[i]), 0.0)
        a_own[i, cols:, :] = beyond.astype(jnp.bfloat16)
        return 0

    def two_rows(one, two):
        one, two = one.astype(jnp.float32), two.astype(jnp.float32)
        up, down = jnp.where(odd == 1, one, two), jnp.where(odd == 1, two, one)
        lower = lane_half(up.shape[0])
        return (
            jnp.where(lower, up, pltpu.roll(down, LANES // 2, 1)),
            jnp.where(lower, pltpu.roll(up, LANES // 2, 1), down),
        )

    def fill_near(i, _):
        for first in range(0, cols, LANES):
            at = slice(first, first + LANES)
            for k, value in enumerate(two_rows(one[i, at, :], two[i, at, :])):
                a_near[i + half * k, at, :] = (activated(value) * inside).astype(jnp.bfloat16)
        for k, value in enumerate(two_rows(corner[0, i], corner[1, i])):
            beyond = jnp.where(mask, activated(value) * inside, 0.0)
            a_near[i + half * k, cols:, :] = beyond.astype(jnp.bfloat16)
        return 0

    lax.fori_loop(0, half, fill_near, 0)
    wait_all(inputs)
    lax.fori_loop(0, STEP, fill_own, 0)
    stats = conv_own_rows(a_own, a_near, weights_of(taps, OWN_TAPS), p_ref, conv_ref)
    given = conv_ref.at[pl.ds(half * (1 - core), half)]
    outputs = start_all(sem, 0, ((given, give_out), (conv_ref, conv_out)))
    stats_ref[...] = jnp.broadcast_to(stats, stats_ref.shape)
    wait_all(outputs)


def pack_kernel(
    cells, block_in, other, conv_in, conv_other, stats, stats_other, gains,
    block_out_out, send_ref,
    out_ref, own, conv, sem,
):
    core = lax.axis_index("gy")
    cols = conv.shape[1]
    half = STEP // 2
    inputs = start_all(sem, 0, ((block_in, own), (conv_in, conv)))
    factor, offset = affine_of(1, (stats, stats_other), gains, cells)
    wide = 2 * STEP
    peers, some = cols // wide, LANES // wide

    def block_out(x, value):
        value = x.astype(jnp.float32) + value.astype(jnp.float32) * factor + offset
        return elu(value).astype(jnp.bfloat16)

    def mine(i, _):
        for first in range(0, cols, LANES):
            at = slice(first, first + LANES)
            out_ref[i, at, :] = block_out(own[i, at, :], conv[i, at, :])
        return 0

    wait_all(inputs[:2])
    lax.fori_loop(0, STEP, mine, 0)
    outputs = start_all(sem, 2, ((out_ref, block_out_out),))

    def step(i, _):
        for first in range(0, cols, LANES):
            at = slice(first, first + LANES)
            value = out_ref[half * core + i, at, :].reshape(some, wide, LANES)
            send_ref[pl.ds(peers * core + first // wide, some), i] = value
            value = block_out(other[i, at, :], conv_other[i, at, :]).reshape(some, wide, LANES)
            send_ref[pl.ds(peers * (1 - core) + first // wide, some), i] = value
        return 0

    lax.fori_loop(0, half, step, 0)
    wait_all(outputs)


def merge_kernel(own_in, received, other, result, out_ref, own, cells_ref, flat_ref, sem):
    core = lax.axis_index("gy")
    channels, rows, cols = out_ref.shape
    peers = other.shape[0]
    inputs = start_all(sem, 0, ((own_in, own),))

    def gather(s, _):
        cells_ref[s, core] = received[peers * core + s].astype(jnp.float32)
        cells_ref[s, 1 - core] = other[s].astype(jnp.float32)
        return 0

    lax.fori_loop(0, peers, gather, 0)
    wait_all(inputs)
    flat = cells_ref.reshape(peers * STEP * rows, LANES)
    some = LANES // rows
    lower = lane_half(some * STEP)

    def step(i, _):
        for block in range(cols // LANES):
            first = block * some * STEP * rows
            upper_row = flat[pl.ds(first + i, some * STEP, stride=rows), :]
            lower_row = flat[pl.ds(first + STEP + i, some * STEP, stride=rows), :]
            even = jnp.where(lower, upper_row, pltpu.roll(lower_row, channels, 1))
            odd = jnp.where(lower, pltpu.roll(upper_row, channels, 1), lower_row)
            mirrored = jnp.concatenate(
                [
                    part[s * STEP : (s + 1) * STEP]
                    for s in range(some)
                    for part in (even, odd)
                ],
                axis=0,
            )
            value = own[i, block * LANES : (block + 1) * LANES, :].astype(jnp.float32) + mirrored
            value = jnp.transpose(0.5 * value)
            for high in range(rows // STEP):
                flat_ref[block, pl.ds(high * STEP + i, channels, stride=rows), :] = value[
                    channels * high : channels * (high + 1)
                ]
        return 0

    lax.fori_loop(0, STEP, step, 0)

    def store(c, _):
        for block in range(cols // LANES):
            value = flat_ref[block, pl.ds(pl.multiple_of(c * rows, 8), rows), :]
            out_ref[c, :, block * LANES : (block + 1) * LANES] = value.astype(jnp.bfloat16)
        return 0

    part = channels // 2
    lax.fori_loop(0, part, store, 0)
    outputs = start_all(sem, 1, ((out_ref.at[pl.ds(0, part)], result.at[pl.ds(0, part)]),))
    lax.fori_loop(part, channels, store, 0)
    outputs += start_all(sem, 2, ((out_ref.at[pl.ds(part, part)], result.at[pl.ds(part, part)]),))
    wait_all(outputs)


def body(residue_feats, pair_feats, w_row, w_col, first_taps, second_taps, norm_scale, norm_shift):
    channels, rows, cols = pair_feats.shape
    cores = lax.axis_size("gy")
    devices = lax.axis_size(GX)
    first_core = lax.axis_index("gy") == 0
    cells = devices * rows * cores * cols
    bf16, f32 = jnp.bfloat16, jnp.float32
    conv_flops = 2 * 9 * channels * channels * rows * cols

    def edge(x):
        return jnp.where(first_core, x[..., cols - LANES :], x[..., :LANES])

    def swap(x):
        return lax.ppermute(x, "gy", SWAP)

    with_next = functools.partial(lax.ppermute, axis_name=GX, perm=pairs_of(devices, 0))
    with_last = functools.partial(lax.ppermute, axis_name=GX, perm=pairs_of(devices, 1))
    eight = (channels + 1, STEP, cols)
    one, two, terms, mine = call(
        prepare_kernel,
        (
            (VMEM, eight, bf16),
            (VMEM, eight, bf16),
            (VMEM, (devices, STEP, LANES), bf16),
            (VMEM, (STEP, LANES), f32),
        ),
        [
            VMEM(residue_feats.shape, bf16),
            VMEM(w_row.T.shape, bf16),
            VMEM(w_col.T.shape, bf16),
        ],
        5,
        conv_flops // 16,
        ((HBM, pair_feats), (HBM, residue_feats), (HBM, w_row.T), (HBM, w_col.T)),
    )
    one, two = with_next(one), with_last(two)
    terms = lax.all_to_all(terms, GX, 0, 0, tiled=True)
    gains = jnp.tile(jnp.concatenate([norm_scale, norm_shift], axis=0), (1, 2))
    near_side = swap(
        jnp.concatenate(
            [edge(one[:channels]), edge(pair_feats), edge(two[:channels])], axis=1
        )
    )

    taps_shape = VMEM(first_taps.shape, bf16)
    whole = (STEP, cols, LANES)
    part = (STEP // 2, cols, LANES)
    wide = (STEP, cols + 2 * STEP, LANES)
    products = VMEM((2, cols + 2 * STEP, 3 * LANES), f32)
    sums = (devices, LANES)
    own_raw, near_raw, near_terms = call(
        turn_kernel,
        ((VMEM, whole, bf16), (VMEM, whole, bf16), (VMEM, (STEP, LANES), f32)),
        [
            VMEM(pair_feats.shape, bf16),
            flat_of(channels, rows, cols),
            flat_of(channels, STEP, cols),
            flat_of(channels, STEP, cols),
        ],
        1,
        conv_flops,
        ((HBM, pair_feats), (VMEM, one), (VMEM, two)),
    )
    own_rows, conv_own, own_give, conv_one, conv_two, edges, stats = call(
        functools.partial(first_kernel, devices),
        (
            (HBM, whole, bf16),
            (HBM, whole, bf16),
            (HBM, part, bf16),
            (VMEM, part, bf16),
            (VMEM, part, bf16),
            (VMEM, (STEP, 2 * STEP, LANES), bf16),
            (VMEM, sums, f32),
        ),
        [
            VMEM(wide, bf16),
            VMEM(wide, bf16),
            VMEM(whole, bf16),
            products,
            taps_shape,
            flat_of(channels, rows + 2 * STEP, LANES),
            VMEM(wide[1:], f32),
            VMEM((STEP, LANES), f32),
        ],
        4,
        conv_flops,
        ((VMEM, own_raw), (VMEM, near_raw), (VMEM, near_terms), (VMEM, near_side),
         (VMEM, terms), (VMEM, mine), (HBM, first_taps)),
    )
    conv_one, conv_two = with_next(conv_one), with_last(conv_two)
    stats = lax.all_to_all(stats, GX, 0, 0, tiled=True)
    stats_other = swap(stats)
    edges = swap(edges)
    last = cols - 2 * STEP
    corners = swap(
        jnp.stack(
            [
                jnp.where(first_core, x[:, last:], x[:, : 2 * STEP])
                for x in (conv_one, conv_two)
            ]
        )
    )
    own_other = swap(own_give)
    conv_second, second_give, stats = call(
        functools.partial(second_kernel, devices, cells),
        ((HBM, whole, bf16), (HBM, part, bf16), (VMEM, sums, f32)),
        [
            VMEM(wide, bf16),
            VMEM(wide, bf16),
            VMEM(whole, bf16),
            products,
            VMEM(whole, bf16),
            taps_shape,
        ],
        2,
        conv_flops,
        ((HBM, conv_own), (VMEM, conv_one), (VMEM, conv_two), (VMEM, edges),
         (VMEM, corners), (VMEM, stats), (VMEM, stats_other), (VMEM, gains),
         (HBM, second_taps)),
    )
    stats = lax.all_to_all(stats, GX, 0, 0, tiled=True)
    stats_other = swap(stats)
    conv_other = swap(second_give)
    block_out, send = call(
        functools.partial(pack_kernel, cells),
        ((HBM, whole, bf16), (VMEM, (devices, STEP // 2, rows, LANES), bf16)),
        [
            VMEM(whole, bf16),
            VMEM(whole, bf16),
            VMEM(whole, bf16),
        ],
        3,
        conv_flops,
        ((HBM, own_rows), (VMEM, own_other), (HBM, conv_second), (VMEM, conv_other),
         (VMEM, stats), (VMEM, stats_other), (VMEM, gains)),
    )
    received = lax.all_to_all(send, GX, 0, 0, tiled=True)
    peers = devices // cores
    other = swap(jnp.where(first_core, received[peers:], received[:peers]))
    return call(
        merge_kernel,
        ((HBM, pair_feats.shape, bf16),),
        [
            VMEM(pair_feats.shape, bf16),
            VMEM(whole, bf16),
            VMEM((peers, cores, STEP // 2, rows, LANES), f32),
            flat_of(channels, rows, cols),
        ],
        3,
        conv_flops,
        ((HBM, block_out), (VMEM, received), (VMEM, other)),
    )[0]


def solution(mesh):
    torus = Mesh(
        mesh.devices.reshape(mesh.shape["grp"], 4, 16, mesh.shape["gy"]),
        ("grp", "gx_0", "gx_1", "gy"),
    )
    placed = (P(GRP_GX, None), P(None, GRP_GX, "gy"), P(), P(), P(), P(), P(), P())
    return jax.shard_map(
        body, mesh=torus, in_specs=placed, out_specs=P(None, GRP_GX, "gy"), check_vma=False
    )
```

```python
import functools

import jax
import jax.numpy as jnp
from jax import lax
from jax.experimental import pallas as pl
from jax.experimental.pallas import tpu as pltpu
from jax.sharding import Mesh
from jax.sharding import PartitionSpec as P

STEP = 8
GX = ("gx_0", "gx_1")
GRP_GX = ("grp", "gx_0", "gx_1")
LANES = 128
SWAP = [(0, 1), (1, 0)]
HBM, VMEM = pltpu.HBM, pltpu.VMEM

epsilon = 1e-05


def pairs_of(count, first):
    return [p for i in range(first, count - 1, 2) for p in ((i, i + 1), (i + 1, i))]


def call(kernel, outs, scratch, n_copies, flops, operands):
    spaces = [space for space, _ in operands]
    held = [pltpu.with_memory_space_constraint(x, space) for space, x in operands]
    return pl.pallas_call(
        kernel,
        out_shape=[space(shape, dtype) for space, shape, dtype in outs],
        in_specs=[pl.BlockSpec(memory_space=space) for space in spaces],
        out_specs=[pl.BlockSpec(memory_space=space) for space, _, _ in outs],
        scratch_shapes=[*scratch, pltpu.SemaphoreType.DMA((n_copies,))],
        cost_estimate=pl.CostEstimate(flops=flops, bytes_accessed=1 << 20, transcendentals=0),
        compiler_params=pltpu.CompilerParams(vmem_limit_bytes=24 << 20),
    )(*held)


def start_all(sem, first, pairs):
    copies = [
        pltpu.make_async_copy(src, dst, sem.at[first + i]) for i, (src, dst) in enumerate(pairs)
    ]
    for copy in copies:
        copy.start()
    return copies


def wait_all(copies):
    for copy in copies:
        copy.wait()


def elu(v):
    return jnp.where(v > 0, v, jnp.exp(jnp.minimum(v, 0.0)) - 1.0)


def as_float(flag):
    return jnp.asarray(flag, jnp.int32).astype(jnp.float32)


def lane_half(rows):
    return lax.broadcasted_iota(jnp.int32, (rows, LANES), 1) < LANES // 2


def halves(first, second):
    return jnp.where(lane_half(first.shape[0]), first, pltpu.roll(second, LANES // 2, 1))


def reach_mask(core):
    row = lax.broadcasted_iota(jnp.int32, (2 * STEP, LANES), 0)
    first = STEP * core
    return (row >= first) & (row < first + STEP)


def inside_of(row_at, devices):
    above = as_float(jnp.minimum(row_at, 1))
    below = as_float(jnp.minimum(devices - 1 - row_at, 1))
    return jnp.where(lane_half(1), above, below)


def flat_of(channels, rows, cols):
    return pltpu.VMEM((cols // LANES, channels * rows, LANES), jnp.float32)


def widen(source_ref, flat_ref):
    channels, rows, cols = source_ref.shape
    some = 64 // rows

    def step(i, _):
        for block in range(cols // LANES):
            value = source_ref[pl.ds(i * some, some), :, block * LANES : (block + 1) * LANES]
            flat_ref[block, pl.ds(pl.multiple_of(i * some * rows, 8), some * rows), :] = (
                value.astype(jnp.float32).reshape(some * rows, LANES)
            )
        return 0

    lax.fori_loop(0, channels // some, step, 0)


def two_rows_turned(sources, block, i):
    channels = LANES // 2
    return jnp.transpose(
        jnp.concatenate(
            [
                flat[block, pl.ds(first + i, channels, stride=rows), :]
                for flat, first, rows in sources
            ],
            axis=0,
        )
    )


def turn_rows(out_ref, sources):
    def step(i, _):
        for block in range(out_ref.shape[1] // LANES):
            at = slice(block * LANES, (block + 1) * LANES)
            out_ref[i, at, :] = two_rows_turned(sources, block, i).astype(jnp.bfloat16)
        return 0

    lax.fori_loop(0, STEP, step, 0)


def add_terms(x_ref, raw_ref, side_sources, row_terms, col_terms, scale, core, mask):
    cols = raw_ref.shape[1]

    for i in range(STEP):
        side = two_rows_turned(side_sources, 0, i)
        value = jnp.where(core == 0, side[: 2 * STEP], side[LANES - 2 * STEP :])
        value = value + (row_terms[i : i + 1] + col_terms[cols:, :])
        if scale is not None:
            value = value * scale
        x_ref[i, cols:, :] = jnp.where(mask, value, 0.0).astype(jnp.bfloat16)

    def step(i, _):
        row = row_terms[pl.ds(i, 1), :]
        for block in range(cols // LANES):
            at = slice(block * LANES, (block + 1) * LANES)
            value = raw_ref[i, at, :].astype(jnp.float32) + (row + col_terms[at, :])
            if scale is not None:
                value = value * scale
            x_ref[i, at, :] = value.astype(jnp.bfloat16)
        return 0

    lax.fori_loop(0, STEP, step, 0)


def weights_of(taps_ref, wanted):
    channels = taps_ref.shape[1]
    zero = jnp.zeros((channels, channels), jnp.bfloat16)
    return jnp.concatenate(
        [
            jnp.concatenate(
                [zero if ky is None else taps_ref[3 * ky + kx] for ky in inputs], axis=1
            )
            for kx in range(3)
            for inputs in wanted
        ],
        axis=0,
    )


OWN_TAPS = ((1, 2, 0, None), (0, 1, None, 2))


def product(values, weights):
    return lax.dot_general(
        values, weights, (((1,), (1,)), ((), ())), preferred_element_type=jnp.float32
    )


def shifted_sum(p_ref, first):
    last = p_ref.shape[0]
    if first == 0:
        left = jnp.concatenate([p_ref[last - STEP :, :LANES], p_ref[: LANES - STEP, :LANES]], axis=0)
    else:
        left = p_ref[first - STEP : first - STEP + LANES, :LANES]
    centre = p_ref[first : first + LANES, LANES : 2 * LANES]
    right = p_ref[first + STEP : first + STEP + LANES, 2 * LANES :]
    return left + centre + right


def conv_own_rows(own_ref, near_ref, weights, p_ref, out_ref):
    cols = out_ref.shape[1]
    total = jnp.zeros((STEP, LANES), jnp.float32)
    squares = total
    for i in range(STEP):
        p = p_ref.at[i % 2]
        p[...] = product(jnp.concatenate([own_ref[i], near_ref[i]], axis=1), weights)
        for first in range(0, cols, LANES):
            value = shifted_sum(p, first)
            out_ref[i, first : first + LANES, :] = value.astype(jnp.bfloat16)
            value = value.reshape(LANES // STEP, STEP, LANES)
            total = total + jnp.sum(value, axis=0)
            squares = squares + jnp.sum(value * value, axis=0)
    total = total + pltpu.roll(total, LANES // 2, 1)
    squares = squares + pltpu.roll(squares, LANES // 2, 1)
    return jnp.sum(jnp.where(lane_half(STEP), total, squares), axis=0, keepdims=True)


def affine_of(which, stats_refs, gains_ref, cells):
    row = sum(jnp.sum(ref[...], axis=0, keepdims=True) for ref in stats_refs) / cells
    row = jnp.broadcast_to(row, (STEP, LANES))
    other = pltpu.roll(row, LANES // 2, 1)
    average = jnp.where(lane_half(STEP), row, other)
    spread = jnp.where(lane_half(STEP), other, row) - average * average
    factor = gains_ref[which : which + 1] * lax.rsqrt(spread + epsilon)
    offset = gains_ref[2 + which : 3 + which] - average * factor
    return factor[0:1], offset[0:1]


def prepare_kernel(
    pair, feats, w_row, w_col, one, two, col_terms, row_terms, feats_in, row_in, col_in, sem
):
    odd = lax.rem(lax.axis_index(GX), 2)
    channels = pair.shape[0]
    lower, upper = pl.multiple_of(STEP * (1 - odd), STEP), pl.multiple_of(STEP * odd, STEP)
    parts = start_all(
        sem, 0,
        ((pair.at[:, pl.ds(lower, STEP)], one.at[pl.ds(0, channels)]),
         (pair.at[:, pl.ds(upper, STEP)], two.at[pl.ds(0, channels)])),
    )
    inputs = start_all(sem, 2, ((feats, feats_in), (w_row, row_in), (w_col, col_in)))
    wait_all(inputs)
    zero = jnp.zeros((2 * STEP, LANES - channels), jnp.float32)
    row = jnp.concatenate([product(feats_in[...], row_in[...]), zero], axis=1)
    col = jnp.concatenate([product(feats_in[...], col_in[...]), zero], axis=1)
    packed = halves(col[:STEP], col[STEP:]).astype(jnp.bfloat16)
    col_terms[...] = jnp.broadcast_to(packed[None], col_terms.shape)
    row_terms[...] = halves(row[:STEP], row[STEP:])
    empty = jnp.zeros((STEP, one.shape[2] - LANES), jnp.float32)
    for ref, which in ((one, odd), (two, 1 - odd)):
        rows = jnp.where(which == 0, row[STEP:], row[:STEP])
        ref[channels] = jnp.concatenate([rows, empty], axis=1).astype(jnp.bfloat16)
    wait_all(parts)


def turn_kernel(
    pair, one, two, own_ref, near_ref, row_terms, own, own_flat, above_flat, below_flat, sem
):
    odd = lax.rem(lax.axis_index(GX), 2)
    channels, rows, _ = own.shape
    inputs = start_all(sem, 0, ((pair, own),))
    one_rows, two_rows = one.at[pl.ds(0, channels)], two.at[pl.ds(0, channels)]

    @pl.when(odd == 0)
    def _():
        widen(two_rows, above_flat)
        widen(one_rows, below_flat)

    @pl.when(odd == 1)
    def _():
        widen(one_rows, above_flat)
        widen(two_rows, below_flat)

    one_terms = one[channels, :, :LANES].astype(jnp.float32)
    two_terms = two[channels, :, :LANES].astype(jnp.float32)
    row_terms[...] = halves(
        jnp.where(odd == 1, one_terms, two_terms), jnp.where(odd == 1, two_terms, one_terms)
    )
    turn_rows(near_ref, ((above_flat, 0, STEP), (below_flat, 0, STEP)))
    wait_all(inputs)
    widen(own, own_flat)
    turn_rows(own_ref, ((own_flat, 0, rows), (own_flat, STEP, rows)))


def first_kernel(
    devices, own_raw, near_raw, near_terms, side, terms, mine, taps_in,
    own_out, conv_out, give_out, one_ref, two_ref, edge_ref, stats_ref,
    x_own, x_near, conv_ref, p_ref, taps, side_flat, col_terms, row_terms, sem,
):
    row_at, core = lax.axis_index(GX), lax.axis_index("gy")
    cols = own_raw.shape[1]
    rows, half = 2 * STEP, STEP // 2
    odd = lax.rem(row_at, 2)
    inputs = start_all(sem, 0, ((taps_in, taps),))

    def put_terms(sources):
        values = [(at, terms[source].astype(jnp.float32)) for source, at in sources]
        values = [(at, value, pltpu.roll(value, LANES // 2, 1)) for at, value in values]
        for at, value, other in values:
            col_terms[at : at + STEP] = jnp.where(lane_half(STEP), value, other)
            col_terms[at + STEP : at + 2 * STEP] = jnp.where(lane_half(STEP), other, value)

    peers = cols // rows
    put_terms([(peers * core + i, i * rows) for i in range(peers)] + [(peers - core, cols)])
    row_terms[...] = mine[...].astype(jnp.bfloat16).astype(jnp.float32)
    mask = reach_mask(core)
    tall = rows + 2 * STEP
    above_at, below_at = (STEP + rows) * (1 - odd), (STEP + rows) * odd
    widen(side, side_flat)
    add_terms(
        x_own, own_raw, ((side_flat, STEP, tall), (side_flat, 2 * STEP, tall)),
        row_terms, col_terms, None, core, mask,
    )
    given = x_own.at[pl.ds(half * (1 - core), half), pl.ds(0, cols)]
    outputs = start_all(sem, 1, ((x_own.at[:, pl.ds(0, cols)], own_out), (given, give_out)))
    add_terms(
        x_near, near_raw, ((side_flat, above_at, tall), (side_flat, below_at, tall)),
        near_terms, col_terms, inside_of(row_at, devices), core, mask,
    )
    wait_all(inputs)
    stats = conv_own_rows(x_own, x_near, weights_of(taps, OWN_TAPS), p_ref, conv_ref)
    stats_ref[...] = jnp.broadcast_to(stats, stats_ref.shape)
    outputs += start_all(sem, 3, ((conv_ref, conv_out),))
    lower = lane_half(LANES)
    for i in range(half):
        for first in range(0, cols, LANES):
            at = slice(first, first + LANES)
            upper_one = conv_ref[i, at, :].astype(jnp.float32)
            upper_two = conv_ref[i + half, at, :].astype(jnp.float32)
            up = jnp.where(lower, upper_one, pltpu.roll(upper_two, LANES // 2, 1))
            down = jnp.where(lower, pltpu.roll(upper_one, LANES // 2, 1), upper_two)
            one_ref[i, at, :] = jnp.where(odd == 1, up, down).astype(jnp.bfloat16)
            two_ref[i, at, :] = jnp.where(odd == 1, down, up).astype(jnp.bfloat16)
    edge_at = pl.multiple_of((cols - 2 * STEP) * (1 - core), 2 * STEP)
    edge_ref[...] = conv_ref[:, pl.ds(edge_at, 2 * STEP), :]
    wait_all(outputs)


def second_kernel(
    devices, cells, own_in, one, two, edge, corner, stats, stats_other, gains, taps_in,
    conv_out, give_out, stats_ref,
    a_own, a_near, conv_ref, p_ref, own, taps, sem,
):
    row_at, core = lax.axis_index(GX), lax.axis_index("gy")
    cols = own.shape[1]
    half = STEP // 2
    odd = lax.rem(row_at, 2)
    inputs = start_all(sem, 0, ((own_in, own), (taps_in, taps)))
    factor, offset = affine_of(0, (stats, stats_other), gains, cells)
    inside = inside_of(row_at, devices)
    mask = reach_mask(core)

    def activated(value):
        return elu(value.astype(jnp.float32) * factor + offset)

    def fill_own(i, _):
        for first in range(0, cols, LANES):
            at = slice(first, first + LANES)
            a_own[i, at, :] = activated(own[i, at, :]).astype(jnp.bfloat16)
        beyond = jnp.where(mask, activated(edge[i]), 0.0)
        a_own[i, cols:, :] = beyond.astype(jnp.bfloat16)
        return 0

    def two_rows(one, two):
        one, two = one.astype(jnp.float32), two.astype(jnp.float32)
        up, down = jnp.where(odd == 1, one, two), jnp.where(odd == 1, two, one)
        lower = lane_half(up.shape[0])
        return (
            jnp.where(lower, up, pltpu.roll(down, LANES // 2, 1)),
            jnp.where(lower, pltpu.roll(up, LANES // 2, 1), down),
        )

    def fill_near(i, _):
        for first in range(0, cols, LANES):
            at = slice(first, first + LANES)
            for k, value in enumerate(two_rows(one[i, at, :], two[i, at, :])):
                a_near[i + half * k, at, :] = (activated(value) * inside).astype(jnp.bfloat16)
        for k, value in enumerate(two_rows(corner[0, i], corner[1, i])):
            beyond = jnp.where(mask, activated(value) * inside, 0.0)
            a_near[i + half * k, cols:, :] = beyond.astype(jnp.bfloat16)
        return 0

    lax.fori_loop(0, half, fill_near, 0)
    wait_all(inputs)
    lax.fori_loop(0, STEP, fill_own, 0)
    stats = conv_own_rows(a_own, a_near, weights_of(taps, OWN_TAPS), p_ref, conv_ref)
    given = conv_ref.at[pl.ds(half * (1 - core), half)]
    outputs = start_all(sem, 0, ((given, give_out), (conv_ref, conv_out)))
    stats_ref[...] = jnp.broadcast_to(stats, stats_ref.shape)
    wait_all(outputs)


def pack_kernel(
    cells, block_in, other, conv_in, conv_other, stats, stats_other, gains,
    block_out_out, send_ref,
    out_ref, own, conv, sem,
):
    core = lax.axis_index("gy")
    cols = conv.shape[1]
    half = STEP // 2
    parts = [
        start_all(
            sem, 2 * n,
            [(src.at[pl.ds(2 * n, 2)], dst.at[pl.ds(2 * n, 2)])
             for src, dst in ((block_in, own), (conv_in, conv))],
        )
        for n in range(STEP // 2)
    ]
    factor, offset = affine_of(1, (stats, stats_other), gains, cells)
    wide = 2 * STEP
    peers, some = cols // wide, LANES // wide

    def block_out(x, value):
        value = x.astype(jnp.float32) + value.astype(jnp.float32) * factor + offset
        return elu(value).astype(jnp.bfloat16)

    def mine(i, _):
        for first in range(0, cols, LANES):
            at = slice(first, first + LANES)
            out_ref[i, at, :] = block_out(own[i, at, :], conv[i, at, :])
        return 0

    for n, part in enumerate(parts):
        wait_all(part)
        lax.fori_loop(2 * n, 2 * n + 2, mine, 0)
    outputs = start_all(sem, STEP, ((out_ref, block_out_out),))

    def step(i, _):
        for first in range(0, cols, LANES):
            at = slice(first, first + LANES)
            value = out_ref[half * core + i, at, :].reshape(some, wide, LANES)
            send_ref[pl.ds(peers * core + first // wide, some), i] = value
            value = block_out(other[i, at, :], conv_other[i, at, :]).reshape(some, wide, LANES)
            send_ref[pl.ds(peers * (1 - core) + first // wide, some), i] = value
        return 0

    lax.fori_loop(0, half, step, 0)
    wait_all(outputs)


def merge_kernel(own_in, received, other, result, out_ref, own, cells_ref, flat_ref, sem):
    core = lax.axis_index("gy")
    channels, rows, cols = out_ref.shape
    peers = other.shape[0]
    inputs = start_all(sem, 0, ((own_in, own),))

    def gather(s, _):
        cells_ref[s, core] = received[peers * core + s].astype(jnp.float32)
        cells_ref[s, 1 - core] = other[s].astype(jnp.float32)
        return 0

    lax.fori_loop(0, peers, gather, 0)
    wait_all(inputs)
    flat = cells_ref.reshape(peers * STEP * rows, LANES)
    some = LANES // rows
    lower = lane_half(some * STEP)

    def step(i, _):
        for block in range(cols // LANES):
            first = block * some * STEP * rows
            upper_row = flat[pl.ds(first + i, some * STEP, stride=rows), :]
            lower_row = flat[pl.ds(first + STEP + i, some * STEP, stride=rows), :]
            even = jnp.where(lower, upper_row, pltpu.roll(lower_row, channels, 1))
            odd = jnp.where(lower, pltpu.roll(upper_row, channels, 1), lower_row)
            mirrored = jnp.concatenate(
                [
                    part[s * STEP : (s + 1) * STEP]
                    for s in range(some)
                    for part in (even, odd)
                ],
                axis=0,
            )
            value = own[i, block * LANES : (block + 1) * LANES, :].astype(jnp.float32) + mirrored
            value = jnp.transpose(0.5 * value)
            for high in range(rows // STEP):
                flat_ref[block, pl.ds(high * STEP + i, channels, stride=rows), :] = value[
                    channels * high : channels * (high + 1)
                ]
        return 0

    lax.fori_loop(0, STEP, step, 0)

    def store(c, _):
        for block in range(cols // LANES):
            value = flat_ref[block, pl.ds(pl.multiple_of(c * rows, 8), rows), :]
            out_ref[c, :, block * LANES : (block + 1) * LANES] = value.astype(jnp.bfloat16)
        return 0

    part = channels // 2
    lax.fori_loop(0, part, store, 0)
    outputs = start_all(sem, 1, ((out_ref.at[pl.ds(0, part)], result.at[pl.ds(0, part)]),))
    lax.fori_loop(part, channels, store, 0)
    outputs += start_all(sem, 2, ((out_ref.at[pl.ds(part, part)], result.at[pl.ds(part, part)]),))
    wait_all(outputs)


def body(residue_feats, pair_feats, w_row, w_col, first_taps, second_taps, norm_scale, norm_shift):
    channels, rows, cols = pair_feats.shape
    cores = lax.axis_size("gy")
    devices = lax.axis_size(GX)
    first_core = lax.axis_index("gy") == 0
    cells = devices * rows * cores * cols
    bf16, f32 = jnp.bfloat16, jnp.float32
    conv_flops = 2 * 9 * channels * channels * rows * cols

    def edge(x):
        return jnp.where(first_core, x[..., cols - LANES :], x[..., :LANES])

    def swap(x):
        return lax.ppermute(x, "gy", SWAP)

    with_next = functools.partial(lax.ppermute, axis_name=GX, perm=pairs_of(devices, 0))
    with_last = functools.partial(lax.ppermute, axis_name=GX, perm=pairs_of(devices, 1))
    eight = (channels + 1, STEP, cols)
    one, two, terms, mine = call(
        prepare_kernel,
        (
            (VMEM, eight, bf16),
            (VMEM, eight, bf16),
            (VMEM, (devices, STEP, LANES), bf16),
            (VMEM, (STEP, LANES), f32),
        ),
        [
            VMEM(residue_feats.shape, bf16),
            VMEM(w_row.T.shape, bf16),
            VMEM(w_col.T.shape, bf16),
        ],
        5,
        conv_flops // 16,
        ((HBM, pair_feats), (HBM, residue_feats), (HBM, w_row.T), (HBM, w_col.T)),
    )
    one, two = with_next(one), with_last(two)
    terms = lax.all_to_all(terms, GX, 0, 0, tiled=True)
    gains = jnp.tile(jnp.concatenate([norm_scale, norm_shift], axis=0), (1, 2))
    near_side = swap(
        jnp.concatenate(
            [edge(one[:channels]), edge(pair_feats), edge(two[:channels])], axis=1
        )
    )

    taps_shape = VMEM(first_taps.shape, bf16)
    whole = (STEP, cols, LANES)
    part = (STEP // 2, cols, LANES)
    wide = (STEP, cols + 2 * STEP, LANES)
    products = VMEM((2, cols + 2 * STEP, 3 * LANES), f32)
    sums = (devices, LANES)
    own_raw, near_raw, near_terms = call(
        turn_kernel,
        ((VMEM, whole, bf16), (VMEM, whole, bf16), (VMEM, (STEP, LANES), f32)),
        [
            VMEM(pair_feats.shape, bf16),
            flat_of(channels, rows, cols),
            flat_of(channels, STEP, cols),
            flat_of(channels, STEP, cols),
        ],
        1,
        conv_flops,
        ((HBM, pair_feats), (VMEM, one), (VMEM, two)),
    )
    own_rows, conv_own, own_give, conv_one, conv_two, edges, stats = call(
        functools.partial(first_kernel, devices),
        (
            (HBM, whole, bf16),
            (HBM, whole, bf16),
            (HBM, part, bf16),
            (VMEM, part, bf16),
            (VMEM, part, bf16),
            (VMEM, (STEP, 2 * STEP, LANES), bf16),
            (VMEM, sums, f32),
        ),
        [
            VMEM(wide, bf16),
            VMEM(wide, bf16),
            VMEM(whole, bf16),
            products,
            taps_shape,
            flat_of(channels, rows + 2 * STEP, LANES),
            VMEM(wide[1:], f32),
            VMEM((STEP, LANES), f32),
        ],
        4,
        conv_flops,
        ((VMEM, own_raw), (VMEM, near_raw), (VMEM, near_terms), (VMEM, near_side),
         (VMEM, terms), (VMEM, mine), (HBM, first_taps)),
    )
    conv_one, conv_two = with_next(conv_one), with_last(conv_two)
    stats = lax.all_to_all(stats, GX, 0, 0, tiled=True)
    stats_other = swap(stats)
    edges = swap(edges)
    last = cols - 2 * STEP
    corners = swap(
        jnp.stack(
            [
                jnp.where(first_core, x[:, last:], x[:, : 2 * STEP])
                for x in (conv_one, conv_two)
            ]
        )
    )
    own_other = swap(own_give)
    conv_second, second_give, stats = call(
        functools.partial(second_kernel, devices, cells),
        ((HBM, whole, bf16), (HBM, part, bf16), (VMEM, sums, f32)),
        [
            VMEM(wide, bf16),
            VMEM(wide, bf16),
            VMEM(whole, bf16),
            products,
            VMEM(whole, bf16),
            taps_shape,
        ],
        2,
        conv_flops,
        ((HBM, conv_own), (VMEM, conv_one), (VMEM, conv_two), (VMEM, edges),
         (VMEM, corners), (VMEM, stats), (VMEM, stats_other), (VMEM, gains),
         (HBM, second_taps)),
    )
    stats = lax.all_to_all(stats, GX, 0, 0, tiled=True)
    stats_other = swap(stats)
    conv_other = swap(second_give)
    block_out, send = call(
        functools.partial(pack_kernel, cells),
        ((HBM, whole, bf16), (VMEM, (devices, STEP // 2, rows, LANES), bf16)),
        [
            VMEM(whole, bf16),
            VMEM(whole, bf16),
            VMEM(whole, bf16),
        ],
        STEP + 1,
        conv_flops,
        ((HBM, own_rows), (VMEM, own_other), (HBM, conv_second), (VMEM, conv_other),
         (VMEM, stats), (VMEM, stats_other), (VMEM, gains)),
    )
    received = lax.all_to_all(send, GX, 0, 0, tiled=True)
    peers = devices // cores
    other = swap(jnp.where(first_core, received[peers:], received[:peers]))
    return call(
        merge_kernel,
        ((HBM, pair_feats.shape, bf16),),
        [
            VMEM(pair_feats.shape, bf16),
            VMEM(whole, bf16),
            VMEM((peers, cores, STEP // 2, rows, LANES), f32),
            flat_of(channels, rows, cols),
        ],
        3,
        conv_flops,
        ((HBM, block_out), (VMEM, received), (VMEM, other)),
    )[0]


def solution(mesh):
    torus = Mesh(
        mesh.devices.reshape(mesh.shape["grp"], 4, 16, mesh.shape["gy"]),
        ("grp", "gx_0", "gx_1", "gy"),
    )
    placed = (P(GRP_GX, None), P(None, GRP_GX, "gy"), P(), P(), P(), P(), P(), P())
    return jax.shard_map(
        body, mesh=torus, in_specs=placed, out_specs=P(None, GRP_GX, "gy"), check_vma=False
    )
```

```python
import functools

import jax
import jax.numpy as jnp
from jax import lax
from jax.experimental import pallas as pl
from jax.experimental.pallas import tpu as pltpu
from jax.sharding import Mesh
from jax.sharding import PartitionSpec as P

STEP = 8
GX = ("gx_0", "gx_1")
GRP_GX = ("grp", "gx_0", "gx_1")
LANES = 128
SWAP = [(0, 1), (1, 0)]
HBM, VMEM = pltpu.HBM, pltpu.VMEM

epsilon = 1e-05


def pairs_of(count, first):
    return [p for i in range(first, count - 1, 2) for p in ((i, i + 1), (i + 1, i))]


def call(kernel, outs, scratch, n_copies, flops, operands):
    spaces = [space for space, _ in operands]
    held = [pltpu.with_memory_space_constraint(x, space) for space, x in operands]
    return pl.pallas_call(
        kernel,
        out_shape=[space(shape, dtype) for space, shape, dtype in outs],
        in_specs=[pl.BlockSpec(memory_space=space) for space in spaces],
        out_specs=[pl.BlockSpec(memory_space=space) for space, _, _ in outs],
        scratch_shapes=[*scratch, pltpu.SemaphoreType.DMA((n_copies,))],
        cost_estimate=pl.CostEstimate(flops=flops, bytes_accessed=1 << 20, transcendentals=0),
        compiler_params=pltpu.CompilerParams(vmem_limit_bytes=12 << 20),
    )(*held)


def start_all(sem, first, pairs):
    copies = [
        pltpu.make_async_copy(src, dst, sem.at[first + i]) for i, (src, dst) in enumerate(pairs)
    ]
    for copy in copies:
        copy.start()
    return copies


def wait_all(copies):
    for copy in copies:
        copy.wait()


def elu(v):
    return jnp.where(v > 0, v, jnp.exp(jnp.minimum(v, 0.0)) - 1.0)


def as_float(flag):
    return jnp.asarray(flag, jnp.int32).astype(jnp.float32)


def lane_half(rows):
    return lax.broadcasted_iota(jnp.int32, (rows, LANES), 1) < LANES // 2


def halves(first, second):
    return jnp.where(lane_half(first.shape[0]), first, pltpu.roll(second, LANES // 2, 1))


def reach_mask(core):
    row = lax.broadcasted_iota(jnp.int32, (2 * STEP, LANES), 0)
    first = STEP * core
    return (row >= first) & (row < first + STEP)


def inside_of(row_at, devices):
    above = as_float(jnp.minimum(row_at, 1))
    below = as_float(jnp.minimum(devices - 1 - row_at, 1))
    return jnp.where(lane_half(1), above, below)


def flat_of(channels, rows, cols):
    return pltpu.VMEM((cols // LANES, channels * rows, LANES), jnp.float32)


def widen(source_ref, flat_ref):
    channels, rows, cols = source_ref.shape
    some = 64 // rows

    def step(i, _):
        for block in range(cols // LANES):
            value = source_ref[pl.ds(i * some, some), :, block * LANES : (block + 1) * LANES]
            flat_ref[block, pl.ds(pl.multiple_of(i * some * rows, 8), some * rows), :] = (
                value.astype(jnp.float32).reshape(some * rows, LANES)
            )
        return 0

    lax.fori_loop(0, channels // some, step, 0)


def two_rows_turned(sources, block, i):
    channels = LANES // 2
    return jnp.transpose(
        jnp.concatenate(
            [
                flat[block, pl.ds(first + i, channels, stride=rows), :]
                for flat, first, rows in sources
            ],
            axis=0,
        )
    )


def turn_rows(out_ref, sources):
    def step(i, _):
        for block in range(out_ref.shape[1] // LANES):
            at = slice(block * LANES, (block + 1) * LANES)
            out_ref[i, at, :] = two_rows_turned(sources, block, i).astype(jnp.bfloat16)
        return 0

    lax.fori_loop(0, STEP, step, 0)


def add_terms(x_ref, raw_ref, side_sources, row_terms, col_terms, scale, core, mask):
    cols = raw_ref.shape[1]

    for i in range(STEP):
        side = two_rows_turned(side_sources, 0, i)
        value = jnp.where(core == 0, side[: 2 * STEP], side[LANES - 2 * STEP :])
        value = value + (row_terms[i : i + 1] + col_terms[cols:, :])
        if scale is not None:
            value = value * scale
        x_ref[i, cols:, :] = jnp.where(mask, value, 0.0).astype(jnp.bfloat16)

    def step(i, _):
        row = row_terms[pl.ds(i, 1), :]
        for block in range(cols // LANES):
            at = slice(block * LANES, (block + 1) * LANES)
            value = raw_ref[i, at, :].astype(jnp.float32) + (row + col_terms[at, :])
            if scale is not None:
                value = value * scale
            x_ref[i, at, :] = value.astype(jnp.bfloat16)
        return 0

    lax.fori_loop(0, STEP, step, 0)


def weights_of(taps_ref, wanted):
    channels = taps_ref.shape[1]
    zero = jnp.zeros((channels, channels), jnp.bfloat16)
    return jnp.concatenate(
        [
            jnp.concatenate(
                [zero if ky is None else taps_ref[3 * ky + kx] for ky in inputs], axis=1
            )
            for kx in range(3)
            for inputs in wanted
        ],
        axis=0,
    )


OWN_TAPS = ((1, 2, 0, None), (0, 1, None, 2))


def product(values, weights):
    return lax.dot_general(
        values, weights, (((1,), (1,)), ((), ())), preferred_element_type=jnp.float32
    )


def shifted_sum(p_ref, first):
    last = p_ref.shape[0]
    if first == 0:
        left = jnp.concatenate([p_ref[last - STEP :, :LANES], p_ref[: LANES - STEP, :LANES]], axis=0)
    else:
        left = p_ref[first - STEP : first - STEP + LANES, :LANES]
    centre = p_ref[first : first + LANES, LANES : 2 * LANES]
    right = p_ref[first + STEP : first + STEP + LANES, 2 * LANES :]
    return left + centre + right


def conv_own_rows(own_ref, near_ref, weights, p_ref, out_ref):
    cols = out_ref.shape[1]
    total = jnp.zeros((STEP, LANES), jnp.float32)
    squares = total
    for i in range(STEP):
        p = p_ref.at[i % 2]
        p[...] = product(jnp.concatenate([own_ref[i], near_ref[i]], axis=1), weights)
        for first in range(0, cols, LANES):
            value = shifted_sum(p, first)
            out_ref[i, first : first + LANES, :] = value.astype(jnp.bfloat16)
            value = value.reshape(LANES // STEP, STEP, LANES)
            total = total + jnp.sum(value, axis=0)
            squares = squares + jnp.sum(value * value, axis=0)
    total = total + pltpu.roll(total, LANES // 2, 1)
    squares = squares + pltpu.roll(squares, LANES // 2, 1)
    return jnp.sum(jnp.where(lane_half(STEP), total, squares), axis=0, keepdims=True)


def affine_of(which, stats_refs, gains_ref, cells):
    row = sum(jnp.sum(ref[...], axis=0, keepdims=True) for ref in stats_refs) / cells
    row = jnp.broadcast_to(row, (STEP, LANES))
    other = pltpu.roll(row, LANES // 2, 1)
    average = jnp.where(lane_half(STEP), row, other)
    spread = jnp.where(lane_half(STEP), other, row) - average * average
    factor = gains_ref[which : which + 1] * lax.rsqrt(spread + epsilon)
    offset = gains_ref[2 + which : 3 + which] - average * factor
    return factor[0:1], offset[0:1]


def prepare_kernel(
    pair, feats, w_row, w_col, one, two, col_terms, row_terms, feats_in, row_in, col_in, sem
):
    odd = lax.rem(lax.axis_index(GX), 2)
    channels = pair.shape[0]
    lower, upper = pl.multiple_of(STEP * (1 - odd), STEP), pl.multiple_of(STEP * odd, STEP)
    parts = start_all(
        sem, 0,
        ((pair.at[:, pl.ds(lower, STEP)], one.at[pl.ds(0, channels)]),
         (pair.at[:, pl.ds(upper, STEP)], two.at[pl.ds(0, channels)])),
    )
    inputs = start_all(sem, 2, ((feats, feats_in), (w_row, row_in), (w_col, col_in)))
    wait_all(inputs)
    zero = jnp.zeros((2 * STEP, LANES - channels), jnp.float32)
    row = jnp.concatenate([product(feats_in[...], row_in[...]), zero], axis=1)
    col = jnp.concatenate([product(feats_in[...], col_in[...]), zero], axis=1)
    packed = halves(col[:STEP], col[STEP:]).astype(jnp.bfloat16)
    col_terms[...] = jnp.broadcast_to(packed[None], col_terms.shape)
    row_terms[...] = halves(row[:STEP], row[STEP:])
    empty = jnp.zeros((STEP, one.shape[2] - LANES), jnp.float32)
    for ref, which in ((one, odd), (two, 1 - odd)):
        rows = jnp.where(which == 0, row[STEP:], row[:STEP])
        ref[channels] = jnp.concatenate([rows, empty], axis=1).astype(jnp.bfloat16)
    wait_all(parts)


def turn_kernel(
    pair, one, two, own_ref, near_ref, row_terms, own, own_flat, above_flat, below_flat, sem
):
    odd = lax.rem(lax.axis_index(GX), 2)
    channels, rows, _ = own.shape
    inputs = start_all(sem, 0, ((pair, own),))
    one_rows, two_rows = one.at[pl.ds(0, channels)], two.at[pl.ds(0, channels)]

    @pl.when(odd == 0)
    def _():
        widen(two_rows, above_flat)
        widen(one_rows, below_flat)

    @pl.when(odd == 1)
    def _():
        widen(one_rows, above_flat)
        widen(two_rows, below_flat)

    one_terms = one[channels, :, :LANES].astype(jnp.float32)
    two_terms = two[channels, :, :LANES].astype(jnp.float32)
    row_terms[...] = halves(
        jnp.where(odd == 1, one_terms, two_terms), jnp.where(odd == 1, two_terms, one_terms)
    )
    turn_rows(near_ref, ((above_flat, 0, STEP), (below_flat, 0, STEP)))
    wait_all(inputs)
    widen(own, own_flat)
    turn_rows(own_ref, ((own_flat, 0, rows), (own_flat, STEP, rows)))


def first_kernel(
    devices, own_raw, near_raw, near_terms, side, terms, mine, taps_in,
    own_out, conv_out, give_out, one_ref, two_ref, edge_ref, stats_ref,
    x_own, x_near, conv_ref, p_ref, taps, side_flat, col_terms, row_terms, sem,
):
    row_at, core = lax.axis_index(GX), lax.axis_index("gy")
    cols = own_raw.shape[1]
    rows, half = 2 * STEP, STEP // 2
    odd = lax.rem(row_at, 2)
    inputs = start_all(sem, 0, ((taps_in, taps),))

    def put_terms(sources):
        values = [(at, terms[source].astype(jnp.float32)) for source, at in sources]
        values = [(at, value, pltpu.roll(value, LANES // 2, 1)) for at, value in values]
        for at, value, other in values:
            col_terms[at : at + STEP] = jnp.where(lane_half(STEP), value, other)
            col_terms[at + STEP : at + 2 * STEP] = jnp.where(lane_half(STEP), other, value)

    peers = cols // rows
    put_terms([(peers * core + i, i * rows) for i in range(peers)] + [(peers - core, cols)])
    row_terms[...] = mine[...].astype(jnp.bfloat16).astype(jnp.float32)
    mask = reach_mask(core)
    tall = rows + 2 * STEP
    above_at, below_at = (STEP + rows) * (1 - odd), (STEP + rows) * odd
    widen(side, side_flat)
    add_terms(
        x_own, own_raw, ((side_flat, STEP, tall), (side_flat, 2 * STEP, tall)),
        row_terms, col_terms, None, core, mask,
    )
    given = x_own.at[pl.ds(half * (1 - core), half), pl.ds(0, cols)]
    outputs = start_all(sem, 1, ((x_own.at[:, pl.ds(0, cols)], own_out), (given, give_out)))
    add_terms(
        x_near, near_raw, ((side_flat, above_at, tall), (side_flat, below_at, tall)),
        near_terms, col_terms, inside_of(row_at, devices), core, mask,
    )
    wait_all(inputs)
    stats = conv_own_rows(x_own, x_near, weights_of(taps, OWN_TAPS), p_ref, conv_ref)
    stats_ref[...] = jnp.broadcast_to(stats, stats_ref.shape)
    outputs += start_all(sem, 3, ((conv_ref, conv_out),))
    lower = lane_half(LANES)
    for i in range(half):
        for first in range(0, cols, LANES):
            at = slice(first, first + LANES)
            upper_one = conv_ref[i, at, :].astype(jnp.float32)
            upper_two = conv_ref[i + half, at, :].astype(jnp.float32)
            up = jnp.where(lower, upper_one, pltpu.roll(upper_two, LANES // 2, 1))
            down = jnp.where(lower, pltpu.roll(upper_one, LANES // 2, 1), upper_two)
            one_ref[i, at, :] = jnp.where(odd == 1, up, down).astype(jnp.bfloat16)
            two_ref[i, at, :] = jnp.where(odd == 1, down, up).astype(jnp.bfloat16)
    edge_at = pl.multiple_of((cols - 2 * STEP) * (1 - core), 2 * STEP)
    edge_ref[...] = conv_ref[:, pl.ds(edge_at, 2 * STEP), :]
    wait_all(outputs)


def second_kernel(
    devices, cells, own_in, one, two, edge, corner, stats, stats_other, gains, taps_in,
    conv_out, give_out, stats_ref,
    a_own, a_near, conv_ref, p_ref, own, taps, sem,
):
    row_at, core = lax.axis_index(GX), lax.axis_index("gy")
    cols = own.shape[1]
    half = STEP // 2
    odd = lax.rem(row_at, 2)
    inputs = start_all(sem, 0, ((own_in, own), (taps_in, taps)))
    factor, offset = affine_of(0, (stats, stats_other), gains, cells)
    inside = inside_of(row_at, devices)
    mask = reach_mask(core)

    def activated(value):
        return elu(value.astype(jnp.float32) * factor + offset)

    def fill_own(i, _):
        for first in range(0, cols, LANES):
            at = slice(first, first + LANES)
            a_own[i, at, :] = activated(own[i, at, :]).astype(jnp.bfloat16)
        beyond = jnp.where(mask, activated(edge[i]), 0.0)
        a_own[i, cols:, :] = beyond.astype(jnp.bfloat16)
        return 0

    def two_rows(one, two):
        one, two = one.astype(jnp.float32), two.astype(jnp.float32)
        up, down = jnp.where(odd == 1, one, two), jnp.where(odd == 1, two, one)
        lower = lane_half(up.shape[0])
        return (
            jnp.where(lower, up, pltpu.roll(down, LANES // 2, 1)),
            jnp.where(lower, pltpu.roll(up, LANES // 2, 1), down),
        )

    def fill_near(i, _):
        for first in range(0, cols, LANES):
            at = slice(first, first + LANES)
            for k, value in enumerate(two_rows(one[i, at, :], two[i, at, :])):
                a_near[i + half * k, at, :] = (activated(value) * inside).astype(jnp.bfloat16)
        return 0

    for i in range(half):
        for k, value in enumerate(two_rows(corner[0, i], corner[1, i])):
            beyond = jnp.where(mask, activated(value) * inside, 0.0)
            a_near[i + half * k, cols:, :] = beyond.astype(jnp.bfloat16)

    lax.fori_loop(0, half, fill_near, 0)
    wait_all(inputs)
    lax.fori_loop(0, STEP, fill_own, 0)
    stats = conv_own_rows(a_own, a_near, weights_of(taps, OWN_TAPS), p_ref, conv_ref)
    given = conv_ref.at[pl.ds(half * (1 - core), half)]
    outputs = start_all(sem, 0, ((given, give_out), (conv_ref, conv_out)))
    stats_ref[...] = jnp.broadcast_to(stats, stats_ref.shape)
    wait_all(outputs)


def pack_kernel(
    cells, block_in, other, conv_in, conv_other, stats, stats_other, gains,
    block_out_out, send_ref,
    out_ref, own, conv, sem,
):
    core = lax.axis_index("gy")
    cols = conv.shape[1]
    half = STEP // 2
    parts = [
        start_all(
            sem, 2 * n,
            [(src.at[pl.ds(2 * n, 2)], dst.at[pl.ds(2 * n, 2)])
             for src, dst in ((block_in, own), (conv_in, conv))],
        )
        for n in range(STEP // 2)
    ]
    factor, offset = affine_of(1, (stats, stats_other), gains, cells)
    wide = 2 * STEP
    peers, some = cols // wide, LANES // wide

    def block_out(x, value):
        value = x.astype(jnp.float32) + value.astype(jnp.float32) * factor + offset
        return elu(value).astype(jnp.bfloat16)

    def mine(i, _):
        for first in range(0, cols, LANES):
            at = slice(first, first + LANES)
            out_ref[i, at, :] = block_out(own[i, at, :], conv[i, at, :])
        return 0

    for n, part in enumerate(parts):
        wait_all(part)
        lax.fori_loop(2 * n, 2 * n + 2, mine, 0)
    outputs = start_all(sem, STEP, ((out_ref, block_out_out),))

    def step(i, _):
        for first in range(0, cols, LANES):
            at = slice(first, first + LANES)
            value = out_ref[half * core + i, at, :].reshape(some, wide, LANES)
            send_ref[pl.ds(peers * core + first // wide, some), i] = value
            value = block_out(other[i, at, :], conv_other[i, at, :]).reshape(some, wide, LANES)
            send_ref[pl.ds(peers * (1 - core) + first // wide, some), i] = value
        return 0

    lax.fori_loop(0, half, step, 0)
    wait_all(outputs)


def merge_kernel(own_in, received, other, result, out_ref, own, cells_ref, flat_ref, sem):
    core = lax.axis_index("gy")
    channels, rows, cols = out_ref.shape
    peers = other.shape[0]
    inputs = start_all(sem, 0, ((own_in, own),))

    def gather(s, _):
        cells_ref[s, core] = received[peers * core + s].astype(jnp.float32)
        cells_ref[s, 1 - core] = other[s].astype(jnp.float32)
        return 0

    lax.fori_loop(0, peers, gather, 0)
    wait_all(inputs)
    flat = cells_ref.reshape(peers * STEP * rows, LANES)
    some = LANES // rows
    lower = lane_half(some * STEP)

    def step(i):
        for block in range(cols // LANES):
            first = block * some * STEP * rows
            upper_row = flat[pl.ds(first + i, some * STEP, stride=rows), :]
            lower_row = flat[pl.ds(first + STEP + i, some * STEP, stride=rows), :]
            even = jnp.where(lower, upper_row, pltpu.roll(lower_row, channels, 1))
            odd = jnp.where(lower, pltpu.roll(upper_row, channels, 1), lower_row)
            mirrored = jnp.concatenate(
                [
                    part[s * STEP : (s + 1) * STEP]
                    for s in range(some)
                    for part in (even, odd)
                ],
                axis=0,
            )
            value = own[i, block * LANES : (block + 1) * LANES, :].astype(jnp.float32) + mirrored
            value = jnp.transpose(0.5 * value)
            for high in range(rows // STEP):
                flat_ref[block, pl.ds(high * STEP + i, channels, stride=rows), :] = value[
                    channels * high : channels * (high + 1)
                ]

    for i in range(STEP):
        step(i)

    batch = 4

    def store(n, _):
        for block in range(cols // LANES):
            value = flat_ref[block, pl.ds(pl.multiple_of(n * batch * rows, 8), batch * rows), :]
            out_ref[pl.ds(n * batch, batch), :, block * LANES : (block + 1) * LANES] = value.reshape(
                batch, rows, LANES
            ).astype(jnp.bfloat16)
        return 0

    outputs = []
    quarter = channels // 4
    for n in range(4):
        lax.fori_loop(n * quarter // batch, (n + 1) * quarter // batch, store, 0)
        at = pl.ds(n * quarter, quarter)
        outputs += start_all(sem, 1 + n, ((out_ref.at[at], result.at[at]),))
    wait_all(outputs)


def body(residue_feats, pair_feats, w_row, w_col, first_taps, second_taps, norm_scale, norm_shift):
    channels, rows, cols = pair_feats.shape
    cores = lax.axis_size("gy")
    devices = lax.axis_size(GX)
    first_core = lax.axis_index("gy") == 0
    cells = devices * rows * cores * cols
    bf16, f32 = jnp.bfloat16, jnp.float32
    conv_flops = 2 * 9 * channels * channels * rows * cols

    def edge(x):
        return jnp.where(first_core, x[..., cols - LANES :], x[..., :LANES])

    def swap(x):
        return lax.ppermute(x, "gy", SWAP)

    with_next = functools.partial(lax.ppermute, axis_name=GX, perm=pairs_of(devices, 0))
    with_last = functools.partial(lax.ppermute, axis_name=GX, perm=pairs_of(devices, 1))
    eight = (channels + 1, STEP, cols)
    one, two, terms, mine = call(
        prepare_kernel,
        (
            (VMEM, eight, bf16),
            (VMEM, eight, bf16),
            (VMEM, (devices, STEP, LANES), bf16),
            (VMEM, (STEP, LANES), f32),
        ),
        [
            VMEM(residue_feats.shape, bf16),
            VMEM(w_row.T.shape, bf16),
            VMEM(w_col.T.shape, bf16),
        ],
        5,
        conv_flops // 16,
        ((HBM, pair_feats), (HBM, residue_feats), (HBM, w_row.T), (HBM, w_col.T)),
    )
    one, two = with_next(one), with_last(two)
    terms = lax.all_to_all(terms, GX, 0, 0, tiled=True)
    gains = jnp.tile(jnp.concatenate([norm_scale, norm_shift], axis=0), (1, 2))
    near_side = swap(
        jnp.concatenate(
            [edge(one[:channels]), edge(pair_feats), edge(two[:channels])], axis=1
        )
    )

    taps_shape = VMEM(first_taps.shape, bf16)
    whole = (STEP, cols, LANES)
    part = (STEP // 2, cols, LANES)
    wide = (STEP, cols + 2 * STEP, LANES)
    products = VMEM((2, cols + 2 * STEP, 3 * LANES), f32)
    sums = (devices, LANES)
    own_raw, near_raw, near_terms = call(
        turn_kernel,
        ((VMEM, whole, bf16), (VMEM, whole, bf16), (VMEM, (STEP, LANES), f32)),
        [
            VMEM(pair_feats.shape, bf16),
            flat_of(channels, rows, cols),
            flat_of(channels, STEP, cols),
            flat_of(channels, STEP, cols),
        ],
        1,
        conv_flops,
        ((HBM, pair_feats), (VMEM, one), (VMEM, two)),
    )
    own_rows, conv_own, own_give, conv_one, conv_two, edges, stats = call(
        functools.partial(first_kernel, devices),
        (
            (HBM, whole, bf16),
            (HBM, whole, bf16),
            (HBM, part, bf16),
            (VMEM, part, bf16),
            (VMEM, part, bf16),
            (VMEM, (STEP, 2 * STEP, LANES), bf16),
            (VMEM, sums, f32),
        ),
        [
            VMEM(wide, bf16),
            VMEM(wide, bf16),
            VMEM(whole, bf16),
            products,
            taps_shape,
            flat_of(channels, rows + 2 * STEP, LANES),
            VMEM(wide[1:], f32),
            VMEM((STEP, LANES), f32),
        ],
        4,
        conv_flops,
        ((VMEM, own_raw), (VMEM, near_raw), (VMEM, near_terms), (VMEM, near_side),
         (VMEM, terms), (VMEM, mine), (HBM, first_taps)),
    )
    conv_one, conv_two = with_next(conv_one), with_last(conv_two)
    stats = lax.all_to_all(stats, GX, 0, 0, tiled=True)
    stats_other = swap(stats)
    edges = swap(edges)
    last = cols - 2 * STEP
    corners = swap(
        jnp.stack(
            [
                jnp.where(first_core, x[:, last:], x[:, : 2 * STEP])
                for x in (conv_one, conv_two)
            ]
        )
    )
    own_other = swap(own_give)
    conv_second, second_give, stats = call(
        functools.partial(second_kernel, devices, cells),
        ((HBM, whole, bf16), (HBM, part, bf16), (VMEM, sums, f32)),
        [
            VMEM(wide, bf16),
            VMEM(wide, bf16),
            VMEM(whole, bf16),
            products,
            VMEM(whole, bf16),
            taps_shape,
        ],
        2,
        conv_flops,
        ((HBM, conv_own), (VMEM, conv_one), (VMEM, conv_two), (VMEM, edges),
         (VMEM, corners), (VMEM, stats), (VMEM, stats_other), (VMEM, gains),
         (HBM, second_taps)),
    )
    stats = lax.all_to_all(stats, GX, 0, 0, tiled=True)
    stats_other = swap(stats)
    conv_other = swap(second_give)
    block_out, send = call(
        functools.partial(pack_kernel, cells),
        ((HBM, whole, bf16), (VMEM, (devices, STEP // 2, rows, LANES), bf16)),
        [
            VMEM(whole, bf16),
            VMEM(whole, bf16),
            VMEM(whole, bf16),
        ],
        STEP + 1,
        conv_flops,
        ((HBM, own_rows), (VMEM, own_other), (HBM, conv_second), (VMEM, conv_other),
         (VMEM, stats), (VMEM, stats_other), (VMEM, gains)),
    )
    received = lax.all_to_all(send, GX, 0, 0, tiled=True)
    peers = devices // cores
    other = swap(jnp.where(first_core, received[peers:], received[:peers]))
    return call(
        merge_kernel,
        ((HBM, pair_feats.shape, bf16),),
        [
            VMEM(pair_feats.shape, bf16),
            VMEM(whole, bf16),
            VMEM((peers, cores, STEP // 2, rows, LANES), f32),
            flat_of(channels, rows, cols),
        ],
        5,
        conv_flops,
        ((HBM, block_out), (VMEM, received), (VMEM, other)),
    )[0]


def solution(mesh):
    torus = Mesh(
        mesh.devices.reshape(mesh.shape["grp"], 4, 16, mesh.shape["gy"]),
        ("grp", "gx_0", "gx_1", "gy"),
    )
    placed = (P(GRP_GX, None), P(None, GRP_GX, "gy"), P(), P(), P(), P(), P(), P())
    return jax.shard_map(
        body, mesh=torus, in_specs=placed, out_specs=P(None, GRP_GX, "gy"), check_vma=False
    )
```

```python
import functools

import jax
import jax.numpy as jnp
from jax import lax
from jax.experimental import pallas as pl
from jax.experimental.pallas import tpu as pltpu
from jax.sharding import Mesh
from jax.sharding import PartitionSpec as P

STEP = 8
GX = ("gx_0", "gx_1")
GRP_GX = ("grp", "gx_0", "gx_1")
LANES = 128
SWAP = [(0, 1), (1, 0)]
HBM, VMEM = pltpu.HBM, pltpu.VMEM

epsilon = 1e-05


def pairs_of(count, first):
    return [p for i in range(first, count - 1, 2) for p in ((i, i + 1), (i + 1, i))]


def call(kernel, outs, scratch, n_copies, flops, operands):
    spaces = [space for space, _ in operands]
    held = [pltpu.with_memory_space_constraint(x, space) for space, x in operands]
    return pl.pallas_call(
        kernel,
        out_shape=[space(shape, dtype) for space, shape, dtype in outs],
        in_specs=[pl.BlockSpec(memory_space=space) for space in spaces],
        out_specs=[pl.BlockSpec(memory_space=space) for space, _, _ in outs],
        scratch_shapes=[*scratch, pltpu.SemaphoreType.DMA((n_copies,))],
        cost_estimate=pl.CostEstimate(flops=flops, bytes_accessed=1 << 20, transcendentals=0),
        compiler_params=pltpu.CompilerParams(vmem_limit_bytes=12 << 20),
    )(*held)


def start_all(sem, first, pairs):
    copies = [
        pltpu.make_async_copy(src, dst, sem.at[first + i]) for i, (src, dst) in enumerate(pairs)
    ]
    for copy in copies:
        copy.start()
    return copies


def wait_all(copies):
    for copy in copies:
        copy.wait()


def elu(v):
    return jnp.where(v > 0, v, jnp.exp(jnp.minimum(v, 0.0)) - 1.0)


def as_float(flag):
    return jnp.asarray(flag, jnp.int32).astype(jnp.float32)


def lane_half(rows):
    return lax.broadcasted_iota(jnp.int32, (rows, LANES), 1) < LANES // 2


def halves(first, second):
    return jnp.where(lane_half(first.shape[0]), first, pltpu.roll(second, LANES // 2, 1))


def reach_mask(core):
    row = lax.broadcasted_iota(jnp.int32, (2 * STEP, LANES), 0)
    first = STEP * core
    return (row >= first) & (row < first + STEP)


def inside_of(row_at, devices):
    above = as_float(jnp.minimum(row_at, 1))
    below = as_float(jnp.minimum(devices - 1 - row_at, 1))
    return jnp.where(lane_half(1), above, below)


def flat_of(channels, rows, cols):
    return pltpu.VMEM((cols // LANES, channels * rows, LANES), jnp.float32)


def widen(source_ref, flat_ref):
    channels, rows, cols = source_ref.shape
    some = 64 // rows

    def step(i, _):
        for block in range(cols // LANES):
            value = source_ref[pl.ds(i * some, some), :, block * LANES : (block + 1) * LANES]
            flat_ref[block, pl.ds(pl.multiple_of(i * some * rows, 8), some * rows), :] = (
                value.astype(jnp.float32).reshape(some * rows, LANES)
            )
        return 0

    lax.fori_loop(0, channels // some, step, 0)


def two_rows_turned(sources, block, i):
    channels = LANES // 2
    return jnp.transpose(
        jnp.concatenate(
            [
                flat[block, pl.ds(first + i, channels, stride=rows), :]
                for flat, first, rows in sources
            ],
            axis=0,
        )
    )


def turn_rows(out_ref, sources):
    def step(i, _):
        for block in range(out_ref.shape[1] // LANES):
            at = slice(block * LANES, (block + 1) * LANES)
            out_ref[i, at, :] = two_rows_turned(sources, block, i).astype(jnp.bfloat16)
        return 0

    lax.fori_loop(0, STEP, step, 0)


def add_terms(x_ref, raw_ref, side_sources, row_terms, col_terms, scale, core, mask):
    cols = raw_ref.shape[1]

    for i in range(STEP):
        side = two_rows_turned(side_sources, 0, i)
        value = jnp.where(core == 0, side[: 2 * STEP], side[LANES - 2 * STEP :])
        value = value + (row_terms[i : i + 1] + col_terms[cols:, :])
        if scale is not None:
            value = value * scale
        x_ref[i, cols:, :] = jnp.where(mask, value, 0.0).astype(jnp.bfloat16)

    def step(i, _):
        row = row_terms[pl.ds(i, 1), :]
        for block in range(cols // LANES):
            at = slice(block * LANES, (block + 1) * LANES)
            value = raw_ref[i, at, :].astype(jnp.float32) + (row + col_terms[at, :])
            if scale is not None:
                value = value * scale
            x_ref[i, at, :] = value.astype(jnp.bfloat16)
        return 0

    lax.fori_loop(0, STEP, step, 0)


def weights_of(taps_ref, wanted):
    channels = taps_ref.shape[1]
    zero = jnp.zeros((channels, channels), jnp.bfloat16)
    return jnp.concatenate(
        [
            jnp.concatenate(
                [zero if ky is None else taps_ref[3 * ky + kx] for ky in inputs], axis=1
            )
            for kx in range(3)
            for inputs in wanted
        ],
        axis=0,
    )


OWN_TAPS = ((1, 2, 0, None), (0, 1, None, 2))


def product(values, weights):
    return lax.dot_general(
        values, weights, (((1,), (1,)), ((), ())), preferred_element_type=jnp.float32
    )


def shifted_sum(p_ref, first):
    last = p_ref.shape[0]
    if first == 0:
        left = jnp.concatenate([p_ref[last - STEP :, :LANES], p_ref[: LANES - STEP, :LANES]], axis=0)
    else:
        left = p_ref[first - STEP : first - STEP + LANES, :LANES]
    centre = p_ref[first : first + LANES, LANES : 2 * LANES]
    right = p_ref[first + STEP : first + STEP + LANES, 2 * LANES :]
    return left + centre + right


def conv_own_rows(own_ref, near_ref, weights, p_ref, out_ref):
    cols = out_ref.shape[1]
    total = jnp.zeros((STEP, LANES), jnp.float32)
    squares = total
    for i in range(STEP):
        p = p_ref.at[i % 2]
        p[...] = product(jnp.concatenate([own_ref[i], near_ref[i]], axis=1), weights)
        for first in range(0, cols, LANES):
            value = shifted_sum(p, first)
            out_ref[i, first : first + LANES, :] = value.astype(jnp.bfloat16)
            value = value.reshape(LANES // STEP, STEP, LANES)
            total = total + jnp.sum(value, axis=0)
            squares = squares + jnp.sum(value * value, axis=0)
    total = total + pltpu.roll(total, LANES // 2, 1)
    squares = squares + pltpu.roll(squares, LANES // 2, 1)
    return jnp.sum(jnp.where(lane_half(STEP), total, squares), axis=0, keepdims=True)


def affine_of(which, stats_refs, gains_ref, cells):
    row = sum(jnp.sum(ref[...], axis=0, keepdims=True) for ref in stats_refs) / cells
    row = jnp.broadcast_to(row, (STEP, LANES))
    other = pltpu.roll(row, LANES // 2, 1)
    average = jnp.where(lane_half(STEP), row, other)
    spread = jnp.where(lane_half(STEP), other, row) - average * average
    factor = gains_ref[which : which + 1] * lax.rsqrt(spread + epsilon)
    offset = gains_ref[2 + which : 3 + which] - average * factor
    return factor[0:1], offset[0:1]


def prepare_kernel(
    pair, feats, w_row, w_col, one, two, col_terms, row_terms, feats_in, row_in, col_in, sem
):
    odd = lax.rem(lax.axis_index(GX), 2)
    channels = pair.shape[0]
    lower, upper = pl.multiple_of(STEP * (1 - odd), STEP), pl.multiple_of(STEP * odd, STEP)
    parts = start_all(
        sem, 0,
        ((pair.at[:, pl.ds(lower, STEP)], one.at[pl.ds(0, channels)]),
         (pair.at[:, pl.ds(upper, STEP)], two.at[pl.ds(0, channels)])),
    )
    inputs = start_all(sem, 2, ((feats, feats_in), (w_row, row_in), (w_col, col_in)))
    wait_all(inputs)
    zero = jnp.zeros((2 * STEP, LANES - channels), jnp.float32)
    row = jnp.concatenate([product(feats_in[...], row_in[...]), zero], axis=1)
    col = jnp.concatenate([product(feats_in[...], col_in[...]), zero], axis=1)
    packed = halves(col[:STEP], col[STEP:]).astype(jnp.bfloat16)
    col_terms[...] = jnp.broadcast_to(packed[None], col_terms.shape)
    row_terms[...] = halves(row[:STEP], row[STEP:])
    empty = jnp.zeros((STEP, one.shape[2] - LANES), jnp.float32)
    for ref, which in ((one, odd), (two, 1 - odd)):
        rows = jnp.where(which == 0, row[STEP:], row[:STEP])
        ref[channels] = jnp.concatenate([rows, empty], axis=1).astype(jnp.bfloat16)
    wait_all(parts)


def turn_own_kernel(pair, own_ref, own, own_flat, sem):
    rows = own.shape[1]
    wait_all(start_all(sem, 0, ((pair, own),)))
    widen(own, own_flat)
    turn_rows(own_ref, ((own_flat, 0, rows), (own_flat, STEP, rows)))


def widen_halo(halo, which, above_flat, below_flat):
    is_above = lax.rem(lax.axis_index(GX) + which, 2)

    @pl.when(is_above == 1)
    def _():
        widen(halo, above_flat)

    @pl.when(is_above == 0)
    def _():
        widen(halo, below_flat)


def turn_near_kernel(one, two_in, near_ref, row_terms, two, above_flat, below_flat, sem):
    odd = lax.rem(lax.axis_index(GX), 2)
    channels = one.shape[0] - 1
    inputs = start_all(sem, 0, ((two_in, two),))
    widen_halo(one.at[pl.ds(0, channels)], 0, above_flat, below_flat)
    one_terms = one[channels, :, :LANES].astype(jnp.float32)
    wait_all(inputs)
    widen_halo(two.at[pl.ds(0, channels)], 1, above_flat, below_flat)
    two_terms = two[channels, :, :LANES].astype(jnp.float32)
    row_terms[...] = halves(
        jnp.where(odd == 1, one_terms, two_terms), jnp.where(odd == 1, two_terms, one_terms)
    )
    turn_rows(near_ref, ((above_flat, 0, STEP), (below_flat, 0, STEP)))


def first_kernel(
    devices, own_raw, near_raw, near_terms, side, side_one, side_two, terms, mine, taps_in,
    own_out, conv_out, give_out, one_ref, two_ref, edge_ref, stats_ref,
    x_own, x_near, conv_ref, p_ref, taps, side_flat, above_flat, below_flat, col_terms, row_terms,
    sem,
):
    row_at, core = lax.axis_index(GX), lax.axis_index("gy")
    cols = own_raw.shape[1]
    rows, half = 2 * STEP, STEP // 2
    odd = lax.rem(row_at, 2)
    inputs = start_all(sem, 0, ((taps_in, taps),))

    def put_terms(sources):
        values = [(at, terms[source].astype(jnp.float32)) for source, at in sources]
        values = [(at, value, pltpu.roll(value, LANES // 2, 1)) for at, value in values]
        for at, value, other in values:
            col_terms[at : at + STEP] = jnp.where(lane_half(STEP), value, other)
            col_terms[at + STEP : at + 2 * STEP] = jnp.where(lane_half(STEP), other, value)

    peers = cols // rows
    put_terms([(peers * core + i, i * rows) for i in range(peers)] + [(peers - core, cols)])
    row_terms[...] = mine[...].astype(jnp.bfloat16).astype(jnp.float32)
    mask = reach_mask(core)
    widen(side, side_flat)
    add_terms(
        x_own, own_raw, ((side_flat, 0, rows), (side_flat, STEP, rows)),
        row_terms, col_terms, None, core, mask,
    )
    given = x_own.at[pl.ds(half * (1 - core), half), pl.ds(0, cols)]
    outputs = start_all(sem, 1, ((x_own.at[:, pl.ds(0, cols)], own_out), (given, give_out)))
    widen_halo(side_one, 0, above_flat, below_flat)
    widen_halo(side_two, 1, above_flat, below_flat)
    add_terms(
        x_near, near_raw, ((above_flat, 0, STEP), (below_flat, 0, STEP)),
        near_terms, col_terms, inside_of(row_at, devices), core, mask,
    )
    wait_all(inputs)
    stats = conv_own_rows(x_own, x_near, weights_of(taps, OWN_TAPS), p_ref, conv_ref)
    stats_ref[...] = jnp.broadcast_to(stats, stats_ref.shape)
    outputs += start_all(sem, 3, ((conv_ref, conv_out),))
    lower = lane_half(LANES)
    for i in range(half):
        for first in range(0, cols, LANES):
            at = slice(first, first + LANES)
            upper_one = conv_ref[i, at, :].astype(jnp.float32)
            upper_two = conv_ref[i + half, at, :].astype(jnp.float32)
            up = jnp.where(lower, upper_one, pltpu.roll(upper_two, LANES // 2, 1))
            down = jnp.where(lower, pltpu.roll(upper_one, LANES // 2, 1), upper_two)
            one_ref[i, at, :] = jnp.where(odd == 1, up, down).astype(jnp.bfloat16)
            two_ref[i, at, :] = jnp.where(odd == 1, down, up).astype(jnp.bfloat16)
    edge_at = pl.multiple_of((cols - 2 * STEP) * (1 - core), 2 * STEP)
    edge_ref[...] = conv_ref[:, pl.ds(edge_at, 2 * STEP), :]
    wait_all(outputs)


def second_kernel(
    devices, cells, own_in, one, two, edge, corner, stats, stats_other, gains, taps_in,
    conv_out, give_out, stats_ref,
    a_own, a_near, conv_ref, p_ref, own, taps, sem,
):
    row_at, core = lax.axis_index(GX), lax.axis_index("gy")
    cols = own.shape[1]
    half = STEP // 2
    odd = lax.rem(row_at, 2)
    inputs = start_all(sem, 0, ((own_in, own), (taps_in, taps)))
    factor, offset = affine_of(0, (stats, stats_other), gains, cells)
    inside = inside_of(row_at, devices)
    mask = reach_mask(core)

    def activated(value):
        return elu(value.astype(jnp.float32) * factor + offset)

    def fill_own(i, _):
        for first in range(0, cols, LANES):
            at = slice(first, first + LANES)
            a_own[i, at, :] = activated(own[i, at, :]).astype(jnp.bfloat16)
        beyond = jnp.where(mask, activated(edge[i]), 0.0)
        a_own[i, cols:, :] = beyond.astype(jnp.bfloat16)
        return 0

    def two_rows(one, two):
        one, two = one.astype(jnp.float32), two.astype(jnp.float32)
        up, down = jnp.where(odd == 1, one, two), jnp.where(odd == 1, two, one)
        lower = lane_half(up.shape[0])
        return (
            jnp.where(lower, up, pltpu.roll(down, LANES // 2, 1)),
            jnp.where(lower, pltpu.roll(up, LANES // 2, 1), down),
        )

    def fill_near(i, _):
        for first in range(0, cols, LANES):
            at = slice(first, first + LANES)
            for k, value in enumerate(two_rows(one[i, at, :], two[i, at, :])):
                a_near[i + half * k, at, :] = (activated(value) * inside).astype(jnp.bfloat16)
        return 0

    for i in range(half):
        for k, value in enumerate(two_rows(corner[0, i], corner[1, i])):
            beyond = jnp.where(mask, activated(value) * inside, 0.0)
            a_near[i + half * k, cols:, :] = beyond.astype(jnp.bfloat16)

    lax.fori_loop(0, half, fill_near, 0)
    wait_all(inputs)
    lax.fori_loop(0, STEP, fill_own, 0)
    stats = conv_own_rows(a_own, a_near, weights_of(taps, OWN_TAPS), p_ref, conv_ref)
    given = conv_ref.at[pl.ds(half * (1 - core), half)]
    outputs = start_all(sem, 0, ((given, give_out), (conv_ref, conv_out)))
    stats_ref[...] = jnp.broadcast_to(stats, stats_ref.shape)
    wait_all(outputs)


def pack_kernel(
    cells, block_in, other, conv_in, conv_other, stats, stats_other, gains,
    block_out_out, send_ref,
    out_ref, own, conv, sem,
):
    core = lax.axis_index("gy")
    cols = conv.shape[1]
    half = STEP // 2
    parts = [
        start_all(
            sem, 2 * n,
            [(src.at[pl.ds(2 * n, 2)], dst.at[pl.ds(2 * n, 2)])
             for src, dst in ((block_in, own), (conv_in, conv))],
        )
        for n in range(STEP // 2)
    ]
    factor, offset = affine_of(1, (stats, stats_other), gains, cells)
    wide = 2 * STEP
    peers, some = cols // wide, LANES // wide

    def block_out(x, value):
        value = x.astype(jnp.float32) + value.astype(jnp.float32) * factor + offset
        return elu(value).astype(jnp.bfloat16)

    def mine(i, _):
        for first in range(0, cols, LANES):
            at = slice(first, first + LANES)
            out_ref[i, at, :] = block_out(own[i, at, :], conv[i, at, :])
        return 0

    outputs = []
    for n, part in enumerate(parts):
        wait_all(part)
        lax.fori_loop(2 * n, 2 * n + 2, mine, 0)
        at = pl.ds(2 * n, 2)
        outputs += start_all(sem, STEP + n, ((out_ref.at[at], block_out_out.at[at]),))

    def step(i, _):
        for first in range(0, cols, LANES):
            at = slice(first, first + LANES)
            value = out_ref[half * core + i, at, :].reshape(some, wide, LANES)
            send_ref[pl.ds(peers * core + first // wide, some), i] = value
            value = block_out(other[i, at, :], conv_other[i, at, :]).reshape(some, wide, LANES)
            send_ref[pl.ds(peers * (1 - core) + first // wide, some), i] = value
        return 0

    lax.fori_loop(0, half, step, 0)
    wait_all(outputs)


def merge_kernel(own_in, received, other, result, out_ref, own, cells_ref, flat_ref, sem):
    core = lax.axis_index("gy")
    channels, rows, cols = out_ref.shape
    peers = other.shape[0]
    inputs = start_all(sem, 0, ((own_in, own),))

    def gather(s, _):
        cells_ref[s, core] = received[peers * core + s].astype(jnp.float32)
        cells_ref[s, 1 - core] = other[s].astype(jnp.float32)
        return 0

    lax.fori_loop(0, peers, gather, 0)
    wait_all(inputs)
    flat = cells_ref.reshape(peers * STEP * rows, LANES)
    some = LANES // rows
    lower = lane_half(some * STEP)

    def step(i):
        for block in range(cols // LANES):
            first = block * some * STEP * rows
            upper_row = flat[pl.ds(first + i, some * STEP, stride=rows), :]
            lower_row = flat[pl.ds(first + STEP + i, some * STEP, stride=rows), :]
            even = jnp.where(lower, upper_row, pltpu.roll(lower_row, channels, 1))
            odd = jnp.where(lower, pltpu.roll(upper_row, channels, 1), lower_row)
            mirrored = jnp.concatenate(
                [
                    part[s * STEP : (s + 1) * STEP]
                    for s in range(some)
                    for part in (even, odd)
                ],
                axis=0,
            )
            value = own[i, block * LANES : (block + 1) * LANES, :].astype(jnp.float32) + mirrored
            value = jnp.transpose(0.5 * value)
            for high in range(rows // STEP):
                flat_ref[block, pl.ds(high * STEP + i, channels, stride=rows), :] = value[
                    channels * high : channels * (high + 1)
                ]

    for i in range(STEP):
        step(i)

    batch = 4

    def store(n, _):
        for block in range(cols // LANES):
            value = flat_ref[block, pl.ds(pl.multiple_of(n * batch * rows, 8), batch * rows), :]
            out_ref[pl.ds(n * batch, batch), :, block * LANES : (block + 1) * LANES] = value.reshape(
                batch, rows, LANES
            ).astype(jnp.bfloat16)
        return 0

    outputs = []
    quarter = channels // 4
    for n in range(4):
        lax.fori_loop(n * quarter // batch, (n + 1) * quarter // batch, store, 0)
        at = pl.ds(n * quarter, quarter)
        outputs += start_all(sem, 1 + n, ((out_ref.at[at], result.at[at]),))
    wait_all(outputs)


def body(residue_feats, pair_feats, w_row, w_col, first_taps, second_taps, norm_scale, norm_shift):
    channels, rows, cols = pair_feats.shape
    cores = lax.axis_size("gy")
    devices = lax.axis_size(GX)
    first_core = lax.axis_index("gy") == 0
    cells = devices * rows * cores * cols
    bf16, f32 = jnp.bfloat16, jnp.float32
    conv_flops = 2 * 9 * channels * channels * rows * cols

    def edge(x):
        return jnp.where(first_core, x[..., cols - LANES :], x[..., :LANES])

    def swap(x):
        return lax.ppermute(x, "gy", SWAP)

    with_next = functools.partial(lax.ppermute, axis_name=GX, perm=pairs_of(devices, 0))
    with_last = functools.partial(lax.ppermute, axis_name=GX, perm=pairs_of(devices, 1))
    eight = (channels + 1, STEP, cols)
    one, two, terms, mine = call(
        prepare_kernel,
        (
            (VMEM, eight, bf16),
            (VMEM, eight, bf16),
            (VMEM, (devices, STEP, LANES), bf16),
            (VMEM, (STEP, LANES), f32),
        ),
        [
            VMEM(residue_feats.shape, bf16),
            VMEM(w_row.T.shape, bf16),
            VMEM(w_col.T.shape, bf16),
        ],
        5,
        conv_flops // 16,
        ((HBM, pair_feats), (HBM, residue_feats), (HBM, w_row.T), (HBM, w_col.T)),
    )
    one, two = with_next(one), with_last(two)
    terms = lax.all_to_all(terms, GX, 0, 0, tiled=True)
    gains = jnp.tile(jnp.concatenate([norm_scale, norm_shift], axis=0), (1, 2))
    own_side = swap(edge(pair_feats))
    one_side, two_side = swap(edge(one[:channels])), swap(edge(two[:channels]))

    taps_shape = VMEM(first_taps.shape, bf16)
    whole = (STEP, cols, LANES)
    part = (STEP // 2, cols, LANES)
    wide = (STEP, cols + 2 * STEP, LANES)
    products = VMEM((2, cols + 2 * STEP, 3 * LANES), f32)
    sums = (devices, LANES)
    (own_raw,) = call(
        turn_own_kernel,
        ((VMEM, whole, bf16),),
        [VMEM(pair_feats.shape, bf16), flat_of(channels, rows, cols)],
        1,
        conv_flops,
        ((HBM, pair_feats),),
    )
    near_raw, near_terms = call(
        turn_near_kernel,
        ((VMEM, whole, bf16), (VMEM, (STEP, LANES), f32)),
        [VMEM(two.shape, bf16), flat_of(channels, STEP, cols), flat_of(channels, STEP, cols)],
        1,
        conv_flops,
        ((VMEM, one), (HBM, two)),
    )
    own_rows, conv_own, own_give, conv_one, conv_two, edges, stats = call(
        functools.partial(first_kernel, devices),
        (
            (HBM, whole, bf16),
            (HBM, whole, bf16),
            (HBM, part, bf16),
            (VMEM, part, bf16),
            (VMEM, part, bf16),
            (VMEM, (STEP, 2 * STEP, LANES), bf16),
            (VMEM, sums, f32),
        ),
        [
            VMEM(wide, bf16),
            VMEM(wide, bf16),
            VMEM(whole, bf16),
            products,
            taps_shape,
            flat_of(channels, rows, LANES),
            flat_of(channels, STEP, LANES),
            flat_of(channels, STEP, LANES),
            VMEM(wide[1:], f32),
            VMEM((STEP, LANES), f32),
        ],
        4,
        conv_flops,
        ((VMEM, own_raw), (VMEM, near_raw), (VMEM, near_terms), (VMEM, own_side),
         (VMEM, one_side), (VMEM, two_side), (VMEM, terms), (VMEM, mine), (HBM, first_taps)),
    )
    conv_one, conv_two = with_next(conv_one), with_last(conv_two)
    stats = lax.all_to_all(stats, GX, 0, 0, tiled=True)
    stats_other = swap(stats)
    edges = swap(edges)
    last = cols - 2 * STEP
    corners = swap(
        jnp.stack(
            [
                jnp.where(first_core, x[:, last:], x[:, : 2 * STEP])
                for x in (conv_one, conv_two)
            ]
        )
    )
    own_other = swap(own_give)
    conv_second, second_give, stats = call(
        functools.partial(second_kernel, devices, cells),
        ((HBM, whole, bf16), (HBM, part, bf16), (VMEM, sums, f32)),
        [
            VMEM(wide, bf16),
            VMEM(wide, bf16),
            VMEM(whole, bf16),
            products,
            VMEM(whole, bf16),
            taps_shape,
        ],
        2,
        conv_flops,
        ((HBM, conv_own), (VMEM, conv_one), (VMEM, conv_two), (VMEM, edges),
         (VMEM, corners), (VMEM, stats), (VMEM, stats_other), (VMEM, gains),
         (HBM, second_taps)),
    )
    stats = lax.all_to_all(stats, GX, 0, 0, tiled=True)
    stats_other = swap(stats)
    conv_other = swap(second_give)
    block_out, send = call(
        functools.partial(pack_kernel, cells),
        ((HBM, whole, bf16), (VMEM, (devices, STEP // 2, rows, LANES), bf16)),
        [
            VMEM(whole, bf16),
            VMEM(whole, bf16),
            VMEM(whole, bf16),
        ],
        STEP + STEP // 2,
        conv_flops,
        ((HBM, own_rows), (VMEM, own_other), (HBM, conv_second), (VMEM, conv_other),
         (VMEM, stats), (VMEM, stats_other), (VMEM, gains)),
    )
    received = lax.all_to_all(send, GX, 0, 0, tiled=True)
    peers = devices // cores
    other = swap(jnp.where(first_core, received[peers:], received[:peers]))
    return call(
        merge_kernel,
        ((HBM, pair_feats.shape, bf16),),
        [
            VMEM(pair_feats.shape, bf16),
            VMEM(whole, bf16),
            VMEM((peers, cores, STEP // 2, rows, LANES), f32),
            flat_of(channels, rows, cols),
        ],
        5,
        conv_flops,
        ((HBM, block_out), (VMEM, received), (VMEM, other)),
    )[0]


def solution(mesh):
    torus = Mesh(
        mesh.devices.reshape(mesh.shape["grp"], 4, 16, mesh.shape["gy"]),
        ("grp", "gx_0", "gx_1", "gy"),
    )
    placed = (P(GRP_GX, None), P(None, GRP_GX, "gy"), P(), P(), P(), P(), P(), P())
    return jax.shard_map(
        body, mesh=torus, in_specs=placed, out_specs=P(None, GRP_GX, "gy"), check_vma=False
    )
```

```python
import functools

import jax
import jax.numpy as jnp
from jax import lax
from jax.experimental import pallas as pl
from jax.experimental.pallas import tpu as pltpu
from jax.sharding import Mesh
from jax.sharding import PartitionSpec as P

STEP = 8
GX = ("gx_0", "gx_1")
GRP_GX = ("grp", "gx_0", "gx_1")
LANES = 128
SWAP = [(0, 1), (1, 0)]
HBM, VMEM = pltpu.HBM, pltpu.VMEM

epsilon = 1e-05


def pairs_of(count, first):
    return [p for i in range(first, count - 1, 2) for p in ((i, i + 1), (i + 1, i))]


def call(kernel, outs, scratch, n_copies, flops, operands):
    spaces = [space for space, _ in operands]
    held = [pltpu.with_memory_space_constraint(x, space) for space, x in operands]
    return pl.pallas_call(
        kernel,
        out_shape=[space(shape, dtype) for space, shape, dtype in outs],
        in_specs=[pl.BlockSpec(memory_space=space) for space in spaces],
        out_specs=[pl.BlockSpec(memory_space=space) for space, _, _ in outs],
        scratch_shapes=[*scratch, pltpu.SemaphoreType.DMA((n_copies,))],
        cost_estimate=pl.CostEstimate(flops=flops, bytes_accessed=1 << 20, transcendentals=0),
        compiler_params=pltpu.CompilerParams(vmem_limit_bytes=12 << 20),
    )(*held)


def start_all(sem, first, pairs):
    copies = [
        pltpu.make_async_copy(src, dst, sem.at[first + i]) for i, (src, dst) in enumerate(pairs)
    ]
    for copy in copies:
        copy.start()
    return copies


def wait_all(copies):
    for copy in copies:
        copy.wait()


def elu(v):
    return jnp.where(v > 0, v, jnp.exp(jnp.minimum(v, 0.0)) - 1.0)


def as_float(flag):
    return jnp.asarray(flag, jnp.int32).astype(jnp.float32)


def lane_half(rows):
    return lax.broadcasted_iota(jnp.int32, (rows, LANES), 1) < LANES // 2


def halves(first, second):
    return jnp.where(lane_half(first.shape[0]), first, pltpu.roll(second, LANES // 2, 1))


def reach_mask(core):
    row = lax.broadcasted_iota(jnp.int32, (2 * STEP, LANES), 0)
    first = STEP * core
    return (row >= first) & (row < first + STEP)


def inside_of(row_at, devices):
    above = as_float(jnp.minimum(row_at, 1))
    below = as_float(jnp.minimum(devices - 1 - row_at, 1))
    return jnp.where(lane_half(1), above, below)


def flat_of(channels, rows, cols):
    return pltpu.VMEM((cols // LANES, channels * rows, LANES), jnp.float32)


def widen(source_ref, flat_ref):
    channels, rows, cols = source_ref.shape
    some = 64 // rows

    def step(i, _):
        for block in range(cols // LANES):
            value = source_ref[pl.ds(i * some, some), :, block * LANES : (block + 1) * LANES]
            flat_ref[block, pl.ds(pl.multiple_of(i * some * rows, 8), some * rows), :] = (
                value.astype(jnp.float32).reshape(some * rows, LANES)
            )
        return 0

    lax.fori_loop(0, channels // some, step, 0)


def two_rows_turned(sources, block, i):
    channels = LANES // 2
    return jnp.transpose(
        jnp.concatenate(
            [
                flat[block, pl.ds(first + i, channels, stride=rows), :]
                for flat, first, rows in sources
            ],
            axis=0,
        )
    )


def turn_rows(out_ref, sources):
    def step(n, _):
        for i in (2 * n, 2 * n + 1):
            for block in range(out_ref.shape[1] // LANES):
                at = slice(block * LANES, (block + 1) * LANES)
                out_ref[i, at, :] = two_rows_turned(sources, block, i).astype(jnp.bfloat16)
        return 0

    lax.fori_loop(0, STEP // 2, step, 0)


def add_terms(x_ref, raw_ref, side_sources, row_terms, col_terms, scale, core, mask):
    cols = raw_ref.shape[1]

    for i in range(STEP):
        side = two_rows_turned(side_sources, 0, i)
        value = jnp.where(core == 0, side[: 2 * STEP], side[LANES - 2 * STEP :])
        value = value + (row_terms[i : i + 1] + col_terms[cols:, :])
        if scale is not None:
            value = value * scale
        x_ref[i, cols:, :] = jnp.where(mask, value, 0.0).astype(jnp.bfloat16)

    def step(i, _):
        row = row_terms[pl.ds(i, 1), :]
        for block in range(cols // LANES):
            at = slice(block * LANES, (block + 1) * LANES)
            value = raw_ref[i, at, :].astype(jnp.float32) + (row + col_terms[at, :])
            if scale is not None:
                value = value * scale
            x_ref[i, at, :] = value.astype(jnp.bfloat16)
        return 0

    lax.fori_loop(0, STEP, step, 0)


def weights_of(taps_ref, wanted):
    channels = taps_ref.shape[1]
    zero = jnp.zeros((channels, channels), jnp.bfloat16)
    return jnp.concatenate(
        [
            jnp.concatenate(
                [zero if ky is None else taps_ref[3 * ky + kx] for ky in inputs], axis=1
            )
            for kx in range(3)
            for inputs in wanted
        ],
        axis=0,
    )


OWN_TAPS = ((1, 2, 0, None), (0, 1, None, 2))


def product(values, weights):
    return lax.dot_general(
        values, weights, (((1,), (1,)), ((), ())), preferred_element_type=jnp.float32
    )


def shifted_sum(p_ref, first):
    last = p_ref.shape[0]
    if first == 0:
        left = jnp.concatenate([p_ref[last - STEP :, :LANES], p_ref[: LANES - STEP, :LANES]], axis=0)
    else:
        left = p_ref[first - STEP : first - STEP + LANES, :LANES]
    centre = p_ref[first : first + LANES, LANES : 2 * LANES]
    right = p_ref[first + STEP : first + STEP + LANES, 2 * LANES :]
    return left + centre + right


def conv_own_rows(own_ref, near_ref, weights, p_ref, out_ref, leave):
    cols = out_ref.shape[1]
    total = jnp.zeros((STEP, LANES), jnp.float32)
    squares = total
    for i in range(STEP):
        p = p_ref.at[i % 2]
        p[...] = product(jnp.concatenate([own_ref[i], near_ref[i]], axis=1), weights)
        for first in range(0, cols, LANES):
            value = shifted_sum(p, first)
            out_ref[i, first : first + LANES, :] = value.astype(jnp.bfloat16)
            value = value.reshape(LANES // STEP, STEP, LANES)
            total = total + jnp.sum(value, axis=0)
            squares = squares + jnp.sum(value * value, axis=0)
        leave(i)
    total = total + pltpu.roll(total, LANES // 2, 1)
    squares = squares + pltpu.roll(squares, LANES // 2, 1)
    return jnp.sum(jnp.where(lane_half(STEP), total, squares), axis=0, keepdims=True)


def affine_of(which, stats_refs, gains_ref, cells):
    row = sum(jnp.sum(ref[...], axis=0, keepdims=True) for ref in stats_refs) / cells
    row = jnp.broadcast_to(row, (STEP, LANES))
    other = pltpu.roll(row, LANES // 2, 1)
    average = jnp.where(lane_half(STEP), row, other)
    spread = jnp.where(lane_half(STEP), other, row) - average * average
    factor = gains_ref[which : which + 1] * lax.rsqrt(spread + epsilon)
    offset = gains_ref[2 + which : 3 + which] - average * factor
    return factor[0:1], offset[0:1]


def prepare_kernel(
    pair, feats, w_row, w_col, one, two, col_terms, row_terms, feats_in, row_in, col_in, sem
):
    odd = lax.rem(lax.axis_index(GX), 2)
    channels = pair.shape[0]
    lower, upper = pl.multiple_of(STEP * (1 - odd), STEP), pl.multiple_of(STEP * odd, STEP)
    parts = start_all(
        sem, 0,
        ((pair.at[:, pl.ds(lower, STEP)], one.at[pl.ds(0, channels)]),
         (pair.at[:, pl.ds(upper, STEP)], two.at[pl.ds(0, channels)])),
    )
    inputs = start_all(sem, 2, ((feats, feats_in), (w_row, row_in), (w_col, col_in)))
    wait_all(inputs)
    zero = jnp.zeros((2 * STEP, LANES - channels), jnp.float32)
    row = jnp.concatenate([product(feats_in[...], row_in[...]), zero], axis=1)
    col = jnp.concatenate([product(feats_in[...], col_in[...]), zero], axis=1)
    packed = halves(col[:STEP], col[STEP:]).astype(jnp.bfloat16)
    col_terms[...] = jnp.broadcast_to(packed[None], col_terms.shape)
    row_terms[...] = halves(row[:STEP], row[STEP:])
    empty = jnp.zeros((STEP, one.shape[2] - LANES), jnp.float32)
    for ref, which in ((one, odd), (two, 1 - odd)):
        rows = jnp.where(which == 0, row[STEP:], row[:STEP])
        ref[channels] = jnp.concatenate([rows, empty], axis=1).astype(jnp.bfloat16)
    wait_all(parts)


def turn_own_kernel(pair, own_ref, own, own_flat, sem):
    rows = own.shape[1]
    wait_all(start_all(sem, 0, ((pair, own),)))
    widen(own, own_flat)
    turn_rows(own_ref, ((own_flat, 0, rows), (own_flat, STEP, rows)))


def widen_halo(halo, which, above_flat, below_flat):
    is_above = lax.rem(lax.axis_index(GX) + which, 2)

    @pl.when(is_above == 1)
    def _():
        widen(halo, above_flat)

    @pl.when(is_above == 0)
    def _():
        widen(halo, below_flat)


def turn_near_kernel(one_in, two, near_ref, row_terms, one, above_flat, below_flat, sem):
    odd = lax.rem(lax.axis_index(GX), 2)
    channels = two.shape[0] - 1
    inputs = start_all(sem, 0, ((one_in, one),))
    widen_halo(two.at[pl.ds(0, channels)], 1, above_flat, below_flat)
    two_terms = two[channels, :, :LANES].astype(jnp.float32)
    wait_all(inputs)
    widen_halo(one.at[pl.ds(0, channels)], 0, above_flat, below_flat)
    one_terms = one[channels, :, :LANES].astype(jnp.float32)
    row_terms[...] = halves(
        jnp.where(odd == 1, one_terms, two_terms), jnp.where(odd == 1, two_terms, one_terms)
    )
    turn_rows(near_ref, ((above_flat, 0, STEP), (below_flat, 0, STEP)))


def first_kernel(
    devices, own_raw, near_raw, near_terms, side, side_one, side_two, terms, mine, taps_in,
    own_out, conv_out, give_out, one_ref, two_ref, edge_ref, stats_ref,
    x_own, x_near, conv_ref, p_ref, taps, side_flat, above_flat, below_flat, col_terms, row_terms,
    sem,
):
    row_at, core = lax.axis_index(GX), lax.axis_index("gy")
    cols = own_raw.shape[1]
    rows, half = 2 * STEP, STEP // 2
    odd = lax.rem(row_at, 2)
    inputs = start_all(sem, 0, ((taps_in, taps),))

    def put_terms(sources):
        values = [(at, terms[source].astype(jnp.float32)) for source, at in sources]
        values = [(at, value, pltpu.roll(value, LANES // 2, 1)) for at, value in values]
        for at, value, other in values:
            col_terms[at : at + STEP] = jnp.where(lane_half(STEP), value, other)
            col_terms[at + STEP : at + 2 * STEP] = jnp.where(lane_half(STEP), other, value)

    peers = cols // rows
    put_terms([(peers * core + i, i * rows) for i in range(peers)] + [(peers - core, cols)])
    row_terms[...] = mine[...].astype(jnp.bfloat16).astype(jnp.float32)
    mask = reach_mask(core)
    widen(side, side_flat)
    add_terms(
        x_own, own_raw, ((side_flat, 0, rows), (side_flat, STEP, rows)),
        row_terms, col_terms, None, core, mask,
    )
    given = x_own.at[pl.ds(half * (1 - core), half), pl.ds(0, cols)]
    outputs = start_all(sem, 1, ((x_own.at[:, pl.ds(0, cols)], own_out), (given, give_out)))
    widen_halo(side_one, 0, above_flat, below_flat)
    widen_halo(side_two, 1, above_flat, below_flat)
    add_terms(
        x_near, near_raw, ((above_flat, 0, STEP), (below_flat, 0, STEP)),
        near_terms, col_terms, inside_of(row_at, devices), core, mask,
    )
    wait_all(inputs)

    def leave(i):
        if i % half == half - 1:
            at = pl.ds(i - half + 1, half)
            outputs.extend(start_all(sem, 3 + i // half, ((conv_ref.at[at], conv_out.at[at]),)))

    stats = conv_own_rows(x_own, x_near, weights_of(taps, OWN_TAPS), p_ref, conv_ref, leave)
    stats_ref[...] = jnp.broadcast_to(stats, stats_ref.shape)
    lower = lane_half(LANES)
    for i in range(half):
        for first in range(0, cols, LANES):
            at = slice(first, first + LANES)
            upper_one = conv_ref[i, at, :].astype(jnp.float32)
            upper_two = conv_ref[i + half, at, :].astype(jnp.float32)
            up = jnp.where(lower, upper_one, pltpu.roll(upper_two, LANES // 2, 1))
            down = jnp.where(lower, pltpu.roll(upper_one, LANES // 2, 1), upper_two)
            one_ref[i, at, :] = jnp.where(odd == 1, up, down).astype(jnp.bfloat16)
            two_ref[i, at, :] = jnp.where(odd == 1, down, up).astype(jnp.bfloat16)
    edge_at = pl.multiple_of((cols - 2 * STEP) * (1 - core), 2 * STEP)
    edge_ref[...] = conv_ref[:, pl.ds(edge_at, 2 * STEP), :]
    wait_all(outputs)


def second_kernel(
    devices, cells, own_in, one, two, edge, corner, stats, stats_other, gains, taps_in,
    conv_out, give_out, stats_ref,
    a_own, a_near, conv_ref, p_ref, own, taps, sem,
):
    row_at, core = lax.axis_index(GX), lax.axis_index("gy")
    cols = own.shape[1]
    half = STEP // 2
    odd = lax.rem(row_at, 2)
    inputs = start_all(sem, 0, ((own_in, own), (taps_in, taps)))
    factor, offset = affine_of(0, (stats, stats_other), gains, cells)
    inside = inside_of(row_at, devices)
    mask = reach_mask(core)

    def activated(value):
        return elu(value.astype(jnp.float32) * factor + offset)

    def fill_own(i, _):
        for first in range(0, cols, LANES):
            at = slice(first, first + LANES)
            a_own[i, at, :] = activated(own[i, at, :]).astype(jnp.bfloat16)
        beyond = jnp.where(mask, activated(edge[i]), 0.0)
        a_own[i, cols:, :] = beyond.astype(jnp.bfloat16)
        return 0

    def two_rows(one, two):
        one, two = one.astype(jnp.float32), two.astype(jnp.float32)
        up, down = jnp.where(odd == 1, one, two), jnp.where(odd == 1, two, one)
        lower = lane_half(up.shape[0])
        return (
            jnp.where(lower, up, pltpu.roll(down, LANES // 2, 1)),
            jnp.where(lower, pltpu.roll(up, LANES // 2, 1), down),
        )

    def fill_near(i, _):
        for first in range(0, cols, LANES):
            at = slice(first, first + LANES)
            for k, value in enumerate(two_rows(one[i, at, :], two[i, at, :])):
                a_near[i + half * k, at, :] = (activated(value) * inside).astype(jnp.bfloat16)
        return 0

    for i in range(half):
        for k, value in enumerate(two_rows(corner[0, i], corner[1, i])):
            beyond = jnp.where(mask, activated(value) * inside, 0.0)
            a_near[i + half * k, cols:, :] = beyond.astype(jnp.bfloat16)

    lax.fori_loop(0, half, fill_near, 0)
    wait_all(inputs)
    lax.fori_loop(0, STEP, fill_own, 0)
    outputs = []

    def leave(i):
        if i % half == half - 1:
            at = pl.ds(i - half + 1, half)
            outputs.extend(start_all(sem, i // half, ((conv_ref.at[at], conv_out.at[at]),)))

    stats = conv_own_rows(a_own, a_near, weights_of(taps, OWN_TAPS), p_ref, conv_ref, leave)
    given = conv_ref.at[pl.ds(half * (1 - core), half)]
    outputs += start_all(sem, 2, ((given, give_out),))
    stats_ref[...] = jnp.broadcast_to(stats, stats_ref.shape)
    wait_all(outputs)


def pack_kernel(
    cells, block_in, other, conv_in, conv_other, stats, stats_other, gains,
    block_out_out, send_ref,
    out_ref, own, conv, sem,
):
    core = lax.axis_index("gy")
    cols = conv.shape[1]
    half = STEP // 2
    parts = [
        start_all(
            sem, 2 * n,
            [(src.at[pl.ds(2 * n, 2)], dst.at[pl.ds(2 * n, 2)])
             for src, dst in ((block_in, own), (conv_in, conv))],
        )
        for n in range(STEP // 2)
    ]
    factor, offset = affine_of(1, (stats, stats_other), gains, cells)
    wide = 2 * STEP
    peers, some = cols // wide, LANES // wide

    def block_out(x, value):
        value = x.astype(jnp.float32) + value.astype(jnp.float32) * factor + offset
        return elu(value).astype(jnp.bfloat16)

    def mine(i, _):
        for first in range(0, cols, LANES):
            at = slice(first, first + LANES)
            out_ref[i, at, :] = block_out(own[i, at, :], conv[i, at, :])
        return 0

    outputs = []
    for n, part in enumerate(parts):
        wait_all(part)
        lax.fori_loop(2 * n, 2 * n + 2, mine, 0)
        at = pl.ds(2 * n, 2)
        outputs += start_all(sem, STEP + n, ((out_ref.at[at], block_out_out.at[at]),))

    def step(i, _):
        for first in range(0, cols, LANES):
            at = slice(first, first + LANES)
            value = out_ref[half * core + i, at, :].reshape(some, wide, LANES)
            send_ref[pl.ds(peers * core + first // wide, some), i] = value
            value = block_out(other[i, at, :], conv_other[i, at, :]).reshape(some, wide, LANES)
            send_ref[pl.ds(peers * (1 - core) + first // wide, some), i] = value
        return 0

    lax.fori_loop(0, half, step, 0)
    wait_all(outputs)


def merge_kernel(own_in, received, other, result, out_ref, own, cells_ref, flat_ref, sem):
    core = lax.axis_index("gy")
    channels, rows, cols = out_ref.shape
    peers = other.shape[0]
    inputs = start_all(sem, 0, ((own_in, own),))

    def gather(s, _):
        cells_ref[s, core] = received[peers * core + s].astype(jnp.float32)
        cells_ref[s, 1 - core] = other[s].astype(jnp.float32)
        return 0

    lax.fori_loop(0, peers, gather, 0)
    wait_all(inputs)
    flat = cells_ref.reshape(peers * STEP * rows, LANES)
    some = LANES // rows
    lower = lane_half(some * STEP)

    def step(i):
        for block in range(cols // LANES):
            first = block * some * STEP * rows
            upper_row = flat[pl.ds(first + i, some * STEP, stride=rows), :]
            lower_row = flat[pl.ds(first + STEP + i, some * STEP, stride=rows), :]
            even = jnp.where(lower, upper_row, pltpu.roll(lower_row, channels, 1))
            odd = jnp.where(lower, pltpu.roll(upper_row, channels, 1), lower_row)
            mirrored = jnp.concatenate(
                [
                    part[s * STEP : (s + 1) * STEP]
                    for s in range(some)
                    for part in (even, odd)
                ],
                axis=0,
            )
            value = own[i, block * LANES : (block + 1) * LANES, :].astype(jnp.float32) + mirrored
            value = jnp.transpose(0.5 * value)
            for high in range(rows // STEP):
                flat_ref[block, pl.ds(high * STEP + i, channels, stride=rows), :] = value[
                    channels * high : channels * (high + 1)
                ]

    for i in range(STEP):
        step(i)

    batch = 4

    def store(n, _):
        for block in range(cols // LANES):
            value = flat_ref[block, pl.ds(pl.multiple_of(n * batch * rows, 8), batch * rows), :]
            out_ref[pl.ds(n * batch, batch), :, block * LANES : (block + 1) * LANES] = value.reshape(
                batch, rows, LANES
            ).astype(jnp.bfloat16)
        return 0

    outputs = []
    quarter = channels // 4
    for n in range(4):
        lax.fori_loop(n * quarter // batch, (n + 1) * quarter // batch, store, 0)
        at = pl.ds(n * quarter, quarter)
        outputs += start_all(sem, 1 + n, ((out_ref.at[at], result.at[at]),))
    wait_all(outputs)


def body(residue_feats, pair_feats, w_row, w_col, first_taps, second_taps, norm_scale, norm_shift):
    channels, rows, cols = pair_feats.shape
    cores = lax.axis_size("gy")
    devices = lax.axis_size(GX)
    first_core = lax.axis_index("gy") == 0
    cells = devices * rows * cores * cols
    bf16, f32 = jnp.bfloat16, jnp.float32
    conv_flops = 2 * 9 * channels * channels * rows * cols

    def edge(x):
        return jnp.where(first_core, x[..., cols - LANES :], x[..., :LANES])

    def swap(x):
        return lax.ppermute(x, "gy", SWAP)

    with_next = functools.partial(lax.ppermute, axis_name=GX, perm=pairs_of(devices, 0))
    with_last = functools.partial(lax.ppermute, axis_name=GX, perm=pairs_of(devices, 1))
    eight = (channels + 1, STEP, cols)
    one, two, terms, mine = call(
        prepare_kernel,
        (
            (VMEM, eight, bf16),
            (VMEM, eight, bf16),
            (VMEM, (devices, STEP, LANES), bf16),
            (VMEM, (STEP, LANES), f32),
        ),
        [
            VMEM(residue_feats.shape, bf16),
            VMEM(w_row.T.shape, bf16),
            VMEM(w_col.T.shape, bf16),
        ],
        5,
        conv_flops // 16,
        ((HBM, pair_feats), (HBM, residue_feats), (HBM, w_row.T), (HBM, w_col.T)),
    )
    one, two = with_next(one), with_last(two)
    terms = lax.all_to_all(terms, GX, 0, 0, tiled=True)
    gains = jnp.tile(jnp.concatenate([norm_scale, norm_shift], axis=0), (1, 2))
    own_side = swap(edge(pair_feats))
    one_side, two_side = swap(edge(one[:channels])), swap(edge(two[:channels]))

    taps_shape = VMEM(first_taps.shape, bf16)
    whole = (STEP, cols, LANES)
    part = (STEP // 2, cols, LANES)
    wide = (STEP, cols + 2 * STEP, LANES)
    products = VMEM((2, cols + 2 * STEP, 3 * LANES), f32)
    sums = (devices, LANES)
    (own_raw,) = call(
        turn_own_kernel,
        ((VMEM, whole, bf16),),
        [VMEM(pair_feats.shape, bf16), flat_of(channels, rows, cols)],
        1,
        conv_flops,
        ((HBM, pair_feats),),
    )
    near_raw, near_terms = call(
        turn_near_kernel,
        ((VMEM, whole, bf16), (VMEM, (STEP, LANES), f32)),
        [VMEM(two.shape, bf16), flat_of(channels, STEP, cols), flat_of(channels, STEP, cols)],
        1,
        conv_flops,
        ((HBM, one), (VMEM, two)),
    )
    own_rows, conv_own, own_give, conv_one, conv_two, edges, stats = call(
        functools.partial(first_kernel, devices),
        (
            (HBM, whole, bf16),
            (HBM, whole, bf16),
            (HBM, part, bf16),
            (VMEM, part, bf16),
            (VMEM, part, bf16),
            (VMEM, (STEP, 2 * STEP, LANES), bf16),
            (VMEM, sums, f32),
        ),
        [
            VMEM(wide, bf16),
            VMEM(wide, bf16),
            VMEM(whole, bf16),
            products,
            taps_shape,
            flat_of(channels, rows, LANES),
            flat_of(channels, STEP, LANES),
            flat_of(channels, STEP, LANES),
            VMEM(wide[1:], f32),
            VMEM((STEP, LANES), f32),
        ],
        5,
        conv_flops,
        ((VMEM, own_raw), (VMEM, near_raw), (VMEM, near_terms), (VMEM, own_side),
         (VMEM, one_side), (VMEM, two_side), (VMEM, terms), (VMEM, mine), (HBM, first_taps)),
    )
    conv_one, conv_two = with_next(conv_one), with_last(conv_two)
    stats = lax.all_to_all(stats, GX, 0, 0, tiled=True)
    stats_other = swap(stats)
    edges = swap(edges)
    last = cols - 2 * STEP
    corners = swap(
        jnp.stack(
            [
                jnp.where(first_core, x[:, last:], x[:, : 2 * STEP])
                for x in (conv_one, conv_two)
            ]
        )
    )
    own_other = swap(own_give)
    conv_second, second_give, stats = call(
        functools.partial(second_kernel, devices, cells),
        ((HBM, whole, bf16), (HBM, part, bf16), (VMEM, sums, f32)),
        [
            VMEM(wide, bf16),
            VMEM(wide, bf16),
            VMEM(whole, bf16),
            products,
            VMEM(whole, bf16),
            taps_shape,
        ],
        3,
        conv_flops,
        ((HBM, conv_own), (VMEM, conv_one), (VMEM, conv_two), (VMEM, edges),
         (VMEM, corners), (VMEM, stats), (VMEM, stats_other), (VMEM, gains),
         (HBM, second_taps)),
    )
    stats = lax.all_to_all(stats, GX, 0, 0, tiled=True)
    stats_other = swap(stats)
    conv_other = swap(second_give)
    block_out, send = call(
        functools.partial(pack_kernel, cells),
        ((HBM, whole, bf16), (VMEM, (devices, STEP // 2, rows, LANES), bf16)),
        [
            VMEM(whole, bf16),
            VMEM(whole, bf16),
            VMEM(whole, bf16),
        ],
        STEP + STEP // 2,
        conv_flops,
        ((HBM, own_rows), (VMEM, own_other), (HBM, conv_second), (VMEM, conv_other),
         (VMEM, stats), (VMEM, stats_other), (VMEM, gains)),
    )
    received = lax.all_to_all(send, GX, 0, 0, tiled=True)
    peers = devices // cores
    other = swap(jnp.where(first_core, received[peers:], received[:peers]))
    return call(
        merge_kernel,
        ((HBM, pair_feats.shape, bf16),),
        [
            VMEM(pair_feats.shape, bf16),
            VMEM(whole, bf16),
            VMEM((peers, cores, STEP // 2, rows, LANES), f32),
            flat_of(channels, rows, cols),
        ],
        5,
        conv_flops,
        ((HBM, block_out), (VMEM, received), (VMEM, other)),
    )[0]


def solution(mesh):
    torus = Mesh(
        mesh.devices.reshape(mesh.shape["grp"], 4, 16, mesh.shape["gy"]),
        ("grp", "gx_0", "gx_1", "gy"),
    )
    placed = (P(GRP_GX, None), P(None, GRP_GX, "gy"), P(), P(), P(), P(), P(), P())
    return jax.shard_map(
        body, mesh=torus, in_specs=placed, out_specs=P(None, GRP_GX, "gy"), check_vma=False
    )
```

```python
import functools

import jax
import jax.numpy as jnp
from jax import lax
from jax.experimental import pallas as pl
from jax.experimental.pallas import tpu as pltpu
from jax.sharding import Mesh
from jax.sharding import PartitionSpec as P

STEP = 8
GX = ("gx_0", "gx_1")
GRP_GX = ("grp", "gx_0", "gx_1")
LANES = 128
SWAP = [(0, 1), (1, 0)]
HBM, VMEM = pltpu.HBM, pltpu.VMEM

epsilon = 1e-05


def pairs_of(count, first):
    return [p for i in range(first, count - 1, 2) for p in ((i, i + 1), (i + 1, i))]


def call(kernel, outs, scratch, n_copies, flops, operands):
    spaces = [space for space, _ in operands]
    held = [pltpu.with_memory_space_constraint(x, space) for space, x in operands]
    return pl.pallas_call(
        kernel,
        out_shape=[space(shape, dtype) for space, shape, dtype in outs],
        in_specs=[pl.BlockSpec(memory_space=space) for space in spaces],
        out_specs=[pl.BlockSpec(memory_space=space) for space, _, _ in outs],
        scratch_shapes=[*scratch, pltpu.SemaphoreType.DMA((n_copies,))],
        cost_estimate=pl.CostEstimate(flops=flops, bytes_accessed=1 << 20, transcendentals=0),
        compiler_params=pltpu.CompilerParams(vmem_limit_bytes=12 << 20),
    )(*held)


def start_all(sem, first, pairs):
    copies = [
        pltpu.make_async_copy(src, dst, sem.at[first + i]) for i, (src, dst) in enumerate(pairs)
    ]
    for copy in copies:
        copy.start()
    return copies


def wait_all(copies):
    for copy in copies:
        copy.wait()


def elu(v):
    return jnp.where(v > 0, v, jnp.exp(jnp.minimum(v, 0.0)) - 1.0)


def as_float(flag):
    return jnp.asarray(flag, jnp.int32).astype(jnp.float32)


def lane_half(rows):
    return lax.broadcasted_iota(jnp.int32, (rows, LANES), 1) < LANES // 2


def halves(first, second):
    return jnp.where(lane_half(first.shape[0]), first, pltpu.roll(second, LANES // 2, 1))


def reach_mask(core):
    row = lax.broadcasted_iota(jnp.int32, (2 * STEP, LANES), 0)
    first = STEP * core
    return (row >= first) & (row < first + STEP)


def inside_of(row_at, devices):
    above = as_float(jnp.minimum(row_at, 1))
    below = as_float(jnp.minimum(devices - 1 - row_at, 1))
    return jnp.where(lane_half(1), above, below)


def flat_of(channels, rows, cols):
    return pltpu.VMEM((cols // LANES, channels * rows, LANES), jnp.float32)


def widen(source_ref, flat_ref):
    channels, rows, cols = source_ref.shape
    some = 64 // rows

    def step(i, _):
        for block in range(cols // LANES):
            value = source_ref[pl.ds(i * some, some), :, block * LANES : (block + 1) * LANES]
            flat_ref[block, pl.ds(pl.multiple_of(i * some * rows, 8), some * rows), :] = (
                value.astype(jnp.float32).reshape(some * rows, LANES)
            )
        return 0

    lax.fori_loop(0, channels // some, step, 0)


def two_rows_turned(sources, block, i):
    channels = LANES // 2
    return jnp.transpose(
        jnp.concatenate(
            [
                flat[block, pl.ds(first + i, channels, stride=rows), :]
                for flat, first, rows in sources
            ],
            axis=0,
        )
    )


def turn_rows(out_ref, sources):
    def step(n, _):
        for i in (2 * n, 2 * n + 1):
            for block in range(out_ref.shape[1] // LANES):
                at = slice(block * LANES, (block + 1) * LANES)
                out_ref[i, at, :] = two_rows_turned(sources, block, i).astype(jnp.bfloat16)
        return 0

    lax.fori_loop(0, STEP // 2, step, 0)


def add_terms(x_ref, raw_ref, side_sources, row_terms, col_terms, scale, core, mask):
    cols = raw_ref.shape[1]

    for i in range(STEP):
        side = two_rows_turned(side_sources, 0, i)
        value = jnp.where(core == 0, side[: 2 * STEP], side[LANES - 2 * STEP :])
        value = value + (row_terms[i : i + 1] + col_terms[cols:, :])
        if scale is not None:
            value = value * scale
        x_ref[i, cols:, :] = jnp.where(mask, value, 0.0).astype(jnp.bfloat16)

    def step(i, _):
        row = row_terms[pl.ds(i, 1), :]
        for block in range(cols // LANES):
            at = slice(block * LANES, (block + 1) * LANES)
            value = raw_ref[i, at, :].astype(jnp.float32) + (row + col_terms[at, :])
            if scale is not None:
                value = value * scale
            x_ref[i, at, :] = value.astype(jnp.bfloat16)
        return 0

    lax.fori_loop(0, STEP, step, 0)


def weights_of(taps_ref, wanted):
    channels = taps_ref.shape[1]
    zero = jnp.zeros((channels, channels), jnp.bfloat16)
    return jnp.concatenate(
        [
            jnp.concatenate(
                [zero if ky is None else taps_ref[3 * ky + kx] for ky in inputs], axis=1
            )
            for kx in range(3)
            for inputs in wanted
        ],
        axis=0,
    )


OWN_TAPS = ((1, 2, 0, None), (0, 1, None, 2))


def product(values, weights):
    return lax.dot_general(
        values, weights, (((1,), (1,)), ((), ())), preferred_element_type=jnp.float32
    )


def shifted_sum(p_ref, first):
    last = p_ref.shape[0]
    if first == 0:
        left = jnp.concatenate([p_ref[last - STEP :, :LANES], p_ref[: LANES - STEP, :LANES]], axis=0)
    else:
        left = p_ref[first - STEP : first - STEP + LANES, :LANES]
    centre = p_ref[first : first + LANES, LANES : 2 * LANES]
    right = p_ref[first + STEP : first + STEP + LANES, 2 * LANES :]
    return left + centre + right


def conv_own_rows(own_ref, near_ref, weights, p_ref, out_ref, leave):
    cols = out_ref.shape[1]
    total = jnp.zeros((STEP, LANES), jnp.float32)
    squares = total
    for i in range(STEP):
        p = p_ref.at[i % 2]
        p[...] = product(jnp.concatenate([own_ref[i], near_ref[i]], axis=1), weights)
        for first in range(0, cols, LANES):
            value = shifted_sum(p, first)
            out_ref[i, first : first + LANES, :] = value.astype(jnp.bfloat16)
            value = value.reshape(LANES // STEP, STEP, LANES)
            total = total + jnp.sum(value, axis=0)
            squares = squares + jnp.sum(value * value, axis=0)
        leave(i)
    total = total + pltpu.roll(total, LANES // 2, 1)
    squares = squares + pltpu.roll(squares, LANES // 2, 1)
    return jnp.sum(jnp.where(lane_half(STEP), total, squares), axis=0, keepdims=True)


def affine_of(which, stats_refs, gains_ref, cells):
    row = sum(jnp.sum(ref[...], axis=0, keepdims=True) for ref in stats_refs) / cells
    row = jnp.broadcast_to(row, (STEP, LANES))
    other = pltpu.roll(row, LANES // 2, 1)
    average = jnp.where(lane_half(STEP), row, other)
    spread = jnp.where(lane_half(STEP), other, row) - average * average
    factor = gains_ref[which : which + 1] * lax.rsqrt(spread + epsilon)
    offset = gains_ref[2 + which : 3 + which] - average * factor
    return factor[0:1], offset[0:1]


def prepare_kernel(
    pair, feats, w_row, w_col, one, two, col_terms, row_terms, feats_in, row_in, col_in, sem
):
    odd = lax.rem(lax.axis_index(GX), 2)
    channels = pair.shape[0]
    lower, upper = pl.multiple_of(STEP * (1 - odd), STEP), pl.multiple_of(STEP * odd, STEP)
    parts = start_all(
        sem, 0,
        ((pair.at[:, pl.ds(lower, STEP)], one.at[pl.ds(0, channels)]),
         (pair.at[:, pl.ds(upper, STEP)], two.at[pl.ds(0, channels)])),
    )
    inputs = start_all(sem, 2, ((feats, feats_in), (w_row, row_in), (w_col, col_in)))
    wait_all(inputs)
    zero = jnp.zeros((2 * STEP, LANES - channels), jnp.float32)
    row = jnp.concatenate([product(feats_in[...], row_in[...]), zero], axis=1)
    col = jnp.concatenate([product(feats_in[...], col_in[...]), zero], axis=1)
    packed = halves(col[:STEP], col[STEP:]).astype(jnp.bfloat16)
    col_terms[...] = jnp.broadcast_to(packed[None], col_terms.shape)
    row_terms[...] = halves(row[:STEP], row[STEP:])
    empty = jnp.zeros((STEP, one.shape[2] - LANES), jnp.float32)
    for ref, which in ((one, odd), (two, 1 - odd)):
        rows = jnp.where(which == 0, row[STEP:], row[:STEP])
        ref[channels] = jnp.concatenate([rows, empty], axis=1).astype(jnp.bfloat16)
    wait_all(parts)


def turn_own_kernel(pair, own_ref, own, own_flat, sem):
    rows = own.shape[1]
    wait_all(start_all(sem, 0, ((pair, own),)))
    widen(own, own_flat)
    turn_rows(own_ref, ((own_flat, 0, rows), (own_flat, STEP, rows)))


def widen_halo(halo, which, above_flat, below_flat):
    is_above = lax.rem(lax.axis_index(GX) + which, 2)

    @pl.when(is_above == 1)
    def _():
        widen(halo, above_flat)

    @pl.when(is_above == 0)
    def _():
        widen(halo, below_flat)


def turn_near_kernel(one_in, two, near_ref, row_terms, one, above_flat, below_flat, sem):
    odd = lax.rem(lax.axis_index(GX), 2)
    channels = two.shape[0] - 1
    inputs = start_all(sem, 0, ((one_in, one),))
    widen_halo(two.at[pl.ds(0, channels)], 1, above_flat, below_flat)
    two_terms = two[channels, :, :LANES].astype(jnp.float32)
    wait_all(inputs)
    widen_halo(one.at[pl.ds(0, channels)], 0, above_flat, below_flat)
    one_terms = one[channels, :, :LANES].astype(jnp.float32)
    row_terms[...] = halves(
        jnp.where(odd == 1, one_terms, two_terms), jnp.where(odd == 1, two_terms, one_terms)
    )
    turn_rows(near_ref, ((above_flat, 0, STEP), (below_flat, 0, STEP)))


def first_kernel(
    devices, own_raw, near_raw, near_terms, side, side_one, side_two, terms, mine, taps_in,
    own_out, conv_out, give_out, one_ref, two_ref, edge_ref, stats_ref,
    x_own, x_near, conv_ref, p_ref, taps, side_flat, above_flat, below_flat, col_terms, row_terms,
    sem,
):
    row_at, core = lax.axis_index(GX), lax.axis_index("gy")
    cols = own_raw.shape[1]
    rows, half = 2 * STEP, STEP // 2
    odd = lax.rem(row_at, 2)
    inputs = start_all(sem, 0, ((taps_in, taps),))

    def put_terms(sources):
        values = [(at, terms[source].astype(jnp.float32)) for source, at in sources]
        values = [(at, value, pltpu.roll(value, LANES // 2, 1)) for at, value in values]
        for at, value, other in values:
            col_terms[at : at + STEP] = jnp.where(lane_half(STEP), value, other)
            col_terms[at + STEP : at + 2 * STEP] = jnp.where(lane_half(STEP), other, value)

    peers = cols // rows
    put_terms([(peers * core + i, i * rows) for i in range(peers)] + [(peers - core, cols)])
    row_terms[...] = mine[...].astype(jnp.bfloat16).astype(jnp.float32)
    mask = reach_mask(core)
    widen(side, side_flat)
    add_terms(
        x_own, own_raw, ((side_flat, 0, rows), (side_flat, STEP, rows)),
        row_terms, col_terms, None, core, mask,
    )
    given = x_own.at[pl.ds(half * (1 - core), half), pl.ds(0, cols)]
    outputs = start_all(sem, 1, ((x_own.at[:, pl.ds(0, cols)], own_out), (given, give_out)))
    widen_halo(side_one, 0, above_flat, below_flat)
    widen_halo(side_two, 1, above_flat, below_flat)
    add_terms(
        x_near, near_raw, ((above_flat, 0, STEP), (below_flat, 0, STEP)),
        near_terms, col_terms, inside_of(row_at, devices), core, mask,
    )
    wait_all(inputs)

    def leave(i):
        if i % half == half - 1:
            at = pl.ds(i - half + 1, half)
            outputs.extend(start_all(sem, 3 + i // half, ((conv_ref.at[at], conv_out.at[at]),)))

    stats = conv_own_rows(x_own, x_near, weights_of(taps, OWN_TAPS), p_ref, conv_ref, leave)
    stats_ref[...] = jnp.broadcast_to(stats, stats_ref.shape)
    lower = lane_half(LANES)
    for i in range(half):
        for first in range(0, cols, LANES):
            at = slice(first, first + LANES)
            upper_one = conv_ref[i, at, :].astype(jnp.float32)
            upper_two = conv_ref[i + half, at, :].astype(jnp.float32)
            up = jnp.where(lower, upper_one, pltpu.roll(upper_two, LANES // 2, 1))
            down = jnp.where(lower, pltpu.roll(upper_one, LANES // 2, 1), upper_two)
            one_ref[i, at, :] = jnp.where(odd == 1, up, down).astype(jnp.bfloat16)
            two_ref[i, at, :] = jnp.where(odd == 1, down, up).astype(jnp.bfloat16)
    edge_at = pl.multiple_of((cols - 2 * STEP) * (1 - core), 2 * STEP)
    edge_ref[...] = conv_ref[:, pl.ds(edge_at, 2 * STEP), :]
    wait_all(outputs)


def second_kernel(
    devices, cells, own_in, one, two, edge, corner, stats, stats_other, gains, taps_in,
    conv_out, give_out, stats_ref,
    a_own, a_near, conv_ref, p_ref, own, taps, sem,
):
    row_at, core = lax.axis_index(GX), lax.axis_index("gy")
    cols = own.shape[1]
    half = STEP // 2
    odd = lax.rem(row_at, 2)
    inputs = start_all(sem, 0, ((own_in, own), (taps_in, taps)))
    factor, offset = affine_of(0, (stats, stats_other), gains, cells)
    inside = inside_of(row_at, devices)
    mask = reach_mask(core)

    def activated(value):
        return elu(value.astype(jnp.float32) * factor + offset)

    def fill_own(i, _):
        for first in range(0, cols, LANES):
            at = slice(first, first + LANES)
            a_own[i, at, :] = activated(own[i, at, :]).astype(jnp.bfloat16)
        beyond = jnp.where(mask, activated(edge[i]), 0.0)
        a_own[i, cols:, :] = beyond.astype(jnp.bfloat16)
        return 0

    def two_rows(one, two):
        one, two = one.astype(jnp.float32), two.astype(jnp.float32)
        up, down = jnp.where(odd == 1, one, two), jnp.where(odd == 1, two, one)
        lower = lane_half(up.shape[0])
        return (
            jnp.where(lower, up, pltpu.roll(down, LANES // 2, 1)),
            jnp.where(lower, pltpu.roll(up, LANES // 2, 1), down),
        )

    def fill_near(i, _):
        for first in range(0, cols, LANES):
            at = slice(first, first + LANES)
            for k, value in enumerate(two_rows(one[i, at, :], two[i, at, :])):
                a_near[i + half * k, at, :] = (activated(value) * inside).astype(jnp.bfloat16)
        return 0

    for i in range(half):
        for k, value in enumerate(two_rows(corner[0, i], corner[1, i])):
            beyond = jnp.where(mask, activated(value) * inside, 0.0)
            a_near[i + half * k, cols:, :] = beyond.astype(jnp.bfloat16)

    lax.fori_loop(0, half, fill_near, 0)
    wait_all(inputs)
    lax.fori_loop(0, STEP, fill_own, 0)
    outputs = []

    def leave(i):
        if i % half == half - 1:
            at = pl.ds(i - half + 1, half)
            outputs.extend(start_all(sem, i // half, ((conv_ref.at[at], conv_out.at[at]),)))

    stats = conv_own_rows(a_own, a_near, weights_of(taps, OWN_TAPS), p_ref, conv_ref, leave)
    given = conv_ref.at[pl.ds(half * (1 - core), half)]
    outputs += start_all(sem, 2, ((given, give_out),))
    stats_ref[...] = jnp.broadcast_to(stats, stats_ref.shape)
    wait_all(outputs)


def pack_kernel(
    cells, block_in, other, conv_in, conv_other, stats, stats_other, gains,
    block_out_out, send_ref,
    out_ref, own, conv, sem,
):
    core = lax.axis_index("gy")
    cols = conv.shape[1]
    half = STEP // 2
    parts = [
        start_all(
            sem, 2 * n,
            [(src.at[pl.ds(2 * n, 2)], dst.at[pl.ds(2 * n, 2)])
             for src, dst in ((block_in, own), (conv_in, conv))],
        )
        for n in range(STEP // 2)
    ]
    factor, offset = affine_of(1, (stats, stats_other), gains, cells)
    wide = 2 * STEP
    peers, some = cols // wide, LANES // wide

    def block_out(x, value):
        value = x.astype(jnp.float32) + value.astype(jnp.float32) * factor + offset
        return elu(value).astype(jnp.bfloat16)

    def mine(i, _):
        for first in range(0, cols, LANES):
            at = slice(first, first + LANES)
            out_ref[i, at, :] = block_out(own[i, at, :], conv[i, at, :])
        return 0

    outputs = []
    for n, part in enumerate(parts):
        wait_all(part)
        lax.fori_loop(2 * n, 2 * n + 2, mine, 0)
        at = pl.ds(2 * n, 2)
        outputs += start_all(sem, STEP + n, ((out_ref.at[at], block_out_out.at[at]),))

    def step(i, _):
        for first in range(0, cols, LANES):
            at = slice(first, first + LANES)
            value = out_ref[half * core + i, at, :].reshape(some, wide, LANES)
            send_ref[pl.ds(peers * core + first // wide, some), i] = value
            value = block_out(other[i, at, :], conv_other[i, at, :]).reshape(some, wide, LANES)
            send_ref[pl.ds(peers * (1 - core) + first // wide, some), i] = value
        return 0

    lax.fori_loop(0, half, step, 0)
    wait_all(outputs)


def merge_kernel(own_in, received, other, result, out_ref, own, cells_ref, flat_ref, sem):
    core = lax.axis_index("gy")
    channels, rows, cols = out_ref.shape
    peers = other.shape[0]
    inputs = start_all(sem, 0, ((own_in, own),))

    def gather(s, _):
        cells_ref[s, core] = received[peers * core + s].astype(jnp.float32)
        cells_ref[s, 1 - core] = other[s].astype(jnp.float32)
        return 0

    lax.fori_loop(0, peers, gather, 0)
    wait_all(inputs)
    flat = cells_ref.reshape(peers * STEP * rows, LANES)
    some = LANES // rows
    lower = lane_half(some * STEP)

    def step(i):
        for block in range(cols // LANES):
            first = block * some * STEP * rows
            upper_row = flat[pl.ds(first + i, some * STEP, stride=rows), :]
            lower_row = flat[pl.ds(first + STEP + i, some * STEP, stride=rows), :]
            even = jnp.where(lower, upper_row, pltpu.roll(lower_row, channels, 1))
            odd = jnp.where(lower, pltpu.roll(upper_row, channels, 1), lower_row)
            mirrored = jnp.concatenate(
                [
                    part[s * STEP : (s + 1) * STEP]
                    for s in range(some)
                    for part in (even, odd)
                ],
                axis=0,
            )
            value = own[i, block * LANES : (block + 1) * LANES, :].astype(jnp.float32) + mirrored
            value = jnp.transpose(0.5 * value)
            for high in range(rows // STEP):
                flat_ref[block, pl.ds(high * STEP + i, channels, stride=rows), :] = value[
                    channels * high : channels * (high + 1)
                ]

    for i in range(STEP):
        step(i)

    batch = 4

    def store(n, _):
        for block in range(cols // LANES):
            value = flat_ref[block, pl.ds(pl.multiple_of(n * batch * rows, 8), batch * rows), :]
            out_ref[pl.ds(n * batch, batch), :, block * LANES : (block + 1) * LANES] = value.reshape(
                batch, rows, LANES
            ).astype(jnp.bfloat16)
        return 0

    outputs = []
    quarter = channels // 4
    for n in range(4):
        lax.fori_loop(n * quarter // batch, (n + 1) * quarter // batch, store, 0)
        at = pl.ds(n * quarter, quarter)
        outputs += start_all(sem, 1 + n, ((out_ref.at[at], result.at[at]),))
    wait_all(outputs)


def body(residue_feats, pair_feats, w_row, w_col, first_taps, second_taps, norm_scale, norm_shift):
    channels, rows, cols = pair_feats.shape
    cores = lax.axis_size("gy")
    devices = lax.axis_size(GX)
    first_core = lax.axis_index("gy") == 0
    cells = devices * rows * cores * cols
    bf16, f32 = jnp.bfloat16, jnp.float32
    conv_flops = 2 * 9 * channels * channels * rows * cols

    def edge(x):
        return jnp.where(first_core, x[..., cols - LANES :], x[..., :LANES])

    def swap(x):
        return lax.ppermute(x, "gy", SWAP)

    with_next = functools.partial(lax.ppermute, axis_name=GX, perm=pairs_of(devices, 0))
    with_last = functools.partial(lax.ppermute, axis_name=GX, perm=pairs_of(devices, 1))
    eight = (channels + 1, STEP, cols)
    one, two, terms, mine = call(
        prepare_kernel,
        (
            (VMEM, eight, bf16),
            (VMEM, eight, bf16),
            (VMEM, (devices, STEP, LANES), bf16),
            (VMEM, (STEP, LANES), f32),
        ),
        [
            VMEM(residue_feats.shape, bf16),
            VMEM(w_row.T.shape, bf16),
            VMEM(w_col.T.shape, bf16),
        ],
        5,
        conv_flops // 16,
        ((HBM, pair_feats), (HBM, residue_feats), (HBM, w_row.T), (HBM, w_col.T)),
    )
    one, two = with_next(one), with_last(two)
    terms = lax.all_to_all(terms, GX, 0, 0, tiled=True)
    gains = jnp.concatenate([norm_scale, norm_shift], axis=0)
    gains = jnp.concatenate([gains, gains], axis=1)
    own_side = swap(edge(pair_feats))
    one_side, two_side = swap(edge(one[:channels])), swap(edge(two[:channels]))

    taps_shape = VMEM(first_taps.shape, bf16)
    whole = (STEP, cols, LANES)
    part = (STEP // 2, cols, LANES)
    wide = (STEP, cols + 2 * STEP, LANES)
    products = VMEM((2, cols + 2 * STEP, 3 * LANES), f32)
    sums = (devices, LANES)
    (own_raw,) = call(
        turn_own_kernel,
        ((VMEM, whole, bf16),),
        [VMEM(pair_feats.shape, bf16), flat_of(channels, rows, cols)],
        1,
        conv_flops,
        ((HBM, pair_feats),),
    )
    near_raw, near_terms = call(
        turn_near_kernel,
        ((VMEM, whole, bf16), (VMEM, (STEP, LANES), f32)),
        [VMEM(two.shape, bf16), flat_of(channels, STEP, cols), flat_of(channels, STEP, cols)],
        1,
        conv_flops,
        ((HBM, one), (VMEM, two)),
    )
    own_rows, conv_own, own_give, conv_one, conv_two, edges, stats = call(
        functools.partial(first_kernel, devices),
        (
            (HBM, whole, bf16),
            (HBM, whole, bf16),
            (HBM, part, bf16),
            (VMEM, part, bf16),
            (VMEM, part, bf16),
            (VMEM, (STEP, 2 * STEP, LANES), bf16),
            (VMEM, sums, f32),
        ),
        [
            VMEM(wide, bf16),
            VMEM(wide, bf16),
            VMEM(whole, bf16),
            products,
            taps_shape,
            flat_of(channels, rows, LANES),
            flat_of(channels, STEP, LANES),
            flat_of(channels, STEP, LANES),
            VMEM(wide[1:], f32),
            VMEM((STEP, LANES), f32),
        ],
        5,
        conv_flops,
        ((VMEM, own_raw), (VMEM, near_raw), (VMEM, near_terms), (VMEM, own_side),
         (VMEM, one_side), (VMEM, two_side), (VMEM, terms), (VMEM, mine), (HBM, first_taps)),
    )
    conv_one = with_next(conv_one)
    conv_two = with_last(conv_two)
    stats = lax.all_to_all(stats, GX, 0, 0, tiled=True)
    stats_other = swap(stats)
    edges = swap(edges)
    last = cols - 2 * STEP
    corners = swap(
        jnp.stack(
            [
                jnp.where(first_core, x[:, last:], x[:, : 2 * STEP])
                for x in (conv_one, conv_two)
            ]
        )
    )
    own_other = swap(own_give)
    conv_second, second_give, stats = call(
        functools.partial(second_kernel, devices, cells),
        ((HBM, whole, bf16), (HBM, part, bf16), (VMEM, sums, f32)),
        [
            VMEM(wide, bf16),
            VMEM(wide, bf16),
            VMEM(whole, bf16),
            products,
            VMEM(whole, bf16),
            taps_shape,
        ],
        3,
        conv_flops,
        ((HBM, conv_own), (VMEM, conv_one), (VMEM, conv_two), (VMEM, edges),
         (VMEM, corners), (VMEM, stats), (VMEM, stats_other), (VMEM, gains),
         (HBM, second_taps)),
    )
    stats = lax.all_to_all(stats, GX, 0, 0, tiled=True)
    stats_other = swap(stats)
    conv_other = swap(second_give)
    block_out, send = call(
        functools.partial(pack_kernel, cells),
        ((HBM, whole, bf16), (VMEM, (devices, STEP // 2, rows, LANES), bf16)),
        [
            VMEM(whole, bf16),
            VMEM(whole, bf16),
            VMEM(whole, bf16),
        ],
        STEP + STEP // 2,
        conv_flops,
        ((HBM, own_rows), (VMEM, own_other), (HBM, conv_second), (VMEM, conv_other),
         (VMEM, stats), (VMEM, stats_other), (VMEM, gains)),
    )
    received = lax.all_to_all(send, GX, 0, 0, tiled=True)
    peers = devices // cores
    other = swap(jnp.where(first_core, received[peers:], received[:peers]))
    return call(
        merge_kernel,
        ((HBM, pair_feats.shape, bf16),),
        [
            VMEM(pair_feats.shape, bf16),
            VMEM(whole, bf16),
            VMEM((peers, cores, STEP // 2, rows, LANES), f32),
            flat_of(channels, rows, cols),
        ],
        5,
        conv_flops,
        ((HBM, block_out), (VMEM, received), (VMEM, other)),
    )[0]


def solution(mesh):
    torus = Mesh(
        mesh.devices.reshape(mesh.shape["grp"], 4, 16, mesh.shape["gy"]),
        ("grp", "gx_0", "gx_1", "gy"),
    )
    placed = (P(GRP_GX, None), P(None, GRP_GX, "gy"), P(), P(), P(), P(), P(), P())
    return jax.shard_map(
        body, mesh=torus, in_specs=placed, out_specs=P(None, GRP_GX, "gy"), check_vma=False
    )
```
